8 devices in a mesh: dp: 2 (over y, z), tp: 4 (over x, core).
Axes of the slice: x: 2, y: 2, z: 1, core: 2. Of those that a mesh axis runs over, the one named last changes fastest.
Arguments:
- x: bfloat16 [4096, 1024], P('dp'), parts along dimension 0
- dy: bfloat16 [4096, 1024], P('dp'), parts along dimension 0
- gate: bfloat16 [4096, 3072], P('dp', 'tp'), parts along dimension 0
- up: bfloat16 [4096, 3072], P('dp', 'tp'), parts along dimension 0
- w_gate: bfloat16 [1024, 3072], P(None, 'tp')
- w_up: bfloat16 [1024, 3072], P(None, 'tp')
- w_down: bfloat16 [3072, 1024], P('tp')
Outputs:
- output 1: bfloat16 [4096, 1024], P('dp'), parts along dimension 0
- output 2: bfloat16 [2048, 3072], P('dp', 'tp'), parts along dimension 0
- output 3: bfloat16 [2048, 3072], P('dp', 'tp'), parts along dimension 0
- output 4: bfloat16 [6144, 1024], P(('dp', 'tp')), parts along dimension 0
There are 2 independent parts. The reference program is written for one: setup_inputs(seed, part) draws one part's arguments, and reference() takes and returns one part's arrays. A program takes and returns all parts, laid end to end along the dimension named above; an argument that names none is the same for every part.
All inputs are finite; a program needn't handle non-finite values.
Results may differ from the reference program's by a relative error of at most 0.012.
Values are sent between devices in bfloat16 or wider.
A program may use at most 2 GiB of HBM per device.

```python
import jax
import jax.numpy as jnp

ROWS = 2048
D = 1024
FF = 3072


def act(gate, up):
    return jax.nn.silu(gate) * up


def setup_inputs(seed: int = 0, part: int = 0) -> dict:
    kx, ky, ka, kb, kg, ku, kd = jax.random.split(jax.random.key(seed), 7)
    kx, ky, ka, kb = (jax.random.fold_in(k, part) for k in (kx, ky, ka, kb))
    drawn = {
        "x": jax.random.normal(kx, (ROWS, D), jnp.float32),
        "dy": jax.random.normal(ky, (ROWS, D), jnp.float32),
        "gate": jax.random.normal(ka, (ROWS, FF), jnp.float32),
        "up": jax.random.normal(kb, (ROWS, FF), jnp.float32),
        "w_gate": jax.random.normal(kg, (D, FF), jnp.float32) * D**-0.5,
        "w_up": jax.random.normal(ku, (D, FF), jnp.float32) * D**-0.5,
        "w_down": jax.random.normal(kd, (FF, D), jnp.float32) * FF**-0.5,
    }
    return {k: v.astype(jnp.bfloat16) for k, v in drawn.items()}


def reference(x, dy, gate, up, w_gate, w_up, w_down):
    hidden, back = jax.vjp(act, gate.astype(jnp.float32), up.astype(jnp.float32))
    d_hidden = jnp.dot(dy, w_down.T, preferred_element_type=jnp.float32)
    d_gate, d_up = (g.astype(jnp.bfloat16) for g in back(d_hidden))
    dx = jnp.dot(d_gate, w_gate.T, preferred_element_type=jnp.float32) + jnp.dot(d_up, w_up.T, preferred_element_type=jnp.float32)
    dw_gate = jnp.dot(x.T, d_gate, preferred_element_type=jnp.float32)
    dw_up = jnp.dot(x.T, d_up, preferred_element_type=jnp.float32)
    dw_down = jnp.dot(hidden.astype(jnp.bfloat16).T, dy, preferred_element_type=jnp.float32)
    return tuple(g.astype(jnp.bfloat16) for g in (dx, dw_gate, dw_up, dw_down))
```

```python
import jax
import jax.numpy as jnp
from jax import lax
from jax.experimental import pallas as pl
from jax.experimental.pallas import tpu as pltpu
from jax.sharding import PartitionSpec as P

MESH = pl.DeviceIdType.MESH
F32, BF16 = jnp.float32, jnp.bfloat16
R = 64


def dot_t(a, b):
    return lax.dot_general(a, b, (((1,), (1,)), ((), ())), preferred_element_type=F32)


def dot(a, b):
    return lax.dot_general(a, b, (((1,), (0,)), ((), ())), preferred_element_type=F32)


def kernel(
    x_h, dy_h, gate_h, up_h, wg_h, wu_h, wd_h,
    dx, dwg, dwu, dwd,
    xv, dyv, gv, uv, wgu, wd, dgu, hid, xt, own, tsend, trecv, psend, precv,
    load_sem, blk_sem, t_s, t_r, p_s, p_r, f_s, f_r, o_s, o_r, w_s, w_r,
):
    rows, d = dyv.shape
    f = wd.shape[0]
    half = rows // 2
    steps = rows // (2 * R)
    hs = steps // 2
    me = lax.axis_index("tp")
    chip, core = me // 2, me % 2
    partner, peer = chip * 2 + (1 - core), (1 - chip) * 2 + core

    def base(i):
        return pl.multiple_of(lax.rem((1 - chip) * half + i * (2 * R), rows), 2 * R)

    def block(b, k):
        return pl.ds(pl.multiple_of(b + k * R, R), R)

    def load(i):
        r = pl.ds(base(i), 2 * R)
        return [
            pltpu.make_async_copy(src.at[r], dst.at[r], blk_sem.at[i, n])
            for n, (src, dst) in enumerate(((dy_h, dyv), (gate_h, gv), (up_h, uv)))
        ]

    def remote(src, dst, s, r, i, to):
        return pltpu.make_async_remote_copy(
            src_ref=src, dst_ref=dst, send_sem=s.at[i], recv_sem=r.at[i], device_id={"tp": to}, device_id_type=MESH
        )

    def term_copy(i):
        return remote(tsend.at[i], trecv.at[i], t_s, t_r, i, partner)

    def part_copy(i):
        return remote(psend.at[i], precv.at[i], p_s, p_r, i, peer)

    def mine(j):
        return block(base(hs + j), core)

    def theirs(j):
        return block(base(j), core)

    def final_copy(j):
        r = mine(j)
        return remote(dx.at[r], dx.at[r], f_s, f_r, j, peer)

    def own_copy(j):
        r = mine(j)
        return remote(dx.at[r], dx.at[r], o_s, o_r, j, partner)

    def pass_copy(j):
        r = theirs(j)
        return remote(dx.at[r], dx.at[r], w_s, w_r, j, partner)

    wd_copy = pltpu.make_async_copy(wd_h, wd, load_sem.at[0])
    wg_copy = pltpu.make_async_copy(wg_h, wgu.at[:, 0:f], load_sem.at[1])
    wu_copy = pltpu.make_async_copy(wu_h, wgu.at[:, f : 2 * f], load_sem.at[2])
    x_copy = pltpu.make_async_copy(x_h, xv, load_sem.at[3])

    wd_copy.start()
    for c in load(0):
        c.start()
    wg_copy.start()
    wu_copy.start()
    for i in (1, 2):
        for c in load(i):
            c.start()

    barrier = pltpu.get_barrier_semaphore()
    for to in (partner, peer):
        pl.semaphore_signal(barrier, inc=1, device_id={"tp": to}, device_id_type=MESH)
    pl.semaphore_wait(barrier, 2)

    def hidden_part(i):
        for c in load(i):
            c.wait()

        @pl.when(i + 3 < steps)
        def _():
            for c in load(i + 3):
                c.start()

        b = base(i)
        other, mine_ = block(b, 1 - core), block(b, core)
        dyb = jnp.concatenate([dyv[other, :], dyv[mine_, :]], axis=0)
        for n in range(f // 256):
            cols = slice(n * 256, (n + 1) * 256)
            dh = dot_t(dyb, wd[cols, :])
            for part, r in ((dh[:R], other), (dh[R:], mine_)):
                g, u = gv[r, cols].astype(F32), uv[r, cols].astype(F32)
                sig = jax.nn.sigmoid(g)
                act = g * sig
                hid[r, cols] = (act * u).astype(BF16)
                dgu[r, cols] = ((part * u) * (sig * (1.0 + g * (1.0 - sig)))).astype(BF16)
                dgu[r, f + n * 256 : f + (n + 1) * 256] = (part * act).astype(BF16)

    def term_part(i):
        b = base(i)
        other, mine_ = block(b, 1 - core), block(b, core)
        lhs = jnp.concatenate([dgu[other, :], dgu[mine_, :]], axis=0)
        for n in range(d // 256):
            cols = slice(n * 256, (n + 1) * 256)
            t = dot_t(lhs, wgu[cols, :])
            tsend[i, :, cols] = t[:R].astype(BF16)
            own[i, :, cols] = t[R:]
        term_copy(i).start()

    def chip_sum(i):
        term_copy(i).wait_recv()
        s = own[i] + trecv[i].astype(F32)

        @pl.when(i < hs)
        def _():
            psend[i] = s.astype(BF16)
            part_copy(i).start()

        @pl.when(i >= hs)
        def _():
            own[i] = s

    wd_copy.wait()
    hidden_part(0)
    wg_copy.wait()
    wu_copy.wait()
    x_copy.start()
    term_part(0)

    @pl.loop(1, steps)
    def _(i):
        hidden_part(i)
        chip_sum(i - 1)
        term_part(i)

    chip_sum(steps - 1)

    def finish(j):
        part_copy(j).wait_recv()
        dx[mine(j), :] = (own[hs + j] + precv[j].astype(F32)).astype(BF16)
        final_copy(j).start()
        own_copy(j).start()

    def pass_on(j):
        final_copy(j).wait_recv()
        pass_copy(j).start()

    x_copy.wait()

    @pl.loop(0, d // 256)
    def _(m):
        r = pl.ds(pl.multiple_of(m * 256, 256), 256)
        xt[...] = xv[:, r].T
        for n in range(f // 256):
            cols = slice(n * 256, (n + 1) * 256)
            dwg[r, cols] = dot(xt[...], dgu[:, cols]).astype(BF16)
            dwu[r, cols] = dot(xt[...], dgu[:, f + n * 256 : f + (n + 1) * 256]).astype(BF16)
        finish(m)

    @pl.loop(0, f // 256)
    def _(m):
        r = pl.ds(pl.multiple_of(m * 256, 256), 256)
        xt[...] = hid[:, r].T
        for n in range(d // 256):
            cols = slice(n * 256, (n + 1) * 256)
            dwd[r, cols] = dot(xt[...], dyv[:, cols]).astype(BF16)
        finish(d // 256 + m)

    @pl.loop(d // 256 + f // 256, hs)
    def _(j):
        finish(j)

    @pl.loop(0, hs)
    def _(j):
        pass_on(j)

    @pl.loop(0, hs)
    def _(j):
        own_copy(j).wait_recv()
        pass_copy(j).wait_recv()
        part_copy(j).wait_send()
        final_copy(j).wait_send()
        own_copy(j).wait_send()
        pass_copy(j).wait_send()

    @pl.loop(0, steps)
    def _(i):
        term_copy(i).wait_send()


def flush(dx_v, dwg_v, dwu_v, dwd_v, dx, dwg, dwu, dwd, sem):
    copies = []
    for src, dst in ((dx_v, dx), (dwg_v, dwg), (dwu_v, dwu), (dwd_v, dwd)):
        rows = src.shape[0]
        for n in range(2):
            r = pl.ds(n * (rows // 2), rows // 2)
            copies.append(pltpu.make_async_copy(src.at[r], dst.at[r], sem.at[len(copies)]))
    for c in copies:
        c.start()
    for c in copies:
        c.wait()


def solution(mesh):
    def step(x, dy, gate, up, w_gate, w_up, w_down):
        rows, d = x.shape
        f = gate.shape[1]
        steps = rows // (2 * R)
        hs = steps // 2
        outs = [((rows, d), BF16), ((d, f), BF16), ((d, f), BF16), ((f, d), BF16)]
        dma = pltpu.SemaphoreType.DMA
        held = pl.pallas_call(
            kernel,
            out_shape=[pltpu.VMEM(s, t) for s, t in outs],
            in_specs=[pl.BlockSpec(memory_space=pl.ANY)] * 7,
            out_specs=[pl.BlockSpec(memory_space=pltpu.VMEM)] * 4,
            scratch_shapes=[
                pltpu.VMEM((rows, d), BF16),
                pltpu.VMEM((rows, d), BF16),
                pltpu.VMEM((rows, f), BF16),
                pltpu.VMEM((rows, f), BF16),
                pltpu.VMEM((d, 2 * f), BF16),
                pltpu.VMEM((f, d), BF16),
                pltpu.VMEM((rows, 2 * f), BF16),
                pltpu.VMEM((rows, f), BF16),
                pltpu.VMEM((256, rows), BF16),
                pltpu.VMEM((steps, R, d), F32),
                pltpu.VMEM((steps, R, d), BF16),
                pltpu.VMEM((steps, R, d), BF16),
                pltpu.VMEM((hs, R, d), BF16),
                pltpu.VMEM((hs, R, d), BF16),
                dma((4,)),
                dma((steps, 3)),
                dma((steps,)),
                dma((steps,)),
            ]
            + [dma((hs,))] * 8,
            compiler_params=pltpu.CompilerParams(
                collective_id=0, has_side_effects=True, vmem_limit_bytes=50 * 2**20
            ),
            name="block",
        )(x, dy, gate, up, w_gate, w_up, w_down)
        return pl.pallas_call(
            flush,
            out_shape=[jax.ShapeDtypeStruct(s, t) for s, t in outs],
            in_specs=[pl.BlockSpec(memory_space=pltpu.VMEM)] * 4,
            out_specs=[pl.BlockSpec(memory_space=pl.ANY)] * 4,
            scratch_shapes=[dma((8,))],
            compiler_params=pltpu.CompilerParams(vmem_limit_bytes=2**20),
            name="flush",
        )(*(pltpu.with_memory_space_constraint(h, pltpu.VMEM) for h in held))

    tokens, columns, rows = P("dp", None), P(None, "tp"), P("tp", None)
    return jax.shard_map(
        step,
        mesh=mesh,
        in_specs=(tokens, tokens, P("dp", "tp"), P("dp", "tp"), columns, columns, rows),
        out_specs=(tokens, P("dp", "tp"), P("dp", "tp"), P(("dp", "tp"), None)),
        check_vma=False,
    )
```

```python
import types

import jax
import jax.numpy as jnp
from jax import lax
from jax.experimental import pallas as pl
from jax.experimental.pallas import tpu as pltpu
from jax.sharding import PartitionSpec as P

MESH = pl.DeviceIdType.MESH
F32, BF16 = jnp.float32, jnp.bfloat16
scope = jax.named_scope
C = 256
SMALL, RS, RB = 2, 64, 128


def dot_t(a, b):
    return lax.dot_general(a, b, (((1,), (1,)), ((), ())), preferred_element_type=F32)


def dot(a, b):
    return lax.dot_general(a, b, (((1,), (0,)), ((), ())), preferred_element_type=F32)


def tile(n, start=0):
    return slice(start + n * C, start + (n + 1) * C)


def kernel(
    x_h, dy_h, gate_h, up_h, wg_h, wu_h, wd_h,
    dx, dwg, dwu, dwd,
    xv, dyv, gv, uv, wgu, wd, dgu, hid, xt,
    own_s, tsend_s, trecv_s, psend_s, precv_s, own_b, tsend_b, trecv_b, psend_b, precv_b,
    wd_sem, wgu_sem, x_sem, sem_s, sem_b, first, load_s, load_b,
):
    rows, d = dyv.shape
    f = wd.shape[0]
    half = rows // 2
    me = lax.axis_index("tp")
    chip, core = me // 2, me % 2
    partner, peer = chip * 2 + (1 - core), (1 - chip) * 2 + core
    nb = (half - SMALL * 2 * RS) // (2 * RB)
    small = types.SimpleNamespace(
        r=RS, off=0, n=SMALL, own=own_s, tsend=tsend_s, trecv=trecv_s, psend=psend_s, precv=precv_s, sem=sem_s, load=load_s
    )
    big = types.SimpleNamespace(
        r=RB, off=SMALL * 2 * RS, n=nb, own=own_b, tsend=tsend_b, trecv=trecv_b, psend=psend_b, precv=precv_b, sem=sem_b, load=load_b
    )

    def base(q, e):
        owner = lax.rem(chip + 1 + e // q.n, 2)
        return pl.multiple_of(owner * half + q.off + lax.rem(e, q.n) * (2 * q.r), 2 * RS)

    def block(q, e, k):
        return pl.ds(pl.multiple_of(base(q, e) + k * q.r, RS), q.r)

    def load(q, e):
        r = pl.ds(base(q, e), 2 * q.r)
        return [
            pltpu.make_async_copy(src.at[r], dst.at[r], q.load.at[e, n])
            for n, (src, dst) in enumerate(((dy_h, dyv), (gate_h, gv), (up_h, uv)))
        ]

    def remote(src, dst, send, recv, to):
        return pltpu.make_async_remote_copy(
            src_ref=src, dst_ref=dst, send_sem=send, recv_sem=recv, device_id={"tp": to}, device_id_type=MESH
        )

    def term_copy(q, e):
        return remote(q.tsend.at[e], q.trecv.at[e], q.sem.at[0, e], q.sem.at[1, e], partner)

    def part_copy(q, e):
        return remote(q.psend.at[e], q.precv.at[e], q.sem.at[2, e], q.sem.at[3, e], peer)

    def term_piece(n):
        return remote(tsend_s.at[0, :, tile(n)], trecv_s.at[0, :, tile(n)], first.at[0, n], first.at[1, n], partner)

    def part_piece(n):
        return remote(psend_s.at[0, :, tile(n)], precv_s.at[0, :, tile(n)], first.at[2, n], first.at[3, n], peer)

    def final_copy(q, j):
        r = block(q, q.n + j, core)
        return remote(dx.at[r], dx.at[r], q.sem.at[4, j], q.sem.at[5, j], peer)

    def own_copy(q, j):
        r = block(q, q.n + j, core)
        return remote(dx.at[r], dx.at[r], q.sem.at[6, j], q.sem.at[7, j], partner)

    def pass_copy(q, j):
        r = block(q, j, core)
        return remote(dx.at[r], dx.at[r], q.sem.at[8, j], q.sem.at[9, j], partner)

    def wd_copy(n):
        return pltpu.make_async_copy(wd_h.at[tile(n)], wd.at[tile(n)], wd_sem.at[n])

    def wgu_copy(n):
        return [
            pltpu.make_async_copy(w.at[tile(n)], wgu.at[tile(n), c * f : (c + 1) * f], wgu_sem.at[n, c])
            for c, w in enumerate((wg_h, wu_h))
        ]

    x_copy = pltpu.make_async_copy(x_h, xv, x_sem)

    def start(copies):
        for c in copies:
            c.start()

    def wait(copies):
        for c in copies:
            c.wait()

    @scope("hidden_tile")
    def hidden_tile(q, e, n, dyb):
        dh = dot_t(dyb, wd[tile(n), :])
        for part, k in ((dh[: q.r], 1 - core), (dh[q.r :], core)):
            r = block(q, e, k)
            g, u = gv[r, tile(n)].astype(F32), uv[r, tile(n)].astype(F32)
            sig = jax.nn.sigmoid(g)
            act = g * sig
            hid[r, tile(n)] = (act * u).astype(BF16)
            dgu[r, tile(n)] = ((part * u) * (sig + act * (1.0 - sig))).astype(BF16)
            dgu[r, tile(n, f)] = (part * act).astype(BF16)

    def both(ref, q, e):
        return jnp.concatenate([ref[block(q, e, 1 - core), :], ref[block(q, e, core), :]], axis=0)

    @scope("hidden_part")
    def hidden_part(q, e):
        with scope("w_load"):
            wait(load(q, e))
        dyb = both(dyv, q, e)
        for n in range(f // C):
            hidden_tile(q, e, n, dyb)

    @scope("term_tile")
    def term_tile(q, e, n, lhs):
        t = dot_t(lhs, wgu[tile(n), :])
        q.tsend[e, :, tile(n)] = t[: q.r].astype(BF16)
        q.own[e, :, tile(n)] = t[q.r :]

    @scope("term_part")
    def term_part(q, e):
        lhs = both(dgu, q, e)
        for n in range(d // C):
            term_tile(q, e, n, lhs)
        term_copy(q, e).start()

    @scope("chip_sum")
    def chip_sum(q, e, theirs):
        with scope("w_term"):
            term_copy(q, e).wait_recv()
        s = q.own[e] + q.trecv[e].astype(F32)
        if theirs:
            q.psend[e] = s.astype(BF16)
            part_copy(q, e).start()
        else:
            q.own[e] = s

    @scope("first_sum")
    def first_sum(n):
        with scope("w_term"):
            term_piece(n).wait_recv()
        psend_s[0, :, tile(n)] = (own_s[0, :, tile(n)] + trecv_s[0, :, tile(n)].astype(F32)).astype(BF16)
        part_piece(n).start()

    @scope("finish")
    def finish(q, j):
        if q is small and j == 0:
            for n in range(d // C):
                part_piece(n).wait_recv()
        else:
            with scope("w_part"):
                part_copy(q, j).wait_recv()
        dx[block(q, q.n + j, core), :] = (q.own[q.n + j] + q.precv[j].astype(F32)).astype(BF16)
        final_copy(q, j).start()
        own_copy(q, j).start()

    @scope("pass_on")
    def pass_on(q, j):
        with scope("w_final"):
            final_copy(q, j).wait_recv()
        pass_copy(q, j).start()

    @scope("grad_x")
    def grad_x(m):
        r = pl.ds(pl.multiple_of(m * C, C), C)
        xt[...] = xv[:, r].T
        for n in range(f // C):
            dwg[r, tile(n)] = dot(xt[...], dgu[:, tile(n)]).astype(BF16)
            dwu[r, tile(n)] = dot(xt[...], dgu[:, tile(n, f)]).astype(BF16)

    @scope("grad_h")
    def grad_h(m):
        r = pl.ds(pl.multiple_of(m * C, C), C)
        xt[...] = hid[:, r].T
        for n in range(d // C):
            dwd[r, tile(n)] = dot(xt[...], dyv[:, tile(n)]).astype(BF16)

    wd_copy(0).start()
    start(load(small, 0))
    for n in range(1, f // C):
        wd_copy(n).start()
    for n in range(d // C):
        start(wgu_copy(n))
    start(load(small, 1))

    barrier = pltpu.get_barrier_semaphore()
    for to in (partner, peer):
        pl.semaphore_signal(barrier, inc=1, device_id={"tp": to}, device_id_type=MESH)

    with scope("w_load"):
        wait(load(small, 0))
    dyb = both(dyv, small, 0)
    for n in range(f // C):
        with scope("w_wd"):
            wd_copy(n).wait()
        hidden_tile(small, 0, n, dyb)
    with scope("barrier"):
        pl.semaphore_wait(barrier, 2)
    lhs = both(dgu, small, 0)
    for n in range(d // C):
        with scope("w_wgu"):
            wait(wgu_copy(n))
        term_tile(small, 0, n, lhs)
        term_piece(n).start()
    for e in range(2 * nb):
        start(load(big, e))
    for e in range(SMALL, 2 * SMALL):
        start(load(small, e))
    x_copy.start()
    first_sum(0)
    first_sum(1)
    hidden_part(small, 1)
    first_sum(2)
    first_sum(3)
    term_part(small, 1)

    @pl.loop(0, 2 * nb)
    def _(e):
        hidden_part(big, e)

        @pl.when(e == 0)
        def _():
            chip_sum(small, 1, True)

        @pl.when((e > 0) & (e <= nb))
        def _():
            chip_sum(big, e - 1, True)

        @pl.when(e > nb)
        def _():
            chip_sum(big, e - 1, False)

        term_part(big, e)

    for e in range(SMALL, 2 * SMALL):
        hidden_part(small, e)
        if e == SMALL:
            chip_sum(big, 2 * nb - 1, False)
        else:
            chip_sum(small, e - 1, False)
        term_part(small, e)

    x_copy.wait()
    finish(big, 0)
    chip_sum(small, 2 * SMALL - 1, False)

    @pl.loop(0, d // C)
    def _(m):
        grad_x(m)

        @pl.when(m == 1)
        def _():
            finish(big, 1)

    finish(big, 2)

    @pl.loop(0, f // C)
    def _(m):
        grad_h(m)

    for j in range(SMALL):
        finish(small, j)

    for j in range(nb):
        pass_on(big, j)
    for j in range(SMALL):
        pass_on(small, j)

    with scope("drain"):
        for q in (big, small):
            for j in range(q.n):
                own_copy(q, j).wait_recv()
                if q is small and j == 0:
                    for n in range(d // C):
                        term_piece(n).wait_send()
                        part_piece(n).wait_send()
                else:
                    term_copy(q, j).wait_send()
                    part_copy(q, j).wait_send()
                term_copy(q, q.n + j).wait_send()
                final_copy(q, j).wait_send()
                own_copy(q, j).wait_send()
                pass_copy(q, j).wait_send()
                pass_copy(q, j).wait_recv()


FLUSH = 4


def flush(*refs):
    half = len(refs) // 2
    srcs, dsts, sem = refs[:half], refs[half:-1], refs[-1]
    copies = []
    for src, dst in zip(srcs, dsts):
        rows = src.shape[0] // FLUSH
        for n in range(FLUSH):
            r = pl.ds(n * rows, rows)
            copies.append(pltpu.make_async_copy(src.at[r], dst.at[r], sem.at[len(copies)]))
    for c in copies:
        c.start()
    for c in copies:
        c.wait()


def solution(mesh):
    def step(x, dy, gate, up, w_gate, w_up, w_down):
        rows, d = x.shape
        f = gate.shape[1]
        nb = (rows // 2 - SMALL * 2 * RS) // (2 * RB)
        outs = [((rows, d), BF16), ((d, f), BF16), ((d, f), BF16), ((f, d), BF16)]
        dma = pltpu.SemaphoreType.DMA

        def buffers(n, r):
            shapes = ((2 * n, F32), (2 * n, BF16), (2 * n, BF16), (n, BF16), (n, BF16))
            return [pltpu.VMEM((m, r, d), t) for m, t in shapes]

        held = pl.pallas_call(
            kernel,
            out_shape=[pltpu.VMEM(s, t) for s, t in outs],
            in_specs=[pl.BlockSpec(memory_space=pl.ANY)] * 7,
            out_specs=[pl.BlockSpec(memory_space=pltpu.VMEM)] * 4,
            scratch_shapes=[
                pltpu.VMEM((rows, d), BF16),
                pltpu.VMEM((rows, d), BF16),
                pltpu.VMEM((rows, f), BF16),
                pltpu.VMEM((rows, f), BF16),
                pltpu.VMEM((d, 2 * f), BF16),
                pltpu.VMEM((f, d), BF16),
                pltpu.VMEM((rows, 2 * f), BF16),
                pltpu.VMEM((rows, f), BF16),
                pltpu.VMEM((C, rows), BF16),
            ]
            + buffers(SMALL, RS)
            + buffers(nb, RB)
            + [
                dma((f // C,)),
                dma((d // C, 2)),
                dma(()),
                dma((10, 2 * SMALL)),
                dma((10, 2 * nb)),
                dma((4, d // C)),
                dma((2 * SMALL, 3)),
                dma((2 * nb, 3)),
            ],
            compiler_params=pltpu.CompilerParams(
                collective_id=0, has_side_effects=True, vmem_limit_bytes=50 * 2**20
            ),
            name="block",
        )(x, dy, gate, up, w_gate, w_up, w_down)
        return pl.pallas_call(
            flush,
            out_shape=[jax.ShapeDtypeStruct(s, t) for s, t in outs],
            in_specs=[pl.BlockSpec(memory_space=pltpu.VMEM)] * 4,
            out_specs=[pl.BlockSpec(memory_space=pl.ANY)] * 4,
            scratch_shapes=[dma((4 * FLUSH,))],
            compiler_params=pltpu.CompilerParams(vmem_limit_bytes=2**20),
            name="flush",
        )(*(pltpu.with_memory_space_constraint(h, pltpu.VMEM) for h in held))

    tokens, columns, rows = P("dp", None), P(None, "tp"), P("tp", None)
    return jax.shard_map(
        step,
        mesh=mesh,
        in_specs=(tokens, tokens, P("dp", "tp"), P("dp", "tp"), columns, columns, rows),
        out_specs=(tokens, P("dp", "tp"), P("dp", "tp"), P(("dp", "tp"), None)),
        check_vma=False,
    )
```

```python
import types

import jax
import jax.numpy as jnp
from jax import lax
from jax.experimental import pallas as pl
from jax.experimental.pallas import tpu as pltpu
from jax.sharding import PartitionSpec as P

MESH = pl.DeviceIdType.MESH
F32, BF16 = jnp.float32, jnp.bfloat16
scope = jax.named_scope
C = 256
SMALL, RS, RB = 2, 64, 128
LAST = 4


def dot_t(a, b):
    return lax.dot_general(a, b, (((1,), (1,)), ((), ())), preferred_element_type=F32)


def dot(a, b):
    return lax.dot_general(a, b, (((1,), (0,)), ((), ())), preferred_element_type=F32)


def tile(n, start=0):
    return slice(start + n * C, start + (n + 1) * C)


def kernel(
    x_h, dy_h, gate_h, up_h, wg_h, wu_h, wd_h,
    dx, dwg, dwu, dwd,
    xv, acts, wgu, wd, dgu, hid, xt,
    own_s, tsend_s, trecv_s, psend_s, precv_s, own_b, tsend_b, trecv_b, psend_b, precv_b,
    load_sem, sent, landed, term_sem, part_sem, final_sem,
):
    rows, d = xv.shape
    f = wd.shape[0]
    half = rows // 2
    dyv, gv, uv = acts.at[:, 0:d], acts.at[:, d : d + f], acts.at[:, d + f : d + 2 * f]
    me = lax.axis_index("tp")
    chip, core = me // 2, me % 2
    partner, peer = chip * 2 + (1 - core), (1 - chip) * 2 + core
    nb = (half - SMALL * 2 * RS) // (2 * RB)
    small = types.SimpleNamespace(
        r=RS, off=0, n=SMALL, at=0, own=own_s, tsend=tsend_s, trecv=trecv_s, psend=psend_s, precv=precv_s
    )
    big = types.SimpleNamespace(
        r=RB, off=SMALL * 2 * RS, n=nb, at=SMALL, own=own_b, tsend=tsend_b, trecv=trecv_b, psend=psend_b, precv=precv_b
    )

    def base(q, e):
        owner = lax.rem(chip + 1 + e // q.n, 2)
        return pl.multiple_of(owner * half + q.off + lax.rem(e, q.n) * (2 * q.r), 2 * RS)

    def block(q, e, k):
        return pl.ds(pl.multiple_of(base(q, e) + k * q.r, RS), q.r)

    def local(src, dst, sem):
        return pltpu.make_async_copy(src, dst, load_sem.at[sem])

    def load(q, e, sem):
        r = pl.ds(base(q, e), 2 * q.r)
        return [local(src.at[r], dst.at[r], sem) for src, dst in ((dy_h, dyv), (gate_h, gv), (up_h, uv))]

    def all_of(ref, sem):
        return pltpu.make_async_copy(ref, ref, sem)

    def remote(src, dst, send, recv, to):
        return pltpu.make_async_remote_copy(
            src_ref=src, dst_ref=dst, send_sem=send, recv_sem=recv, device_id={"tp": to}, device_id_type=MESH
        )

    def term_copy(q, e, cols=slice(None), sem=None):
        recv = term_sem.at[2 * q.at + e if sem is None else sem]
        return remote(q.tsend.at[e, :, cols], q.trecv.at[e, :, cols], sent.at[0], recv, partner)

    def part_copy(q, e, cols=slice(None)):
        return remote(q.psend.at[e, :, cols], q.precv.at[e, :, cols], sent.at[1], part_sem.at[q.at + e], peer)

    def final_copy(q, j, n=0, pieces=1):
        size = q.r // pieces
        r = pl.ds(pl.multiple_of(base(q, q.n + j) + core * q.r + n * size, size), size)
        return remote(dx.at[r], dx.at[r], sent.at[2], final_sem.at[(nb if q is small else 0) + j + n], peer)

    def core_copy(r):
        return remote(dx.at[r], dx.at[r], sent.at[3], landed, partner)

    def start(copies, priority=0):
        for c in copies:
            c.start()

    def hidden_tile(q, e, n, dyb):
        dh = dot_t(dyb, wd[tile(n), :])
        for part, k in ((dh[: q.r], 1 - core), (dh[q.r :], core)):
            r = block(q, e, k)
            g, u = gv[r, tile(n)].astype(F32), uv[r, tile(n)].astype(F32)
            sig = jax.nn.sigmoid(g)
            act = g * sig
            hid[r, tile(n)] = (act * u).astype(BF16)
            dgu[r, tile(n)] = ((part * u) * (sig + act * (1.0 - sig))).astype(BF16)
            dgu[r, tile(n, f)] = (part * act).astype(BF16)

    def both(ref, q, e):
        return jnp.concatenate([ref[block(q, e, 1 - core), :], ref[block(q, e, core), :]], axis=0)

    @scope("hidden_part")
    def hidden_part(q, e):
        dyb = both(dyv, q, e)
        for n in range(f // C):
            hidden_tile(q, e, n, dyb)

    @scope("term_tile")
    def term_tile(q, e, n, lhs, split=False):
        w = wgu.at[tile(n), :]
        if split:
            t = dot_t(lhs[:, :f], w[:, :f]) + dot_t(lhs[:, f:], w[:, f:])
        else:
            t = dot_t(lhs, w[...])
        q.tsend[e, :, tile(n)] = t[: q.r].astype(BF16)
        q.own[e, :, tile(n)] = t[q.r :]

    @scope("term_part")
    def term_part(q, e):
        lhs = both(dgu, q, e)
        for n in range(d // C):
            term_tile(q, e, n, lhs)
        term_copy(q, e).start()

    @scope("chip_sum")
    def chip_sum(q, e, theirs, cols=slice(None), sem=None):
        with scope("w_term"):
            term_copy(q, e, cols, sem).wait_recv()
        s = q.own[e, :, cols] + q.trecv[e, :, cols].astype(F32)
        if theirs:
            q.psend[e, :, cols] = s.astype(BF16)
            part_copy(q, e, cols).start()
        else:
            q.own[e, :, cols] = s

    @scope("finish")
    def finish(q, j):
        with scope("w_part"):
            part_copy(q, j).wait_recv()
        r = block(q, q.n + j, core)
        dx[r, :] = (q.own[q.n + j] + q.precv[j].astype(F32)).astype(BF16)
        pieces = LAST if q is small and j == SMALL - 1 else 1
        for n in range(pieces):
            final_copy(q, j, n, pieces).start()
        core_copy(r).start()

    @scope("pass_on")
    def pass_on(q, j):
        pieces = LAST if q is small and j == SMALL - 1 else 1
        for n in range(pieces):
            with scope("w_final"):
                final_copy(q, j, n, pieces).wait_recv()
            size = q.r // pieces
            core_copy(pl.ds(pl.multiple_of(base(q, j) + core * q.r + n * size, size), size)).start()

    @scope("grad_x")
    def grad_x(m):
        r = pl.ds(pl.multiple_of(m * C, C), C)
        xt[...] = xv[:, r].T
        for n in range(f // C):
            dwg[r, tile(n)] = dot(xt[...], dgu[:, tile(n)]).astype(BF16)
            dwu[r, tile(n)] = dot(xt[...], dgu[:, tile(n, f)]).astype(BF16)

    @scope("grad_h")
    def grad_h(m):
        r = pl.ds(pl.multiple_of(m * C, C), C)
        xt[...] = hid[:, r].T
        for n in range(d // C):
            dwd[r, tile(n)] = dot(xt[...], dyv[:, tile(n)]).astype(BF16)

    nf, nd = f // C, d // C
    first_rows, gu, second_rows, rest, x_sem = nf, nf + 1, nf + 1 + nd, nf + 2 + nd, nf + 3 + nd
    first = load(small, 0, first_rows)
    wds = [local(wd_h.at[tile(n)], wd.at[tile(n)], n) for n in range(nf)]
    start(first[:1] + wds[:1] + first[1:] + wds[1:])
    for n in range(nd):
        start([local(w.at[tile(n)], wgu.at[tile(n), c * f : (c + 1) * f], gu + n) for c, w in enumerate((wg_h, wu_h))], 1)
    start(load(small, 1, second_rows), 1)
    for e in range(2 * nb):
        start(load(big, e, rest), 1)
    for e in range(SMALL, 2 * SMALL):
        start(load(small, e, rest), 1)
    x_copy = local(x_h, xv, x_sem)
    start([x_copy], 1)

    barrier = pltpu.get_barrier_semaphore()
    for to in (partner, peer):
        pl.semaphore_signal(barrier, inc=1, device_id={"tp": to}, device_id_type=MESH)

    with scope("w_first"):
        all_of(acts.at[pl.ds(base(small, 0), 2 * RS)], load_sem.at[first_rows]).wait()
    with scope("w_wd"):
        for c in wds:
            c.wait()
    hidden_part(small, 0)
    with scope("barrier"):
        pl.semaphore_wait(barrier, 2)
    lhs = both(dgu, small, 0)
    spare = 2 * (SMALL + nb)
    for n in range(nd):
        with scope("w_wgu"):
            all_of(wgu.at[tile(n)], load_sem.at[gu + n]).wait()
        term_tile(small, 0, n, lhs, split=True)
        term_copy(small, 0, tile(n), spare + n).start()
    chip_sum(small, 0, True, tile(0), spare)
    with scope("w_second"):
        all_of(acts.at[pl.ds(base(small, 1), 2 * RS)], load_sem.at[second_rows]).wait()
    hidden_part(small, 1)
    for n in range(1, nd):
        chip_sum(small, 0, True, tile(n), spare + n)
    lhs = both(dgu, small, 1)
    for n in range(2):
        for m in range(nd // 2):
            term_tile(small, 1, n * (nd // 2) + m, lhs)
        term_copy(small, 1, slice(n * (d // 2), (n + 1) * (d // 2)), n).start()
    with scope("w_rest"):
        all_of(acts.at[0 : rows - SMALL * 2 * RS], load_sem.at[rest]).wait()

    @pl.loop(0, 2 * nb)
    def _(e):
        hidden_part(big, e)

        @pl.when(e == 0)
        def _():
            for n in range(2):
                chip_sum(small, 1, True, slice(n * (d // 2), (n + 1) * (d // 2)), n)

        @pl.when((e > 0) & (e <= nb))
        def _():
            chip_sum(big, e - 1, True)

        @pl.when(e > nb)
        def _():
            chip_sum(big, e - 1, False)

        term_part(big, e)

    for e in range(SMALL, 2 * SMALL):
        hidden_part(small, e)
        if e == SMALL:
            chip_sum(big, 2 * nb - 1, False)
        else:
            chip_sum(small, e - 1, False)
        term_part(small, e)

    with scope("w_x"):
        x_copy.wait()
    finish(big, 0)
    chip_sum(small, 2 * SMALL - 1, False)

    @pl.loop(0, d // C)
    def _(m):
        grad_x(m)

        @pl.when(m == 1)
        def _():
            finish(big, 1)

    finish(big, 2)

    @pl.loop(0, f // C)
    def _(m):
        grad_h(m)

    for j in range(SMALL):
        finish(small, j)

    for j in range(nb):
        pass_on(big, j)
    for j in range(SMALL):
        pass_on(small, j)

    with scope("drain"):
        all_of(dx.at[0:half], sent.at[0]).wait()
    with scope("drain"):
        all_of(dx.at[0 : half // 2], sent.at[1]).wait()
    with scope("drain"):
        all_of(dx.at[0 : half // 2], sent.at[2]).wait()
    with scope("drain"):
        all_of(dx.at[0:half], sent.at[3]).wait()
    with scope("drain"):
        all_of(dx.at[0:half], landed).wait()


def flush(*refs):
    half = len(refs) // 2
    copies = []
    for src, dst in zip(refs[:half], refs[half:-1]):
        rows = src.shape[0] // 2
        for n in range(2):
            r = pl.ds(n * rows, rows)
            copies.append(pltpu.make_async_copy(src.at[r], dst.at[r], refs[-1]))
    for c in copies:
        c.start()
    for c in copies:
        c.wait()


def solution(mesh):
    def step(x, dy, gate, up, w_gate, w_up, w_down):
        rows, d = x.shape
        f = gate.shape[1]
        nb = (rows // 2 - SMALL * 2 * RS) // (2 * RB)
        outs = [((rows, d), BF16), ((d, f), BF16), ((d, f), BF16), ((f, d), BF16)]
        dma = pltpu.SemaphoreType.DMA

        def buffers(n, r):
            shapes = ((2 * n, F32), (2 * n, BF16), (2 * n, BF16), (n, BF16), (n, BF16))
            return [pltpu.VMEM((m, r, d), t) for m, t in shapes]

        held = pl.pallas_call(
            kernel,
            out_shape=[pltpu.VMEM(s, t) for s, t in outs],
            in_specs=[pl.BlockSpec(memory_space=pl.ANY)] * 7,
            out_specs=[pl.BlockSpec(memory_space=pltpu.VMEM)] * 4,
            scratch_shapes=[
                pltpu.VMEM((rows, d), BF16),
                pltpu.VMEM((rows, d + 2 * f), BF16),
                pltpu.VMEM((d, 2 * f), BF16),
                pltpu.VMEM((f, d), BF16),
                pltpu.VMEM((rows, 2 * f), BF16),
                pltpu.VMEM((rows, f), BF16),
                pltpu.VMEM((C, rows), BF16),
            ]
            + buffers(SMALL, RS)
            + buffers(nb, RB)
            + [
                dma((f // C + d // C + 4,)),
                dma((4,)),
                dma(()),
                dma((2 * (SMALL + nb) + d // C,)),
                dma((SMALL + nb,)),
                dma((SMALL + nb + LAST - 1,)),
            ],
            compiler_params=pltpu.CompilerParams(
                collective_id=0, has_side_effects=True, vmem_limit_bytes=50 * 2**20
            ),
            name="block",
        )(x, dy, gate, up, w_gate, w_up, w_down)
        return pl.pallas_call(
            flush,
            out_shape=[jax.ShapeDtypeStruct(s, t) for s, t in outs],
            in_specs=[pl.BlockSpec(memory_space=pltpu.VMEM)] * 4,
            out_specs=[pl.BlockSpec(memory_space=pl.ANY)] * 4,
            scratch_shapes=[dma(())],
            compiler_params=pltpu.CompilerParams(vmem_limit_bytes=2**20),
            name="flush",
        )(*(pltpu.with_memory_space_constraint(h, pltpu.VMEM) for h in held))

    tokens, columns, rows = P("dp", None), P(None, "tp"), P("tp", None)
    return jax.shard_map(
        step,
        mesh=mesh,
        in_specs=(tokens, tokens, P("dp", "tp"), P("dp", "tp"), columns, columns, rows),
        out_specs=(tokens, P("dp", "tp"), P("dp", "tp"), P(("dp", "tp"), None)),
        check_vma=False,
    )
```

```python
import types

import jax
import jax.numpy as jnp
from jax import lax
from jax.experimental import pallas as pl
from jax.experimental.pallas import tpu as pltpu
from jax.sharding import PartitionSpec as P

MESH = pl.DeviceIdType.MESH
F32, BF16 = jnp.float32, jnp.bfloat16
scope = jax.named_scope
C = 256
SMALL, RS, RB = 2, 64, 128
EARLY, AHEAD, LAST = 1, 2, 4


def dot_t(a, b):
    return lax.dot_general(a, b, (((1,), (1,)), ((), ())), preferred_element_type=F32)


def dot(a, b):
    return lax.dot_general(a, b, (((1,), (0,)), ((), ())), preferred_element_type=F32)


def tile(n, start=0):
    return slice(start + n * C, start + (n + 1) * C)


def kernel(
    x_h, dy_h, gate_h, up_h, wg_h, wu_h, wd_h,
    dx, dwg, dwu, dwd,
    xv, acts, wgu, wd, dgu, hid, xt,
    own_s, tsend_s, trecv_s, psend_s, precv_s, own_b, tsend_b, trecv_b, psend_b, precv_b,
    load_sem, sent, landed, term_sem, part_sem, final_sem,
):
    rows, d = xv.shape
    f = wd.shape[0]
    half = rows // 2
    dyv, gv, uv = acts.at[:, 0:d], acts.at[:, d : d + f], acts.at[:, d + f : d + 2 * f]
    me = lax.axis_index("tp")
    chip, core = me // 2, me % 2
    partner, peer = chip * 2 + (1 - core), (1 - chip) * 2 + core
    nb = (half - SMALL * 2 * RS) // (2 * RB)
    small = types.SimpleNamespace(
        r=RS, off=0, n=SMALL, at=0, own=own_s, tsend=tsend_s, trecv=trecv_s, psend=psend_s, precv=precv_s
    )
    big = types.SimpleNamespace(
        r=RB, off=SMALL * 2 * RS, n=nb, at=SMALL, own=own_b, tsend=tsend_b, trecv=trecv_b, psend=psend_b, precv=precv_b
    )

    def base(q, e):
        owner = lax.rem(chip + 1 + e // q.n, 2)
        return pl.multiple_of(owner * half + q.off + lax.rem(e, q.n) * (2 * q.r), 2 * RS)

    def block(q, e, k):
        return pl.ds(pl.multiple_of(base(q, e) + k * q.r, RS), q.r)

    def local(src, dst, sem):
        return pltpu.make_async_copy(src, dst, load_sem.at[sem])

    def load(q, e, sem):
        r = pl.ds(base(q, e), 2 * q.r)
        return [local(src.at[r], dst.at[r], sem) for src, dst in ((dy_h, dyv), (gate_h, gv), (up_h, uv))]

    def all_of(ref, sem):
        return pltpu.make_async_copy(ref, ref, sem)

    def remote(src, dst, send, recv, to):
        return pltpu.make_async_remote_copy(
            src_ref=src, dst_ref=dst, send_sem=send, recv_sem=recv, device_id={"tp": to}, device_id_type=MESH
        )

    def term_copy(q, e, cols=slice(None), sem=None):
        recv = term_sem.at[2 * q.at + e if sem is None else sem]
        return remote(q.tsend.at[e, :, cols], q.trecv.at[e, :, cols], sent.at[0], recv, partner)

    def part_copy(q, e, cols=slice(None)):
        return remote(q.psend.at[e, :, cols], q.precv.at[e, :, cols], sent.at[1], part_sem.at[q.at + e], peer)

    def final_copy(q, j):
        r = block(q, q.n + j, core)
        return remote(dx.at[r], dx.at[r], sent.at[2], final_sem.at[q.at + j], peer)

    def core_copy(r):
        return remote(dx.at[r], dx.at[r], sent.at[3], landed, partner)

    def start(copies):
        for c in copies:
            c.start()

    def hidden_tile(q, e, n, dyb):
        dh = dot_t(dyb, wd[tile(n), :])
        for part, k in ((dh[: q.r], 1 - core), (dh[q.r :], core)):
            r = block(q, e, k)
            g, u = gv[r, tile(n)].astype(F32), uv[r, tile(n)].astype(F32)
            sig = jax.nn.sigmoid(g)
            act = g * sig
            hid[r, tile(n)] = (act * u).astype(BF16)
            dgu[r, tile(n)] = ((part * u) * (sig + act * (1.0 - sig))).astype(BF16)
            dgu[r, tile(n, f)] = (part * act).astype(BF16)

    def both(ref, q, e):
        return jnp.concatenate([ref[block(q, e, 1 - core), :], ref[block(q, e, core), :]], axis=0)

    @scope("hidden_part")
    def hidden_part(q, e):
        dyb = both(dyv, q, e)
        for n in range(f // C):
            hidden_tile(q, e, n, dyb)

    @scope("term_tile")
    def term_tile(q, e, n, lhs):
        t = dot_t(lhs, wgu[tile(n), :])
        q.tsend[e, :, tile(n)] = t[: q.r].astype(BF16)
        q.own[e, :, tile(n)] = t[q.r :]

    @scope("term_part")
    def term_part(q, e):
        lhs = both(dgu, q, e)
        for n in range(d // C):
            term_tile(q, e, n, lhs)
        term_copy(q, e).start()

    @scope("chip_sum")
    def chip_sum(q, e, theirs, cols=slice(None), sem=None):
        with scope("w_term"):
            term_copy(q, e, cols, sem).wait_recv()
        s = q.own[e, :, cols] + q.trecv[e, :, cols].astype(F32)
        if theirs:
            q.psend[e, :, cols] = s.astype(BF16)
            part_copy(q, e, cols).start()
        else:
            q.own[e, :, cols] = s

    @scope("finish")
    def finish(q, j):
        with scope("w_part"):
            part_copy(q, j).wait_recv()
        r = block(q, q.n + j, core)
        dx[r, :] = (q.own[q.n + j] + q.precv[j].astype(F32)).astype(BF16)
        if q is big and j < AHEAD:
            final_copy(q, j).start()
        else:

            @pl.when(core != EARLY)
            def _():
                final_copy(q, j).start()

        core_copy(r).start()

    @scope("pass_on")
    def pass_on(q, j):
        with scope("w_final"):
            final_copy(q, j).wait_recv()
        core_copy(block(q, j, core)).start()

    @scope("grad_x")
    def grad_x(m):
        r = pl.ds(pl.multiple_of(m * C, C), C)
        xt[...] = xv[:, r].T
        for n in range(f // C):
            dwg[r, tile(n)] = dot(xt[...], dgu[:, tile(n)]).astype(BF16)
            dwu[r, tile(n)] = dot(xt[...], dgu[:, tile(n, f)]).astype(BF16)

    @scope("grad_h")
    def grad_h(m):
        r = pl.ds(pl.multiple_of(m * C, C), C)
        xt[...] = hid[:, r].T
        for n in range(d // C):
            dwd[r, tile(n)] = dot(xt[...], dyv[:, tile(n)]).astype(BF16)

    nf, nd = f // C, d // C
    w_sem, first_rows, gu, second_rows, rest, x_sem = 0, 1, 2, 4, 5, 6
    first = load(small, 0, first_rows)
    wds = [local(wd_h.at[tile(n)], wd.at[tile(n)], w_sem) for n in range(nf)]
    start(first[:1] + wds[:1] + first[1:] + wds[1:])
    for n in range(nd):
        start([local(w.at[tile(n)], wgu.at[tile(n), c * f : (c + 1) * f], gu + n // 2) for c, w in enumerate((wg_h, wu_h))])
    start(load(small, 1, second_rows))
    for e in range(2 * nb):
        start(load(big, e, rest))
    for e in range(SMALL, 2 * SMALL):
        start(load(small, e, rest))
    x_copy = local(x_h, xv, x_sem)
    start([x_copy])

    barrier = pltpu.get_barrier_semaphore()
    for to in (partner, peer):
        pl.semaphore_signal(barrier, inc=1, device_id={"tp": to}, device_id_type=MESH)

    with scope("w_first"):
        all_of(acts.at[pl.ds(base(small, 0), 2 * RS)], load_sem.at[first_rows]).wait()
    with scope("w_wd"):
        all_of(wd, load_sem.at[w_sem]).wait()
    hidden_part(small, 0)
    with scope("barrier"):
        pl.semaphore_wait(barrier, 2)
    lhs = both(dgu, small, 0)
    spare = 2 * (SMALL + nb)
    halves = [slice(n * (d // 2), (n + 1) * (d // 2)) for n in range(2)]
    for n in range(2):
        with scope("w_wgu"):
            all_of(wgu.at[halves[n]], load_sem.at[gu + n]).wait()
        for m in range(nd // 2):
            term_tile(small, 0, n * (nd // 2) + m, lhs)
        term_copy(small, 0, halves[n], spare + n).start()
    chip_sum(small, 0, True, halves[0], spare)
    with scope("w_second"):
        all_of(acts.at[pl.ds(base(small, 1), 2 * RS)], load_sem.at[second_rows]).wait()
    hidden_part(small, 1)
    chip_sum(small, 0, True, halves[1], spare + 1)
    lhs = both(dgu, small, 1)
    for n in range(2):
        for m in range(nd // 2):
            term_tile(small, 1, n * (nd // 2) + m, lhs)
        term_copy(small, 1, halves[n], n).start()
    with scope("w_rest"):
        all_of(acts.at[0 : rows - SMALL * 2 * RS], load_sem.at[rest]).wait()

    @pl.loop(0, 2 * nb)
    def _(e):
        hidden_part(big, e)

        @pl.when(e == 0)
        def _():
            for n in range(2):
                chip_sum(small, 1, True, halves[n], n)

        @pl.when((e > 0) & (e <= nb))
        def _():
            chip_sum(big, e - 1, True)

        @pl.when(e > nb)
        def _():
            chip_sum(big, e - 1, False)

        term_part(big, e)

    for e in range(SMALL, 2 * SMALL):
        hidden_part(small, e)
        if e == SMALL:
            chip_sum(big, 2 * nb - 1, False)
        else:
            chip_sum(small, e - 1, False)
        term_part(small, e)

    with scope("w_x"):
        x_copy.wait()
    finish(big, 0)
    chip_sum(small, 2 * SMALL - 1, False)

    @pl.loop(0, d // C)
    def _(m):
        grad_x(m)

        @pl.when(m == 1)
        def _():
            finish(big, 1)

    finish(big, 2)

    @pl.loop(0, f // C)
    def _(m):
        grad_h(m)

    for j in range(SMALL):
        finish(small, j)

    for j in range(AHEAD):
        pass_on(big, j)

    ahead = AHEAD * RB
    with scope("drain"):
        all_of(dx.at[0:half], sent.at[0]).wait()
    with scope("drain"):
        all_of(dx.at[0 : half // 2], sent.at[1]).wait()
    with scope("drain"):
        all_of(dx.at[0 : half // 2 + ahead], sent.at[3]).wait()
    with scope("drain"):
        all_of(dx.at[0 : half // 2 + ahead], landed).wait()

    @pl.when(core == EARLY)
    def _():
        with scope("drain"):
            all_of(dx.at[0:ahead], sent.at[2]).wait()

    @pl.when(core != EARLY)
    def _():
        for j in range(AHEAD, nb):
            with scope("w_lfinal"):
                final_copy(big, j).wait_recv()
        for j in range(SMALL):
            with scope("w_lfinal"):
                final_copy(small, j).wait_recv()
        with scope("drain"):
            all_of(dx.at[0 : half // 2], sent.at[2]).wait()


def rest_kernel(_, dx, recv, ready, sent, landed):
    half = dx.shape[0] // 2
    me = lax.axis_index("tp")
    chip, core = me // 2, me % 2
    partner, peer = chip * 2 + (1 - core), (1 - chip) * 2 + core
    big = [(SMALL * 2 * RS + j * 2 * RB, RB, 0, RB) for j in range(AHEAD, (half - SMALL * 2 * RS) // (2 * RB))]
    small = [(j * 2 * RS, RS, 0, RS) for j in range(SMALL - 1)]
    last = [((SMALL - 1) * 2 * RS, RS, n * RS // LAST, RS // LAST) for n in range(LAST)]
    pieces = big + small + last

    def rows(owner, piece):
        at, r, off, size = piece
        return pl.ds(pl.multiple_of(owner * half + at + core * r + off, size), size)

    def copy(r, send, recv, to):
        return pltpu.make_async_remote_copy(
            src_ref=dx.at[r], dst_ref=dx.at[r], send_sem=send, recv_sem=recv, device_id={"tp": to}, device_id_type=MESH
        )

    def final_copy(n):
        return copy(rows(chip, pieces[n]), sent.at[0], recv.at[n], peer)

    def core_copy(n):
        return copy(rows(1 - chip, pieces[n]), sent.at[1], landed, partner)

    barrier = pltpu.get_barrier_semaphore()

    @pl.when(core == EARLY)
    def _():
        for to in (peer, partner):
            pl.semaphore_signal(barrier, inc=1, device_id={"tp": to}, device_id_type=MESH)

    with scope("barrier"):
        pl.semaphore_wait(barrier, 1)
    total = dx.at[0 : half // 2 - AHEAD * RB]

    @pl.when(core == EARLY)
    def _():
        for n in range(len(pieces)):
            final_copy(n).start()
        with scope("w_ready"):
            pl.semaphore_wait(ready, 1)
        for n in range(len(pieces)):
            with scope("w_final"):
                final_copy(n).wait_recv()
            core_copy(n).start()
        with scope("drain"):
            pltpu.make_async_copy(total, total, sent.at[0]).wait()

    @pl.when(core != EARLY)
    def _():
        pl.semaphore_signal(ready, inc=1, device_id={"tp": partner}, device_id_type=MESH)
        for n in range(len(pieces)):
            core_copy(n).start()

    with scope("drain"):
        pltpu.make_async_copy(total, total, sent.at[1]).wait()
    with scope("drain"):
        pltpu.make_async_copy(total, total, landed).wait()


def copy_all(pairs, sem):
    copies = [pltpu.make_async_copy(a, b, sem) for a, b in pairs]
    for c in copies:
        c.start()
    for c in copies:
        c.wait()


def late_rows(half, chip):
    first, ahead = SMALL * 2 * RS, AHEAD * 2 * RB
    at = (1 - chip) * half
    return [
        pl.ds(pl.multiple_of(at, first), first),
        pl.ds(pl.multiple_of(at + first + ahead, first), half - first - ahead),
    ]


def write_most(dx_v, dwg_v, dwu_v, dwd_v, _, dx, dwg, dwu, dwd, sem):
    half = dx.shape[0] // 2
    chip = lax.axis_index("tp") // 2
    first, ahead = SMALL * 2 * RS, AHEAD * 2 * RB
    rows = [
        pl.ds(pl.multiple_of((1 - chip) * half + first, first), ahead),
        pl.ds(pl.multiple_of(chip * half, first), half // 2),
        pl.ds(pl.multiple_of(chip * half + half // 2, first), half // 2),
    ]
    pairs = [(dx_v.at[r], dx.at[r]) for r in rows]
    for src, dst in ((dwg_v, dwg), (dwu_v, dwu), (dwd_v, dwd)):
        n = src.shape[0] // 2
        pairs += [(src.at[r], dst.at[r]) for r in (pl.ds(0, n), pl.ds(n, n))]
    copy_all(pairs, sem)


def write_late(dx_v, _, dx, sem):
    half = dx.shape[0] // 2
    copy_all([(dx_v.at[r], dx.at[r]) for r in late_rows(half, lax.axis_index("tp") // 2)], sem)


def solution(mesh):
    def step(x, dy, gate, up, w_gate, w_up, w_down):
        rows, d = x.shape
        f = gate.shape[1]
        nb = (rows // 2 - SMALL * 2 * RS) // (2 * RB)
        outs = [((rows, d), BF16), ((d, f), BF16), ((d, f), BF16), ((f, d), BF16)]
        dma = pltpu.SemaphoreType.DMA

        def buffers(n, r):
            shapes = ((2 * n, F32), (2 * n, BF16), (2 * n, BF16), (n, BF16), (n, BF16))
            return [pltpu.VMEM((m, r, d), t) for m, t in shapes]

        dx, *grads = pl.pallas_call(
            kernel,
            out_shape=[pltpu.VMEM(s, t) for s, t in outs],
            in_specs=[pl.BlockSpec(memory_space=pl.ANY)] * 7,
            out_specs=[pl.BlockSpec(memory_space=pltpu.VMEM)] * 4,
            scratch_shapes=[
                pltpu.VMEM((rows, d), BF16),
                pltpu.VMEM((rows, d + 2 * f), BF16),
                pltpu.VMEM((d, 2 * f), BF16),
                pltpu.VMEM((f, d), BF16),
                pltpu.VMEM((rows, 2 * f), BF16),
                pltpu.VMEM((rows, f), BF16),
                pltpu.VMEM((C, rows), BF16),
            ]
            + buffers(SMALL, RS)
            + buffers(nb, RB)
            + [
                dma((7,)),
                dma((4,)),
                dma(()),
                dma((2 * (SMALL + nb) + 2,)),
                dma((SMALL + nb,)),
                dma((SMALL + nb,)),
            ],
            compiler_params=pltpu.CompilerParams(
                collective_id=0, has_side_effects=True, vmem_limit_bytes=50 * 2**20
            ),
            name="block",
        )(x, dy, gate, up, w_gate, w_up, w_down)
        held, plain = pl.BlockSpec(memory_space=pltpu.VMEM), pl.BlockSpec(memory_space=pl.ANY)
        shapes = [jax.ShapeDtypeStruct(s, t) for s, t in outs]
        little = 2**20

        def pin(a):
            return pltpu.with_memory_space_constraint(a, pltpu.VMEM)

        dx, most, *grads = pl.pallas_call(
            write_most,
            out_shape=[pltpu.VMEM(*outs[0])] + shapes,
            in_specs=[plain] + [held] * 3,
            out_specs=[plain] * 5,
            scratch_shapes=[dma(())],
            input_output_aliases={0: 0},
            compiler_params=pltpu.CompilerParams(vmem_limit_bytes=little),
            name="write_most",
        )(pin(dx), *(pin(g) for g in grads))
        dx = pl.pallas_call(
            rest_kernel,
            out_shape=pltpu.VMEM(*outs[0]),
            in_specs=[plain],
            out_specs=plain,
            scratch_shapes=[dma((nb - AHEAD + SMALL - 1 + LAST,)), pltpu.SemaphoreType.REGULAR, dma((2,)), dma(())],
            input_output_aliases={0: 0},
            compiler_params=pltpu.CompilerParams(collective_id=1, has_side_effects=True, vmem_limit_bytes=little),
            name="rest",
        )(pin(dx))
        dx = pl.pallas_call(
            write_late,
            out_shape=shapes[0],
            in_specs=[held, plain],
            out_specs=plain,
            scratch_shapes=[dma(())],
            input_output_aliases={1: 0},
            compiler_params=pltpu.CompilerParams(vmem_limit_bytes=little),
            name="write_late",
        )(pin(dx), most)
        return dx, *grads

    tokens, columns, rows = P("dp", None), P(None, "tp"), P("tp", None)
    return jax.shard_map(
        step,
        mesh=mesh,
        in_specs=(tokens, tokens, P("dp", "tp"), P("dp", "tp"), columns, columns, rows),
        out_specs=(tokens, P("dp", "tp"), P("dp", "tp"), P(("dp", "tp"), None)),
        check_vma=False,
    )
```

```python
import types

import jax
import jax.numpy as jnp
from jax import lax
from jax.experimental import pallas as pl
from jax.experimental.pallas import tpu as pltpu
from jax.sharding import PartitionSpec as P

MESH = pl.DeviceIdType.MESH
F32, BF16 = jnp.float32, jnp.bfloat16
scope = jax.named_scope
C = 256
SMALL, RS, RB = 2, 64, 128
EARLY, AHEAD, PASSED, LAST = 1, 2, 1, 4


def dot_t(a, b):
    return lax.dot_general(a, b, (((1,), (1,)), ((), ())), preferred_element_type=F32)


def dot(a, b):
    return lax.dot_general(a, b, (((1,), (0,)), ((), ())), preferred_element_type=F32)


def tile(n, start=0):
    return slice(start + n * C, start + (n + 1) * C)


def kernel(
    x_h, dy_h, gate_h, up_h, wg_h, wu_h, wd_h,
    dx, dwg, dwu, dwd,
    xv, acts, wgu, wd, dgu, hid, xt,
    own_s, tsend_s, trecv_s, psend_s, precv_s, own_b, tsend_b, trecv_b, psend_b, precv_b,
    load_sem, sent, landed, term_sem, part_sem, final_sem,
):
    rows, d = xv.shape
    f = wd.shape[0]
    half = rows // 2
    dyv, gv, uv = acts.at[:, 0:d], acts.at[:, d : d + f], acts.at[:, d + f : d + 2 * f]
    me = lax.axis_index("tp")
    chip, core = me // 2, me % 2
    partner, peer = chip * 2 + (1 - core), (1 - chip) * 2 + core
    nb = (half - SMALL * 2 * RS) // (2 * RB)
    small = types.SimpleNamespace(
        r=RS, off=0, n=SMALL, at=0, own=own_s, tsend=tsend_s, trecv=trecv_s, psend=psend_s, precv=precv_s
    )
    big = types.SimpleNamespace(
        r=RB, off=SMALL * 2 * RS, n=nb, at=SMALL, own=own_b, tsend=tsend_b, trecv=trecv_b, psend=psend_b, precv=precv_b
    )

    def base(q, e):
        owner = lax.rem(chip + 1 + e // q.n, 2)
        return pl.multiple_of(owner * half + q.off + lax.rem(e, q.n) * (2 * q.r), 2 * RS)

    def block(q, e, k):
        return pl.ds(pl.multiple_of(base(q, e) + k * q.r, RS), q.r)

    def local(src, dst, sem):
        return pltpu.make_async_copy(src, dst, load_sem.at[sem])

    def load(q, e, sem):
        r = pl.ds(base(q, e), 2 * q.r)
        return [local(src.at[r], dst.at[r], sem) for src, dst in ((dy_h, dyv), (gate_h, gv), (up_h, uv))]

    def all_of(ref, sem):
        return pltpu.make_async_copy(ref, ref, sem)

    def remote(src, dst, send, recv, to):
        return pltpu.make_async_remote_copy(
            src_ref=src, dst_ref=dst, send_sem=send, recv_sem=recv, device_id={"tp": to}, device_id_type=MESH
        )

    def term_copy(q, e, cols=slice(None), sem=None):
        recv = term_sem.at[2 * q.at + e if sem is None else sem]
        return remote(q.tsend.at[e, :, cols], q.trecv.at[e, :, cols], sent.at[0], recv, partner)

    def part_copy(q, e, cols=slice(None)):
        return remote(q.psend.at[e, :, cols], q.precv.at[e, :, cols], sent.at[1], part_sem.at[q.at + e], peer)

    def final_copy(q, j):
        r = block(q, q.n + j, core)
        return remote(dx.at[r], dx.at[r], sent.at[2], final_sem.at[q.at + j], peer)

    def core_copy(r):
        return remote(dx.at[r], dx.at[r], sent.at[3], landed, partner)

    def start(copies):
        for c in copies:
            c.start()

    def hidden_tile(q, e, n, dyb):
        dh = dot_t(dyb, wd[tile(n), :])
        for part, k in ((dh[: q.r], 1 - core), (dh[q.r :], core)):
            r = block(q, e, k)
            g, u = gv[r, tile(n)].astype(F32), uv[r, tile(n)].astype(F32)
            sig = jax.nn.sigmoid(g)
            act = g * sig
            hid[r, tile(n)] = (act * u).astype(BF16)
            dgu[r, tile(n)] = ((part * u) * (sig + act * (1.0 - sig))).astype(BF16)
            dgu[r, tile(n, f)] = (part * act).astype(BF16)

    def both(ref, q, e):
        return jnp.concatenate([ref[block(q, e, 1 - core), :], ref[block(q, e, core), :]], axis=0)

    @scope("hidden_part")
    def hidden_part(q, e):
        dyb = both(dyv, q, e)
        for n in range(f // C):
            hidden_tile(q, e, n, dyb)

    @scope("term_tile")
    def term_tile(q, e, n, lhs):
        t = dot_t(lhs, wgu[tile(n), :])
        q.tsend[e, :, tile(n)] = t[: q.r].astype(BF16)
        q.own[e, :, tile(n)] = t[q.r :]

    @scope("term_part")
    def term_part(q, e):
        lhs = both(dgu, q, e)
        for n in range(d // C):
            term_tile(q, e, n, lhs)
        term_copy(q, e).start()

    @scope("chip_sum")
    def chip_sum(q, e, theirs, cols=slice(None), sem=None):
        with scope("w_term"):
            term_copy(q, e, cols, sem).wait_recv()
        s = q.own[e, :, cols] + q.trecv[e, :, cols].astype(F32)
        if theirs:
            q.psend[e, :, cols] = s.astype(BF16)
            part_copy(q, e, cols).start()
        else:
            q.own[e, :, cols] = s

    @scope("finish")
    def finish(q, j):
        with scope("w_part"):
            part_copy(q, j).wait_recv()
        r = block(q, q.n + j, core)
        dx[r, :] = (q.own[q.n + j] + q.precv[j].astype(F32)).astype(BF16)
        if q is big and j < AHEAD:
            final_copy(q, j).start()
        else:

            @pl.when(core != EARLY)
            def _():
                final_copy(q, j).start()

        core_copy(r).start()

    @scope("pass_on")
    def pass_on(q, j):
        with scope("w_final"):
            final_copy(q, j).wait_recv()
        core_copy(block(q, j, core)).start()

    @scope("grad_x")
    def grad_x(m):
        r = pl.ds(pl.multiple_of(m * C, C), C)
        xt[...] = xv[:, r].T
        for n in range(f // C):
            dwg[r, tile(n)] = dot(xt[...], dgu[:, tile(n)]).astype(BF16)
            dwu[r, tile(n)] = dot(xt[...], dgu[:, tile(n, f)]).astype(BF16)

    @scope("grad_h")
    def grad_h(m):
        r = pl.ds(pl.multiple_of(m * C, C), C)
        xt[...] = hid[:, r].T
        for n in range(d // C):
            dwd[r, tile(n)] = dot(xt[...], dyv[:, tile(n)]).astype(BF16)

    nf, nd = f // C, d // C
    w_sem, first_rows, gu, second_rows, rest, x_sem = 0, 1, 2, 4, 5, 6
    first = load(small, 0, first_rows)
    wds = [local(wd_h.at[tile(n)], wd.at[tile(n)], w_sem) for n in range(nf)]
    start(first[:1] + wds[:1] + first[1:] + wds[1:])
    for n in range(nd):
        start([local(w.at[tile(n)], wgu.at[tile(n), c * f : (c + 1) * f], gu + n // 2) for c, w in enumerate((wg_h, wu_h))])
    start(load(small, 1, second_rows))
    for e in range(2 * nb):
        start(load(big, e, rest))
    for e in range(SMALL, 2 * SMALL):
        start(load(small, e, rest))
    x_copy = local(x_h, xv, x_sem)
    start([x_copy])

    barrier = pltpu.get_barrier_semaphore()
    for to in (partner, peer):
        pl.semaphore_signal(barrier, inc=1, device_id={"tp": to}, device_id_type=MESH)

    with scope("w_first"):
        all_of(acts.at[pl.ds(base(small, 0), 2 * RS)], load_sem.at[first_rows]).wait()
    with scope("w_wd"):
        all_of(wd, load_sem.at[w_sem]).wait()
    hidden_part(small, 0)
    with scope("barrier"):
        pl.semaphore_wait(barrier, 2)
    lhs = both(dgu, small, 0)
    spare = 2 * (SMALL + nb)
    halves = [slice(n * (d // 2), (n + 1) * (d // 2)) for n in range(2)]
    for n in range(2):
        with scope("w_wgu"):
            all_of(wgu.at[halves[n]], load_sem.at[gu + n]).wait()
        for m in range(nd // 2):
            term_tile(small, 0, n * (nd // 2) + m, lhs)
        term_copy(small, 0, halves[n], spare + n).start()
    chip_sum(small, 0, True, halves[0], spare)
    with scope("w_second"):
        all_of(acts.at[pl.ds(base(small, 1), 2 * RS)], load_sem.at[second_rows]).wait()
    hidden_part(small, 1)
    chip_sum(small, 0, True, halves[1], spare + 1)
    lhs = both(dgu, small, 1)
    for n in range(2):
        for m in range(nd // 2):
            term_tile(small, 1, n * (nd // 2) + m, lhs)
        term_copy(small, 1, halves[n], n).start()
    with scope("w_rest"):
        all_of(acts.at[0 : rows - SMALL * 2 * RS], load_sem.at[rest]).wait()

    @pl.loop(0, 2 * nb)
    def _(e):
        hidden_part(big, e)

        @pl.when(e == 0)
        def _():
            for n in range(2):
                chip_sum(small, 1, True, halves[n], n)

        @pl.when((e > 0) & (e <= nb))
        def _():
            chip_sum(big, e - 1, True)

        @pl.when(e > nb)
        def _():
            chip_sum(big, e - 1, False)

        term_part(big, e)

    for e in range(SMALL, 2 * SMALL):
        hidden_part(small, e)
        if e == SMALL:
            chip_sum(big, 2 * nb - 1, False)
        else:
            chip_sum(small, e - 1, False)
        term_part(small, e)

    with scope("w_x"):
        x_copy.wait()
    finish(big, 0)
    chip_sum(small, 2 * SMALL - 1, False)

    @pl.loop(0, d // C)
    def _(m):
        grad_x(m)

        @pl.when(m == 1)
        def _():
            finish(big, 1)

    finish(big, 2)

    @pl.loop(0, f // C)
    def _(m):
        grad_h(m)

    for j in range(SMALL):
        finish(small, j)

    for j in range(PASSED):
        pass_on(big, j)
    for j in range(PASSED, AHEAD):
        with scope("w_lfinal"):
            final_copy(big, j).wait_recv()

    ahead, passed = AHEAD * RB, half // 2 + PASSED * RB
    with scope("drain"):
        all_of(dx.at[0:half], sent.at[0]).wait()
    with scope("drain"):
        all_of(dx.at[0 : half // 2], sent.at[1]).wait()
    with scope("drain"):
        all_of(dx.at[0:passed], sent.at[3]).wait()
    with scope("drain"):
        all_of(dx.at[0:passed], landed).wait()

    @pl.when(core == EARLY)
    def _():
        with scope("drain"):
            all_of(dx.at[0:ahead], sent.at[2]).wait()

    @pl.when(core != EARLY)
    def _():
        for j in range(AHEAD, nb):
            with scope("w_lfinal"):
                final_copy(big, j).wait_recv()
        for j in range(SMALL):
            with scope("w_lfinal"):
                final_copy(small, j).wait_recv()
        with scope("drain"):
            all_of(dx.at[0 : half // 2], sent.at[2]).wait()


def rest_kernel(_, dx, recv, ready, sent, landed):
    half = dx.shape[0] // 2
    me = lax.axis_index("tp")
    chip, core = me // 2, me % 2
    partner, peer = chip * 2 + (1 - core), (1 - chip) * 2 + core
    big = [(SMALL * 2 * RS + j * 2 * RB, RB, 0, RB) for j in range(PASSED, (half - SMALL * 2 * RS) // (2 * RB))]
    here = AHEAD - PASSED
    small = [(j * 2 * RS, RS, 0, RS) for j in range(SMALL - 1)]
    last = [((SMALL - 1) * 2 * RS, RS, n * RS // LAST, RS // LAST) for n in range(LAST)]
    pieces = big + small + last

    def rows(owner, piece):
        at, r, off, size = piece
        return pl.ds(pl.multiple_of(owner * half + at + core * r + off, size), size)

    def copy(r, send, recv, to):
        return pltpu.make_async_remote_copy(
            src_ref=dx.at[r], dst_ref=dx.at[r], send_sem=send, recv_sem=recv, device_id={"tp": to}, device_id_type=MESH
        )

    def final_copy(n):
        return copy(rows(chip, pieces[n]), sent.at[0], recv.at[n - here], peer)

    def core_copy(n):
        return copy(rows(1 - chip, pieces[n]), sent.at[1], landed, partner)

    barrier = pltpu.get_barrier_semaphore()

    @pl.when(core == EARLY)
    def _():
        for to in (peer, partner):
            pl.semaphore_signal(barrier, inc=1, device_id={"tp": to}, device_id_type=MESH)

    with scope("barrier"):
        pl.semaphore_wait(barrier, 1)
    finals, passes = dx.at[0 : half // 2 - AHEAD * RB], dx.at[0 : half // 2 - PASSED * RB]

    @pl.when(core == EARLY)
    def _():
        for n in range(here, len(pieces)):
            final_copy(n).start()
        with scope("w_ready"):
            pl.semaphore_wait(ready, 1)
        for n in range(len(pieces)):
            if n >= here:
                with scope("w_final"):
                    final_copy(n).wait_recv()
            core_copy(n).start()
        with scope("drain"):
            pltpu.make_async_copy(finals, finals, sent.at[0]).wait()

    @pl.when(core != EARLY)
    def _():
        pl.semaphore_signal(ready, inc=1, device_id={"tp": partner}, device_id_type=MESH)
        for n in range(len(pieces)):
            core_copy(n).start()

    with scope("drain"):
        pltpu.make_async_copy(passes, passes, sent.at[1]).wait()
    with scope("drain"):
        pltpu.make_async_copy(passes, passes, landed).wait()


def copy_all(pairs, sem):
    copies = [pltpu.make_async_copy(a, b, sem) for a, b in pairs]
    for c in copies:
        c.start()
    for c in copies:
        c.wait()


def late_rows(half, chip):
    first, passed = SMALL * 2 * RS, PASSED * 2 * RB
    at = (1 - chip) * half
    return [
        pl.ds(pl.multiple_of(at, first), first),
        pl.ds(pl.multiple_of(at + first + passed, first), half - first - passed),
    ]


def write_most(dx_v, dwg_v, dwu_v, dwd_v, _, dx, dwg, dwu, dwd, sem):
    half = dx.shape[0] // 2
    chip = lax.axis_index("tp") // 2
    first, passed = SMALL * 2 * RS, PASSED * 2 * RB
    rows = [
        pl.ds(pl.multiple_of((1 - chip) * half + first, first), passed),
        pl.ds(pl.multiple_of(chip * half, first), half // 2),
        pl.ds(pl.multiple_of(chip * half + half // 2, first), half // 2),
    ]
    pairs = [(dx_v.at[r], dx.at[r]) for r in rows]
    for src, dst in ((dwg_v, dwg), (dwu_v, dwu), (dwd_v, dwd)):
        n = src.shape[0] // 2
        pairs += [(src.at[r], dst.at[r]) for r in (pl.ds(0, n), pl.ds(n, n))]
    copy_all(pairs, sem)


def write_late(dx_v, _, dx, sem):
    half = dx.shape[0] // 2
    copy_all([(dx_v.at[r], dx.at[r]) for r in late_rows(half, lax.axis_index("tp") // 2)], sem)


def solution(mesh):
    def step(x, dy, gate, up, w_gate, w_up, w_down):
        rows, d = x.shape
        f = gate.shape[1]
        nb = (rows // 2 - SMALL * 2 * RS) // (2 * RB)
        outs = [((rows, d), BF16), ((d, f), BF16), ((d, f), BF16), ((f, d), BF16)]
        dma = pltpu.SemaphoreType.DMA

        def buffers(n, r):
            shapes = ((2 * n, F32), (2 * n, BF16), (2 * n, BF16), (n, BF16), (n, BF16))
            return [pltpu.VMEM((m, r, d), t) for m, t in shapes]

        dx, *grads = pl.pallas_call(
            kernel,
            out_shape=[pltpu.VMEM(s, t) for s, t in outs],
            in_specs=[pl.BlockSpec(memory_space=pl.ANY)] * 7,
            out_specs=[pl.BlockSpec(memory_space=pltpu.VMEM)] * 4,
            scratch_shapes=[
                pltpu.VMEM((rows, d), BF16),
                pltpu.VMEM((rows, d + 2 * f), BF16),
                pltpu.VMEM((d, 2 * f), BF16),
                pltpu.VMEM((f, d), BF16),
                pltpu.VMEM((rows, 2 * f), BF16),
                pltpu.VMEM((rows, f), BF16),
                pltpu.VMEM((C, rows), BF16),
            ]
            + buffers(SMALL, RS)
            + buffers(nb, RB)
            + [
                dma((7,)),
                dma((4,)),
                dma(()),
                dma((2 * (SMALL + nb) + 2,)),
                dma((SMALL + nb,)),
                dma((SMALL + nb,)),
            ],
            compiler_params=pltpu.CompilerParams(
                collective_id=0, has_side_effects=True, vmem_limit_bytes=50 * 2**20
            ),
            name="block",
        )(x, dy, gate, up, w_gate, w_up, w_down)
        held, plain = pl.BlockSpec(memory_space=pltpu.VMEM), pl.BlockSpec(memory_space=pl.ANY)
        shapes = [jax.ShapeDtypeStruct(s, t) for s, t in outs]
        little = 2**20

        def pin(a):
            return pltpu.with_memory_space_constraint(a, pltpu.VMEM)

        dx, most, *grads = pl.pallas_call(
            write_most,
            out_shape=[pltpu.VMEM(*outs[0])] + shapes,
            in_specs=[plain] + [held] * 3,
            out_specs=[plain] * 5,
            scratch_shapes=[dma(())],
            input_output_aliases={0: 0},
            compiler_params=pltpu.CompilerParams(vmem_limit_bytes=little),
            name="write_most",
        )(pin(dx), *(pin(g) for g in grads))
        dx = pl.pallas_call(
            rest_kernel,
            out_shape=pltpu.VMEM(*outs[0]),
            in_specs=[plain],
            out_specs=plain,
            scratch_shapes=[dma((nb - AHEAD + SMALL - 1 + LAST,)), pltpu.SemaphoreType.REGULAR, dma((2,)), dma(())],
            input_output_aliases={0: 0},
            compiler_params=pltpu.CompilerParams(collective_id=1, has_side_effects=True, vmem_limit_bytes=little),
            name="rest",
        )(pin(dx))
        dx = pl.pallas_call(
            write_late,
            out_shape=shapes[0],
            in_specs=[held, plain],
            out_specs=plain,
            scratch_shapes=[dma(())],
            input_output_aliases={1: 0},
            compiler_params=pltpu.CompilerParams(vmem_limit_bytes=little),
            name="write_late",
        )(pin(dx), most)
        return dx, *grads

    tokens, columns, rows = P("dp", None), P(None, "tp"), P("tp", None)
    return jax.shard_map(
        step,
        mesh=mesh,
        in_specs=(tokens, tokens, P("dp", "tp"), P("dp", "tp"), columns, columns, rows),
        out_specs=(tokens, P("dp", "tp"), P("dp", "tp"), P(("dp", "tp"), None)),
        check_vma=False,
    )
```

```python
import types

import jax
import jax.numpy as jnp
from jax import lax
from jax.experimental import pallas as pl
from jax.experimental.pallas import tpu as pltpu
from jax.sharding import PartitionSpec as P

MESH = pl.DeviceIdType.MESH
F32, BF16 = jnp.float32, jnp.bfloat16
scope = jax.named_scope
C = 256
SMALL, RS, RB = 2, 64, 128
EARLY, AHEAD, PASSED, LAST = 1, 2, 1, 4


def dot_t(a, b):
    return lax.dot_general(a, b, (((1,), (1,)), ((), ())), preferred_element_type=F32)


def dot(a, b):
    return lax.dot_general(a, b, (((1,), (0,)), ((), ())), preferred_element_type=F32)


def tile(n, start=0):
    return slice(start + n * C, start + (n + 1) * C)


def kernel(
    x_h, dy_h, gate_h, up_h, wg_h, wu_h, wd_h,
    dx, dwg, dwu, dwd,
    xv, acts, wgu, wd, dgu, hid, xt,
    own_s, tsend_s, trecv_s, psend_s, precv_s, own_b, tsend_b, trecv_b, psend_b, precv_b, extra,
    load_sem, sent, landed, term_sem, part_sem, final_sem, extra_sem,
):
    rows, d = xv.shape
    f = wd.shape[0]
    half = rows // 2
    dyv, gv, uv = acts.at[:, 0:d], acts.at[:, d : d + f], acts.at[:, d + f : d + 2 * f]
    me = lax.axis_index("tp")
    chip, core = me // 2, me % 2
    partner, peer, across = chip * 2 + (1 - core), (1 - chip) * 2 + core, (1 - chip) * 2 + (1 - core)
    nb = (half - SMALL * 2 * RS) // (2 * RB)
    small = types.SimpleNamespace(
        r=RS, off=0, n=SMALL, at=0, own=own_s, tsend=tsend_s, trecv=trecv_s, psend=psend_s, precv=precv_s
    )
    big = types.SimpleNamespace(
        r=RB, off=SMALL * 2 * RS, n=nb, at=SMALL, own=own_b, tsend=tsend_b, trecv=trecv_b, psend=psend_b, precv=precv_b
    )

    def base(q, e):
        owner = lax.rem(chip + 1 + e // q.n, 2)
        return pl.multiple_of(owner * half + q.off + lax.rem(e, q.n) * (2 * q.r), 2 * RS)

    def block(q, e, k):
        return pl.ds(pl.multiple_of(base(q, e) + k * q.r, RS), q.r)

    def local(src, dst, sem):
        return pltpu.make_async_copy(src, dst, load_sem.at[sem])

    def load(q, e, sem):
        r = pl.ds(base(q, e), 2 * q.r)
        return [local(src.at[r], dst.at[r], sem) for src, dst in ((dy_h, dyv), (gate_h, gv), (up_h, uv))]

    def all_of(ref, sem):
        return pltpu.make_async_copy(ref, ref, sem)

    def remote(src, dst, send, recv, to):
        return pltpu.make_async_remote_copy(
            src_ref=src, dst_ref=dst, send_sem=send, recv_sem=recv, device_id={"tp": to}, device_id_type=MESH
        )

    def term_copy(q, e, cols=slice(None), n=0):
        recv = term_sem.at[2 * (2 * q.at + e) + n]
        return remote(q.tsend.at[e, :, cols], q.trecv.at[e, :, cols], sent.at[0], recv, partner)

    def part_copy(q, e, cols=slice(None)):
        return remote(q.psend.at[e, :, cols], q.precv.at[e, :, cols], sent.at[1], part_sem.at[q.at + e], peer)

    def extra_copy():
        return remote(tsend_s.at[0, :, tile(0)], extra, sent.at[0], extra_sem, across)

    def final_copy(q, j):
        r = block(q, q.n + j, core)
        return remote(dx.at[r], dx.at[r], sent.at[2], final_sem.at[q.at + j], peer)

    def core_copy(r):
        return remote(dx.at[r], dx.at[r], sent.at[3], landed, partner)

    def start(copies):
        for c in copies:
            c.start()

    def hidden_tile(q, e, n, dyb):
        dh = dot_t(dyb, wd[tile(n), :])
        for part, k in ((dh[: q.r], 1 - core), (dh[q.r :], core)):
            r = block(q, e, k)
            g, u = gv[r, tile(n)].astype(F32), uv[r, tile(n)].astype(F32)
            sig = jax.nn.sigmoid(g)
            act = g * sig
            hid[r, tile(n)] = (act * u).astype(BF16)
            dgu[r, tile(n)] = ((part * u) * (sig + act * (1.0 - sig))).astype(BF16)
            dgu[r, tile(n, f)] = (part * act).astype(BF16)

    def both(ref, q, e):
        return jnp.concatenate([ref[block(q, e, 1 - core), :], ref[block(q, e, core), :]], axis=0)

    @scope("hidden_part")
    def hidden_part(q, e):
        dyb = both(dyv, q, e)
        for n in range(f // C):
            hidden_tile(q, e, n, dyb)

    @scope("term_tile")
    def term_tile(q, e, n, lhs):
        t = dot_t(lhs, wgu[tile(n), :])
        q.tsend[e, :, tile(n)] = t[: q.r].astype(BF16)
        q.own[e, :, tile(n)] = t[q.r :]

    @scope("term_part")
    def term_part(q, e):
        lhs = both(dgu, q, e)
        for n in range(d // C):
            term_tile(q, e, n, lhs)
        term_copy(q, e).start()

    @scope("chip_sum")
    def chip_sum(q, e, theirs, cols=slice(None), n=0):
        with scope("w_term"):
            term_copy(q, e, cols, n).wait_recv()
        s = q.own[e, :, cols] + q.trecv[e, :, cols].astype(F32)
        if theirs:
            q.psend[e, :, cols] = s.astype(BF16)
            part_copy(q, e, cols).start()
        else:
            q.own[e, :, cols] = s

    @scope("finish")
    def finish(q, j):
        with scope("w_part"):
            part_copy(q, j).wait_recv()
        r = block(q, q.n + j, core)
        total = q.own[q.n + j] + q.precv[j].astype(F32)
        if q is small and j == 0:
            extra_copy().wait_recv()
            dx[r, C:] = total[:, C:].astype(BF16)
            dx[r, :C] = (total[:, :C] + extra[...].astype(F32)).astype(BF16)
        else:
            dx[r, :] = total.astype(BF16)
        if q is big and j < AHEAD:
            final_copy(q, j).start()
        else:

            @pl.when(core != EARLY)
            def _():
                final_copy(q, j).start()

        core_copy(r).start()

    @scope("pass_on")
    def pass_on(q, j):
        with scope("w_final"):
            final_copy(q, j).wait_recv()
        core_copy(block(q, j, core)).start()

    @scope("grad_x")
    def grad_x(m):
        r = pl.ds(pl.multiple_of(m * C, C), C)
        xt[...] = xv[:, r].T
        for n in range(f // C):
            dwg[r, tile(n)] = dot(xt[...], dgu[:, tile(n)]).astype(BF16)
            dwu[r, tile(n)] = dot(xt[...], dgu[:, tile(n, f)]).astype(BF16)

    @scope("grad_h")
    def grad_h(m):
        r = pl.ds(pl.multiple_of(m * C, C), C)
        xt[...] = hid[:, r].T
        for n in range(d // C):
            dwd[r, tile(n)] = dot(xt[...], dyv[:, tile(n)]).astype(BF16)

    nf, nd = f // C, d // C
    w_sem, first_rows, gu, second_rows, rest, x_sem = 0, 1, 2, 4, 5, 6
    first = load(small, 0, first_rows)
    wds = [local(wd_h.at[tile(n)], wd.at[tile(n)], w_sem) for n in range(nf)]
    start(first[:1] + wds[:1] + first[1:] + wds[1:])
    for n in range(nd):
        start([local(w.at[tile(n)], wgu.at[tile(n), c * f : (c + 1) * f], gu + n // 2) for c, w in enumerate((wg_h, wu_h))])
    start(load(small, 1, second_rows))
    for e in range(2 * nb):
        start(load(big, e, rest))
    for e in range(SMALL, 2 * SMALL):
        start(load(small, e, rest))
    x_copy = local(x_h, xv, x_sem)
    start([x_copy])

    barrier = pltpu.get_barrier_semaphore()
    for to in (partner, peer, across):
        pl.semaphore_signal(barrier, inc=1, device_id={"tp": to}, device_id_type=MESH)

    with scope("w_first"):
        all_of(acts.at[pl.ds(base(small, 0), 2 * RS)], load_sem.at[first_rows]).wait()
    with scope("w_wd"):
        all_of(wd, load_sem.at[w_sem]).wait()
    hidden_part(small, 0)
    with scope("barrier"):
        pl.semaphore_wait(barrier, 3)
    halves = [slice(n * (d // 2), (n + 1) * (d // 2)) for n in range(2)]

    def halves_of_term(q, e):
        lhs = both(dgu, q, e)
        for n in range(2):
            if q is small and e == 0:
                with scope("w_wgu"):
                    all_of(wgu.at[halves[n]], load_sem.at[gu + n]).wait()
            for m in range(nd // 2):
                term_tile(q, e, n * (nd // 2) + m, lhs)
            cols = halves[n]
            if q is small and e == 0 and n == 0:
                psend_s[0, :, tile(0)] = own_s[0, :, tile(0)].astype(BF16)
                part_copy(small, 0, tile(0)).start()
                extra_copy().start()
                cols = rest_cols
            term_copy(q, e, cols, n).start()

    rest_cols = slice(C, d // 2)
    halves_of_term(small, 0)
    with scope("w_second"):
        all_of(acts.at[pl.ds(base(small, 1), 2 * RS)], load_sem.at[second_rows]).wait()
    hidden_part(small, 1)
    chip_sum(small, 0, True, rest_cols, 0)
    chip_sum(small, 0, True, halves[1], 1)
    halves_of_term(small, 1)
    chip_sum(small, 1, True, halves[0], 0)
    with scope("w_rest"):
        all_of(acts.at[0 : rows - SMALL * 2 * RS], load_sem.at[rest]).wait()
    hidden_part(big, 0)
    chip_sum(small, 1, True, halves[1], 1)
    halves_of_term(big, 0)

    @pl.loop(1, 2 * nb)
    def _(e):
        hidden_part(big, e)

        @pl.when(e == 1)
        def _():
            for n in range(2):
                chip_sum(big, 0, True, halves[n], n)

        @pl.when((e > 1) & (e <= nb))
        def _():
            chip_sum(big, e - 1, True)

        @pl.when(e > nb)
        def _():
            chip_sum(big, e - 1, False)

        term_part(big, e)

    for e in range(SMALL, 2 * SMALL):
        hidden_part(small, e)
        if e == SMALL:
            chip_sum(big, 2 * nb - 1, False)
        else:
            chip_sum(small, e - 1, False)
        term_part(small, e)

    with scope("w_x"):
        x_copy.wait()
    finish(big, 0)
    chip_sum(small, 2 * SMALL - 1, False)

    @pl.loop(0, d // C)
    def _(m):
        grad_x(m)

        @pl.when(m == 1)
        def _():
            finish(big, 1)

    finish(big, 2)

    @pl.loop(0, f // C)
    def _(m):
        grad_h(m)

    for j in range(SMALL):
        finish(small, j)

    for j in range(PASSED):
        pass_on(big, j)
    for j in range(PASSED, AHEAD):
        with scope("w_lfinal"):
            final_copy(big, j).wait_recv()

    ahead, passed = AHEAD * RB, half // 2 + PASSED * RB
    with scope("drain"):
        all_of(dx.at[0:half], sent.at[0]).wait()
    with scope("drain"):
        all_of(dx.at[0 : half // 2], sent.at[1]).wait()
    with scope("drain"):
        all_of(dx.at[0:passed], sent.at[3]).wait()
    with scope("drain"):
        all_of(dx.at[0:passed], landed).wait()

    @pl.when(core == EARLY)
    def _():
        with scope("drain"):
            all_of(dx.at[0:ahead], sent.at[2]).wait()

    @pl.when(core != EARLY)
    def _():
        for j in range(AHEAD, nb):
            with scope("w_lfinal"):
                final_copy(big, j).wait_recv()
        for j in range(SMALL):
            with scope("w_lfinal"):
                final_copy(small, j).wait_recv()
        with scope("drain"):
            all_of(dx.at[0 : half // 2], sent.at[2]).wait()


def rest_kernel(_, dx, recv, direct, ready, sent, landed):
    half = dx.shape[0] // 2
    me = lax.axis_index("tp")
    chip, core = me // 2, me % 2
    partner, peer, across = chip * 2 + (1 - core), (1 - chip) * 2 + core, (1 - chip) * 2 + (1 - core)
    big = [(SMALL * 2 * RS + j * 2 * RB, RB, 0, RB) for j in range(PASSED, (half - SMALL * 2 * RS) // (2 * RB))]
    here = AHEAD - PASSED
    small = [(j * 2 * RS, RS, 0, RS) for j in range(SMALL - 1)]
    last = [((SMALL - 1) * 2 * RS, RS, n * RS // LAST, RS // LAST) for n in range(LAST)]
    pieces = big + small + last

    def rows(owner, piece):
        at, r, off, size = piece
        return pl.ds(pl.multiple_of(owner * half + at + core * r + off, size), size)

    def copy(r, send, recv, to):
        return pltpu.make_async_remote_copy(
            src_ref=dx.at[r], dst_ref=dx.at[r], send_sem=send, recv_sem=recv, device_id={"tp": to}, device_id_type=MESH
        )

    def final_copy(n):
        return copy(rows(chip, pieces[n]), sent.at[0], recv.at[n - here], peer)

    def core_copy(n):
        return copy(rows(1 - chip, pieces[n]), sent.at[1], landed, partner)

    end = len(pieces) - 1
    direct_copy = copy(rows(chip, pieces[end]), sent.at[0], direct, across)

    def all_of(n, sem):
        return pltpu.make_async_copy(dx.at[0:n], dx.at[0:n], sem)

    size = pieces[end][3]
    finals, passes = half // 2 - AHEAD * RB + size, half // 2 - PASSED * RB
    barrier = pltpu.get_barrier_semaphore()

    @pl.when(core == EARLY)
    def _():
        for to in (peer, partner, across):
            pl.semaphore_signal(barrier, inc=1, device_id={"tp": to}, device_id_type=MESH)

    with scope("barrier"):
        pl.semaphore_wait(barrier, 1 + lax.rem(core + EARLY, 2))

    @pl.when(core == EARLY)
    def _():
        for n in range(here, len(pieces)):
            final_copy(n).start()
        with scope("w_ready"):
            pl.semaphore_wait(ready, 2)
        direct_copy.start()
        for n in range(len(pieces)):
            if n >= here:
                with scope("w_final"):
                    final_copy(n).wait_recv()
            if n < end:
                core_copy(n).start()
        with scope("drain"):
            all_of(finals, sent.at[0]).wait()
        with scope("drain"):
            all_of(passes - size, sent.at[1]).wait()
        with scope("drain"):
            all_of(passes, landed).wait()

    @pl.when(core != EARLY)
    def _():
        for to in (partner, across):
            pl.semaphore_signal(ready, inc=1, device_id={"tp": to}, device_id_type=MESH)
        for n in range(len(pieces)):
            core_copy(n).start()
        with scope("drain"):
            all_of(passes, sent.at[1]).wait()
        with scope("drain"):
            all_of(passes - size, landed).wait()
        with scope("w_direct"):
            direct_copy.wait_recv()


def copy_all(pairs, sem):
    copies = [pltpu.make_async_copy(a, b, sem) for a, b in pairs]
    for c in copies:
        c.start()
    for c in copies:
        c.wait()


def late_rows(half, chip):
    first, passed = SMALL * 2 * RS, PASSED * 2 * RB
    at = (1 - chip) * half
    return [
        pl.ds(pl.multiple_of(at, first), first),
        pl.ds(pl.multiple_of(at + first + passed, first), half - first - passed),
    ]


def write_most(dx_v, dwg_v, dwu_v, dwd_v, _, dx, dwg, dwu, dwd, sem):
    half = dx.shape[0] // 2
    chip = lax.axis_index("tp") // 2
    first, passed = SMALL * 2 * RS, PASSED * 2 * RB
    rows = [
        pl.ds(pl.multiple_of((1 - chip) * half + first, first), passed),
        pl.ds(pl.multiple_of(chip * half, first), half // 2),
        pl.ds(pl.multiple_of(chip * half + half // 2, first), half // 2),
    ]
    pairs = [(dx_v.at[r], dx.at[r]) for r in rows]
    for src, dst in ((dwg_v, dwg), (dwu_v, dwu), (dwd_v, dwd)):
        n = src.shape[0] // 2
        pairs += [(src.at[r], dst.at[r]) for r in (pl.ds(0, n), pl.ds(n, n))]
    copy_all(pairs, sem)


def write_late(dx_v, _, dx, sem):
    half = dx.shape[0] // 2
    copy_all([(dx_v.at[r], dx.at[r]) for r in late_rows(half, lax.axis_index("tp") // 2)], sem)


def solution(mesh):
    def step(x, dy, gate, up, w_gate, w_up, w_down):
        rows, d = x.shape
        f = gate.shape[1]
        nb = (rows // 2 - SMALL * 2 * RS) // (2 * RB)
        outs = [((rows, d), BF16), ((d, f), BF16), ((d, f), BF16), ((f, d), BF16)]
        dma = pltpu.SemaphoreType.DMA

        def buffers(n, r):
            shapes = ((2 * n, F32), (2 * n, BF16), (2 * n, BF16), (n, BF16), (n, BF16))
            return [pltpu.VMEM((m, r, d), t) for m, t in shapes]

        dx, *grads = pl.pallas_call(
            kernel,
            out_shape=[pltpu.VMEM(s, t) for s, t in outs],
            in_specs=[pl.BlockSpec(memory_space=pl.ANY)] * 7,
            out_specs=[pl.BlockSpec(memory_space=pltpu.VMEM)] * 4,
            scratch_shapes=[
                pltpu.VMEM((rows, d), BF16),
                pltpu.VMEM((rows, d + 2 * f), BF16),
                pltpu.VMEM((d, 2 * f), BF16),
                pltpu.VMEM((f, d), BF16),
                pltpu.VMEM((rows, 2 * f), BF16),
                pltpu.VMEM((rows, f), BF16),
                pltpu.VMEM((C, rows), BF16),
            ]
            + buffers(SMALL, RS)
            + buffers(nb, RB)
            + [
                pltpu.VMEM((RS, C), BF16),
                dma((7,)),
                dma((4,)),
                dma(()),
                dma((4 * (SMALL + nb),)),
                dma((SMALL + nb,)),
                dma((SMALL + nb,)),
                dma(()),
            ],
            compiler_params=pltpu.CompilerParams(
                collective_id=0, has_side_effects=True, vmem_limit_bytes=50 * 2**20
            ),
            name="block",
        )(x, dy, gate, up, w_gate, w_up, w_down)
        held, plain = pl.BlockSpec(memory_space=pltpu.VMEM), pl.BlockSpec(memory_space=pl.ANY)
        shapes = [jax.ShapeDtypeStruct(s, t) for s, t in outs]
        little = 2**20

        def pin(a):
            return pltpu.with_memory_space_constraint(a, pltpu.VMEM)

        dx, most, *grads = pl.pallas_call(
            write_most,
            out_shape=[pltpu.VMEM(*outs[0])] + shapes,
            in_specs=[plain] + [held] * 3,
            out_specs=[plain] * 5,
            scratch_shapes=[dma(())],
            input_output_aliases={0: 0},
            compiler_params=pltpu.CompilerParams(vmem_limit_bytes=little),
            name="write_most",
        )(pin(dx), *(pin(g) for g in grads))
        dx = pl.pallas_call(
            rest_kernel,
            out_shape=pltpu.VMEM(*outs[0]),
            in_specs=[plain],
            out_specs=plain,
            scratch_shapes=[
                dma((nb - AHEAD + SMALL - 1 + LAST,)), dma(()), pltpu.SemaphoreType.REGULAR, dma((2,)), dma(())
            ],
            input_output_aliases={0: 0},
            compiler_params=pltpu.CompilerParams(collective_id=1, has_side_effects=True, vmem_limit_bytes=little),
            name="rest",
        )(pin(dx))
        dx = pl.pallas_call(
            write_late,
            out_shape=shapes[0],
            in_specs=[held, plain],
            out_specs=plain,
            scratch_shapes=[dma(())],
            input_output_aliases={1: 0},
            compiler_params=pltpu.CompilerParams(vmem_limit_bytes=little),
            name="write_late",
        )(pin(dx), most)
        return dx, *grads

    tokens, columns, rows = P("dp", None), P(None, "tp"), P("tp", None)
    return jax.shard_map(
        step,
        mesh=mesh,
        in_specs=(tokens, tokens, P("dp", "tp"), P("dp", "tp"), columns, columns, rows),
        out_specs=(tokens, P("dp", "tp"), P("dp", "tp"), P(("dp", "tp"), None)),
        check_vma=False,
    )
```

```python
import types

import jax
import jax.numpy as jnp
from jax import lax
from jax.experimental import pallas as pl
from jax.experimental.pallas import tpu as pltpu
from jax.sharding import PartitionSpec as P

MESH = pl.DeviceIdType.MESH
F32, BF16 = jnp.float32, jnp.bfloat16
scope = jax.named_scope
C = 256
SMALL, RS, RB = 2, 64, 128
EARLY, LAST = 1, 4


def dot_t(a, b):
    return lax.dot_general(a, b, (((1,), (1,)), ((), ())), preferred_element_type=F32)


def dot(a, b):
    return lax.dot_general(a, b, (((1,), (0,)), ((), ())), preferred_element_type=F32)


def tile(n, start=0):
    return slice(start + n * C, start + (n + 1) * C)


def kernel(
    x_h, dy_h, gate_h, up_h, wg_h, wu_h, wd_h,
    dx, dwg, dwu, dwd,
    xv, acts, wgu, wd, dgu, hid, xt,
    own_s, tsend_s, trecv_s, psend_s, precv_s, own_b, tsend_b, trecv_b, psend_b, precv_b, extra,
    load_sem, sent, landed, term_sem, part_sem, final_sem, extra_sem,
):
    rows, d = xv.shape
    f = wd.shape[0]
    half = rows // 2
    dyv, gv, uv = acts.at[:, 0:d], acts.at[:, d : d + f], acts.at[:, d + f : d + 2 * f]
    me = lax.axis_index("tp")
    chip, core = me // 2, me % 2
    partner, peer, across = chip * 2 + (1 - core), (1 - chip) * 2 + core, (1 - chip) * 2 + (1 - core)
    nb = (half - SMALL * 2 * RS) // (2 * RB)
    small = types.SimpleNamespace(
        r=RS, off=0, n=SMALL, at=0, own=own_s, tsend=tsend_s, trecv=trecv_s, psend=psend_s, precv=precv_s
    )
    big = types.SimpleNamespace(
        r=RB, off=SMALL * 2 * RS, n=nb, at=SMALL, own=own_b, tsend=tsend_b, trecv=trecv_b, psend=psend_b, precv=precv_b
    )

    def base(q, e):
        owner = lax.rem(chip + 1 + e // q.n, 2)
        return pl.multiple_of(owner * half + q.off + lax.rem(e, q.n) * (2 * q.r), 2 * RS)

    def block(q, e, k):
        return pl.ds(pl.multiple_of(base(q, e) + k * q.r, RS), q.r)

    def local(src, dst, sem):
        return pltpu.make_async_copy(src, dst, load_sem.at[sem])

    def load(q, e, sem):
        r = pl.ds(base(q, e), 2 * q.r)
        return [local(src.at[r], dst.at[r], sem) for src, dst in ((dy_h, dyv), (gate_h, gv), (up_h, uv))]

    def all_of(ref, sem):
        return pltpu.make_async_copy(ref, ref, sem)

    def remote(src, dst, send, recv, to):
        return pltpu.make_async_remote_copy(
            src_ref=src, dst_ref=dst, send_sem=send, recv_sem=recv, device_id={"tp": to}, device_id_type=MESH
        )

    def term_copy(q, e, cols=slice(None), n=0):
        recv = term_sem.at[2 * (2 * q.at + e) + n]
        return remote(q.tsend.at[e, :, cols], q.trecv.at[e, :, cols], sent.at[0], recv, partner)

    def part_copy(q, e, cols=slice(None)):
        return remote(q.psend.at[e, :, cols], q.precv.at[e, :, cols], sent.at[1], part_sem.at[q.at + e], peer)

    def extra_copy():
        return remote(tsend_s.at[0, :, tile(0)], extra, sent.at[0], extra_sem, across)

    def final_copy(q, j):
        r = block(q, q.n + j, core)
        return remote(dx.at[r], dx.at[r], sent.at[2], final_sem.at[q.at + j], peer)

    def core_copy(r):
        return remote(dx.at[r], dx.at[r], sent.at[3], landed, partner)

    def start(copies):
        for c in copies:
            c.start()

    def hidden_tile(q, e, n, dyb):
        dh = dot_t(dyb, wd[tile(n), :])
        for part, k in ((dh[: q.r], 1 - core), (dh[q.r :], core)):
            r = block(q, e, k)
            g, u = gv[r, tile(n)].astype(F32), uv[r, tile(n)].astype(F32)
            sig = jax.nn.sigmoid(g)
            act = g * sig
            hid[r, tile(n)] = (act * u).astype(BF16)
            dgu[r, tile(n)] = ((part * u) * (sig + act * (1.0 - sig))).astype(BF16)
            dgu[r, tile(n, f)] = (part * act).astype(BF16)

    def both(ref, q, e):
        return jnp.concatenate([ref[block(q, e, 1 - core), :], ref[block(q, e, core), :]], axis=0)

    @scope("hidden_part")
    def hidden_part(q, e):
        dyb = both(dyv, q, e)
        for n in range(f // C):
            hidden_tile(q, e, n, dyb)

    @scope("term_tile")
    def term_tile(q, e, n, lhs):
        t = dot_t(lhs, wgu[tile(n), :])
        q.tsend[e, :, tile(n)] = t[: q.r].astype(BF16)
        q.own[e, :, tile(n)] = t[q.r :]

    @scope("term_part")
    def term_part(q, e):
        lhs = both(dgu, q, e)
        for n in range(d // C):
            term_tile(q, e, n, lhs)
        term_copy(q, e).start()

    @scope("chip_sum")
    def chip_sum(q, e, theirs, cols=slice(None), n=0):
        with scope("w_term"):
            term_copy(q, e, cols, n).wait_recv()
        s = q.own[e, :, cols] + q.trecv[e, :, cols].astype(F32)
        if theirs:
            q.psend[e, :, cols] = s.astype(BF16)
            part_copy(q, e, cols).start()
        else:
            q.own[e, :, cols] = s

    @scope("finish")
    def finish(q, j):
        with scope("w_part"):
            part_copy(q, j).wait_recv()
        r = block(q, q.n + j, core)
        total = q.own[q.n + j] + q.precv[j].astype(F32)
        if q is small and j == 0:
            extra_copy().wait_recv()
            dx[r, C:] = total[:, C:].astype(BF16)
            dx[r, :C] = (total[:, :C] + extra[...].astype(F32)).astype(BF16)
        else:
            dx[r, :] = total.astype(BF16)
        if j == 0:
            final_copy(q, j).start()
        else:

            @pl.when(core != EARLY)
            def _():
                final_copy(q, j).start()

        core_copy(r).start()

    @scope("pass_on")
    def pass_on(q, j):
        with scope("w_final"):
            final_copy(q, j).wait_recv()
        core_copy(block(q, j, core)).start()

    @scope("grad_x")
    def grad_x(m):
        r = pl.ds(pl.multiple_of(m * C, C), C)
        xt[...] = xv[:, r].T
        for n in range(f // C):
            dwg[r, tile(n)] = dot(xt[...], dgu[:, tile(n)]).astype(BF16)
            dwu[r, tile(n)] = dot(xt[...], dgu[:, tile(n, f)]).astype(BF16)

    @scope("grad_h")
    def grad_h(m):
        r = pl.ds(pl.multiple_of(m * C, C), C)
        xt[...] = hid[:, r].T
        for n in range(d // C):
            dwd[r, tile(n)] = dot(xt[...], dyv[:, tile(n)]).astype(BF16)

    nf, nd = f // C, d // C
    w_sem, first_rows, gu, second_rows, rest, x_sem = 0, 1, 2, 4, 5, 6
    first = load(small, 0, first_rows)
    wds = [local(wd_h.at[tile(n)], wd.at[tile(n)], w_sem) for n in range(nf)]
    start(first[:1] + wds[:1] + first[1:] + wds[1:])
    for n in range(nd):
        start([local(w.at[tile(n)], wgu.at[tile(n), c * f : (c + 1) * f], gu + n // 2) for c, w in enumerate((wg_h, wu_h))])
    start(load(small, 1, second_rows))
    for e in range(2 * nb):
        start(load(big, e, rest))
    for e in range(SMALL, 2 * SMALL):
        start(load(small, e, rest))
    x_copy = local(x_h, xv, x_sem)
    start([x_copy])

    barrier = pltpu.get_barrier_semaphore()
    for to in (partner, peer, across):
        pl.semaphore_signal(barrier, inc=1, device_id={"tp": to}, device_id_type=MESH)

    with scope("w_first"):
        all_of(acts.at[pl.ds(base(small, 0), 2 * RS)], load_sem.at[first_rows]).wait()
    with scope("w_wd"):
        all_of(wd, load_sem.at[w_sem]).wait()
    hidden_part(small, 0)
    with scope("barrier"):
        pl.semaphore_wait(barrier, 3)
    halves = [slice(n * (d // 2), (n + 1) * (d // 2)) for n in range(2)]

    def halves_of_term(q, e):
        lhs = both(dgu, q, e)
        for n in range(2):
            if q is small and e == 0:
                with scope("w_wgu"):
                    all_of(wgu.at[halves[n]], load_sem.at[gu + n]).wait()
            for m in range(nd // 2):
                term_tile(q, e, n * (nd // 2) + m, lhs)
            cols = halves[n]
            if q is small and e == 0 and n == 0:
                psend_s[0, :, tile(0)] = own_s[0, :, tile(0)].astype(BF16)
                part_copy(small, 0, tile(0)).start()
                extra_copy().start()
                cols = rest_cols
            term_copy(q, e, cols, n).start()

    rest_cols = slice(C, d // 2)
    halves_of_term(small, 0)
    with scope("w_second"):
        all_of(acts.at[pl.ds(base(small, 1), 2 * RS)], load_sem.at[second_rows]).wait()
    hidden_part(small, 1)
    chip_sum(small, 0, True, rest_cols, 0)
    chip_sum(small, 0, True, halves[1], 1)
    halves_of_term(small, 1)
    chip_sum(small, 1, True, halves[0], 0)
    with scope("w_rest"):
        all_of(acts.at[0 : rows - SMALL * 2 * RS], load_sem.at[rest]).wait()
    hidden_part(big, 0)
    chip_sum(small, 1, True, halves[1], 1)
    halves_of_term(big, 0)

    @pl.loop(1, 2 * nb)
    def _(e):
        hidden_part(big, e)

        @pl.when(e == 1)
        def _():
            for n in range(2):
                chip_sum(big, 0, True, halves[n], n)

        term_part(big, e)

        @pl.when((e > 1) & (e <= nb))
        def _():
            chip_sum(big, e - 1, True)

        @pl.when(e > nb)
        def _():
            chip_sum(big, e - 1, False)

    for e in range(SMALL, 2 * SMALL):
        hidden_part(small, e)
        term_part(small, e)
        if e == SMALL:
            chip_sum(big, 2 * nb - 1, False)
        else:
            chip_sum(small, e - 1, False)

    with scope("w_x"):
        x_copy.wait()
    finish(big, 0)
    chip_sum(small, 2 * SMALL - 1, False)
    for j in range(SMALL):
        finish(small, j)
    for j in range(1, nb - 1):
        finish(big, j)

    @pl.loop(0, d // C)
    def _(m):
        grad_x(m)

        @pl.when(m == 1)
        def _():
            finish(big, nb - 1)

    @pl.loop(0, f // C)
    def _(m):
        grad_h(m)

    for q in (big, small):
        pass_on(q, 0)

    ahead = RB + RS
    with scope("drain"):
        all_of(dx.at[0:half], sent.at[0]).wait()
    with scope("drain"):
        all_of(dx.at[0 : half // 2], sent.at[1]).wait()
    with scope("drain"):
        all_of(dx.at[0 : half // 2 + ahead], sent.at[3]).wait()
    with scope("drain"):
        all_of(dx.at[0 : half // 2 + ahead], landed).wait()

    @pl.when(core == EARLY)
    def _():
        with scope("drain"):
            all_of(dx.at[0:ahead], sent.at[2]).wait()

    @pl.when(core != EARLY)
    def _():
        for q in (small, big):
            for j in range(1, q.n):
                with scope("w_final"):
                    final_copy(q, j).wait_recv()
        with scope("drain"):
            all_of(dx.at[0 : half // 2], sent.at[2]).wait()


def rest_kernel(_, dx, recv, direct, ready, sent, landed):
    half = dx.shape[0] // 2
    me = lax.axis_index("tp")
    chip, core = me // 2, me % 2
    partner, peer, across = chip * 2 + (1 - core), (1 - chip) * 2 + core, (1 - chip) * 2 + (1 - core)
    big = [(SMALL * 2 * RS + j * 2 * RB, RB, 0, RB) for j in range(1, (half - SMALL * 2 * RS) // (2 * RB))]
    small = [(j * 2 * RS, RS, 0, RS) for j in range(1, SMALL - 1)]
    last = [((SMALL - 1) * 2 * RS, RS, n * RS // LAST, RS // LAST) for n in range(LAST)]
    pieces = big + small + last

    def rows(owner, piece):
        at, r, off, size = piece
        return pl.ds(pl.multiple_of(owner * half + at + core * r + off, size), size)

    def copy(r, send, recv, to):
        return pltpu.make_async_remote_copy(
            src_ref=dx.at[r], dst_ref=dx.at[r], send_sem=send, recv_sem=recv, device_id={"tp": to}, device_id_type=MESH
        )

    def final_copy(n):
        return copy(rows(chip, pieces[n]), sent.at[0], recv.at[n], peer)

    def core_copy(n):
        return copy(rows(1 - chip, pieces[n]), sent.at[1], landed, partner)

    end = len(pieces) - 1
    direct_copy = copy(rows(chip, pieces[end]), sent.at[0], direct, across)

    def all_of(n, sem):
        return pltpu.make_async_copy(dx.at[0:n], dx.at[0:n], sem)

    size = pieces[end][3]
    passes = half // 2 - RB - RS
    barrier = pltpu.get_barrier_semaphore()

    @pl.when(core == EARLY)
    def _():
        for to in (peer, partner, across):
            pl.semaphore_signal(barrier, inc=1, device_id={"tp": to}, device_id_type=MESH)

    with scope("barrier"):
        pl.semaphore_wait(barrier, 1 + lax.rem(core + EARLY, 2))

    @pl.when(core == EARLY)
    def _():
        for n in range(len(pieces)):
            final_copy(n).start()
        with scope("w_ready"):
            pl.semaphore_wait(ready, 2)
        direct_copy.start()
        for n in range(len(pieces)):
            with scope("w_final"):
                final_copy(n).wait_recv()
            if n < end:
                core_copy(n).start()
        with scope("drain"):
            all_of(passes + size, sent.at[0]).wait()
        with scope("drain"):
            all_of(passes - size, sent.at[1]).wait()
        with scope("drain"):
            all_of(passes, landed).wait()

    @pl.when(core != EARLY)
    def _():
        for to in (partner, across):
            pl.semaphore_signal(ready, inc=1, device_id={"tp": to}, device_id_type=MESH)
        for n in range(len(pieces)):
            core_copy(n).start()
        with scope("drain"):
            all_of(passes, sent.at[1]).wait()
        with scope("drain"):
            all_of(passes - size, landed).wait()
        with scope("w_direct"):
            direct_copy.wait_recv()


def copy_all(pairs, sem):
    copies = [pltpu.make_async_copy(a, b, sem) for a, b in pairs]
    for c in copies:
        c.start()
    for c in copies:
        c.wait()


def rows_of(dx):
    half = dx.shape[0] // 2
    at = (1 - lax.axis_index("tp") // 2) * half
    cuts = [0, 2 * RS, SMALL * 2 * RS, SMALL * 2 * RS + 2 * RB, half]
    parts = [pl.ds(pl.multiple_of(at + a, 2 * RS), b - a) for a, b in zip(cuts, cuts[1:])]
    return parts[1::2], parts[::2]


def write_most(dx_v, dwg_v, dwu_v, dwd_v, _, dx, dwg, dwu, dwd, sem):
    half = dx.shape[0] // 2
    at = lax.axis_index("tp") // 2 * half
    rows = [pl.ds(pl.multiple_of(at + n * (half // 2), 2 * RS), half // 2) for n in range(2)] + rows_of(dx)[1]
    pairs = [(dx_v.at[r], dx.at[r]) for r in rows]
    for src, dst in ((dwg_v, dwg), (dwu_v, dwu), (dwd_v, dwd)):
        n = src.shape[0] // 2
        pairs += [(src.at[r], dst.at[r]) for r in (pl.ds(0, n), pl.ds(n, n))]
    copy_all(pairs, sem)


def write_late(dx_v, _, dx, sem):
    copy_all([(dx_v.at[r], dx.at[r]) for r in rows_of(dx)[0]], sem)


def solution(mesh):
    def step(x, dy, gate, up, w_gate, w_up, w_down):
        rows, d = x.shape
        f = gate.shape[1]
        nb = (rows // 2 - SMALL * 2 * RS) // (2 * RB)
        outs = [((rows, d), BF16), ((d, f), BF16), ((d, f), BF16), ((f, d), BF16)]
        dma = pltpu.SemaphoreType.DMA

        def buffers(n, r):
            shapes = ((2 * n, F32), (2 * n, BF16), (2 * n, BF16), (n, BF16), (n, BF16))
            return [pltpu.VMEM((m, r, d), t) for m, t in shapes]

        dx, *grads = pl.pallas_call(
            kernel,
            out_shape=[pltpu.VMEM(s, t) for s, t in outs],
            in_specs=[pl.BlockSpec(memory_space=pl.ANY)] * 7,
            out_specs=[pl.BlockSpec(memory_space=pltpu.VMEM)] * 4,
            scratch_shapes=[
                pltpu.VMEM((rows, d), BF16),
                pltpu.VMEM((rows, d + 2 * f), BF16),
                pltpu.VMEM((d, 2 * f), BF16),
                pltpu.VMEM((f, d), BF16),
                pltpu.VMEM((rows, 2 * f), BF16),
                pltpu.VMEM((rows, f), BF16),
                pltpu.VMEM((C, rows), BF16),
            ]
            + buffers(SMALL, RS)
            + buffers(nb, RB)
            + [
                pltpu.VMEM((RS, C), BF16),
                dma((7,)),
                dma((4,)),
                dma(()),
                dma((4 * (SMALL + nb),)),
                dma((SMALL + nb,)),
                dma((SMALL + nb,)),
                dma(()),
            ],
            compiler_params=pltpu.CompilerParams(
                collective_id=0, has_side_effects=True, vmem_limit_bytes=50 * 2**20
            ),
            name="block",
        )(x, dy, gate, up, w_gate, w_up, w_down)
        held, plain = pl.BlockSpec(memory_space=pltpu.VMEM), pl.BlockSpec(memory_space=pl.ANY)
        shapes = [jax.ShapeDtypeStruct(s, t) for s, t in outs]
        little = 2**20

        def pin(a):
            return pltpu.with_memory_space_constraint(a, pltpu.VMEM)

        dx, most, *grads = pl.pallas_call(
            write_most,
            out_shape=[pltpu.VMEM(*outs[0])] + shapes,
            in_specs=[plain] + [held] * 3,
            out_specs=[plain] * 5,
            scratch_shapes=[dma(())],
            input_output_aliases={0: 0},
            compiler_params=pltpu.CompilerParams(vmem_limit_bytes=little),
            name="write_most",
        )(pin(dx), *(pin(g) for g in grads))
        dx = pl.pallas_call(
            rest_kernel,
            out_shape=pltpu.VMEM(*outs[0]),
            in_specs=[plain],
            out_specs=plain,
            scratch_shapes=[
                dma((nb + SMALL - 3 + LAST,)), dma(()), pltpu.SemaphoreType.REGULAR, dma((2,)), dma(())
            ],
            input_output_aliases={0: 0},
            compiler_params=pltpu.CompilerParams(collective_id=1, has_side_effects=True, vmem_limit_bytes=little),
            name="rest",
        )(pin(dx))
        dx = pl.pallas_call(
            write_late,
            out_shape=shapes[0],
            in_specs=[held, plain],
            out_specs=plain,
            scratch_shapes=[dma(())],
            input_output_aliases={1: 0},
            compiler_params=pltpu.CompilerParams(vmem_limit_bytes=little),
            name="write_late",
        )(pin(dx), most)
        return dx, *grads

    tokens, columns, rows = P("dp", None), P(None, "tp"), P("tp", None)
    return jax.shard_map(
        step,
        mesh=mesh,
        in_specs=(tokens, tokens, P("dp", "tp"), P("dp", "tp"), columns, columns, rows),
        out_specs=(tokens, P("dp", "tp"), P("dp", "tp"), P(("dp", "tp"), None)),
        check_vma=False,
    )
```

```python
import types

import jax
import jax.numpy as jnp
from jax import lax
from jax.experimental import pallas as pl
from jax.experimental.pallas import tpu as pltpu
from jax.sharding import PartitionSpec as P

MESH = pl.DeviceIdType.MESH
F32, BF16 = jnp.float32, jnp.bfloat16
scope = jax.named_scope
C = 256
SMALL, RS, RB = 2, 64, 128
EARLY, LAST = 1, 4


def dot_t(a, b):
    return lax.dot_general(a, b, (((1,), (1,)), ((), ())), preferred_element_type=F32)


def dot(a, b):
    return lax.dot_general(a, b, (((1,), (0,)), ((), ())), preferred_element_type=F32)


def tile(n, start=0):
    return slice(start + n * C, start + (n + 1) * C)


def kernel(
    x_h, dy_h, gate_h, up_h, wg_h, wu_h, wd_h,
    dx, dwg, dwu, dwd,
    xv, acts, wgu, wd, dgu, hid, xt,
    own_s, tsend_s, trecv_s, psend_s, precv_s, own_b, tsend_b, trecv_b, psend_b, precv_b, extra,
    load_sem, sent, landed, term_sem, part_sem, final_sem, extra_sem,
):
    rows, d = xv.shape
    f = wd.shape[0]
    half = rows // 2
    dyv, gv, uv = acts.at[:, 0:d], acts.at[:, d : d + f], acts.at[:, d + f : d + 2 * f]
    me = lax.axis_index("tp")
    chip, core = me // 2, me % 2
    partner, peer, across = chip * 2 + (1 - core), (1 - chip) * 2 + core, (1 - chip) * 2 + (1 - core)
    nb = (half - SMALL * 2 * RS) // (2 * RB)
    small = types.SimpleNamespace(
        r=RS, off=0, n=SMALL, at=0, own=own_s, tsend=tsend_s, trecv=trecv_s, psend=psend_s, precv=precv_s
    )
    big = types.SimpleNamespace(
        r=RB, off=SMALL * 2 * RS, n=nb, at=SMALL, own=own_b, tsend=tsend_b, trecv=trecv_b, psend=psend_b, precv=precv_b
    )

    def base(q, e):
        owner = lax.rem(chip + 1 + e // q.n, 2)
        return pl.multiple_of(owner * half + q.off + lax.rem(e, q.n) * (2 * q.r), 2 * RS)

    def block(q, e, k):
        return pl.ds(pl.multiple_of(base(q, e) + k * q.r, RS), q.r)

    def local(src, dst, sem):
        return pltpu.make_async_copy(src, dst, load_sem.at[sem])

    def load(q, e, sem):
        r = pl.ds(base(q, e), 2 * q.r)
        return [local(src.at[r], dst.at[r], sem) for src, dst in ((dy_h, dyv), (gate_h, gv), (up_h, uv))]

    def all_of(ref, sem):
        return pltpu.make_async_copy(ref, ref, sem)

    def remote(src, dst, send, recv, to):
        return pltpu.make_async_remote_copy(
            src_ref=src, dst_ref=dst, send_sem=send, recv_sem=recv, device_id={"tp": to}, device_id_type=MESH
        )

    def term_copy(q, e, cols=slice(None), n=0):
        recv = term_sem.at[2 * (2 * q.at + e) + n]
        return remote(q.tsend.at[e, :, cols], q.trecv.at[e, :, cols], sent.at[0], recv, partner)

    def part_copy(q, e, cols=slice(None)):
        return remote(q.psend.at[e, :, cols], q.precv.at[e, :, cols], sent.at[1], part_sem.at[q.at + e], peer)

    def extra_copy():
        return remote(tsend_s.at[0, :, tile(0)], extra, sent.at[0], extra_sem, across)

    def final_copy(q, j):
        r = block(q, q.n + j, core)
        return remote(dx.at[r], dx.at[r], sent.at[2], final_sem.at[q.at + j], peer)

    def core_copy(r):
        return remote(dx.at[r], dx.at[r], sent.at[3], landed, partner)

    def start(copies):
        for c in copies:
            c.start()

    def hidden_tile(q, e, n, dyb):
        dh = dot_t(dyb, wd[tile(n), :])
        for part, k in ((dh[: q.r], 1 - core), (dh[q.r :], core)):
            r = block(q, e, k)
            g, u = gv[r, tile(n)].astype(F32), uv[r, tile(n)].astype(F32)
            sig = jax.nn.sigmoid(g)
            act = g * sig
            hid[r, tile(n)] = (act * u).astype(BF16)
            dgu[r, tile(n)] = ((part * u) * (sig + act * (1.0 - sig))).astype(BF16)
            dgu[r, tile(n, f)] = (part * act).astype(BF16)

    def both(ref, q, e):
        return jnp.concatenate([ref[block(q, e, 1 - core), :], ref[block(q, e, core), :]], axis=0)

    @scope("hidden_part")
    def hidden_part(q, e):
        dyb = both(dyv, q, e)
        for n in range(f // C):
            hidden_tile(q, e, n, dyb)

    @scope("term_tile")
    def term_tile(q, e, n, lhs):
        t = dot_t(lhs, wgu[tile(n), :])
        q.tsend[e, :, tile(n)] = t[: q.r].astype(BF16)
        q.own[e, :, tile(n)] = t[q.r :]

    @scope("term_part")
    def term_part(q, e):
        lhs = both(dgu, q, e)
        for n in range(d // C):
            term_tile(q, e, n, lhs)
        term_copy(q, e).start()

    @scope("chip_sum")
    def chip_sum(q, e, theirs, cols=slice(None), n=0):
        with scope("w_term"):
            term_copy(q, e, cols, n).wait_recv()
        s = q.own[e, :, cols] + q.trecv[e, :, cols].astype(F32)
        if theirs:
            q.psend[e, :, cols] = s.astype(BF16)
            part_copy(q, e, cols).start()
        else:
            q.own[e, :, cols] = s

    @scope("finish")
    def finish(q, j):
        with scope("w_part"):
            part_copy(q, j).wait_recv()
        r = block(q, q.n + j, core)
        total = q.own[q.n + j] + q.precv[j].astype(F32)
        if q is small and j == 0:
            extra_copy().wait_recv()
            dx[r, C:] = total[:, C:].astype(BF16)
            dx[r, :C] = (total[:, :C] + extra[...].astype(F32)).astype(BF16)
        else:
            dx[r, :] = total.astype(BF16)
        if q is big and j == 0:
            final_copy(q, j).start()
        else:

            @pl.when(core != EARLY)
            def _():
                final_copy(q, j).start()

        core_copy(r).start()

    @scope("pass_on")
    def pass_on(q, j):
        with scope("w_final"):
            final_copy(q, j).wait_recv()
        core_copy(block(q, j, core)).start()

    @scope("grad_x")
    def grad_x(m):
        r = pl.ds(pl.multiple_of(m * C, C), C)
        xt[...] = xv[:, r].T
        for n in range(f // C):
            dwg[r, tile(n)] = dot(xt[...], dgu[:, tile(n)]).astype(BF16)
            dwu[r, tile(n)] = dot(xt[...], dgu[:, tile(n, f)]).astype(BF16)

    @scope("grad_h")
    def grad_h(m):
        r = pl.ds(pl.multiple_of(m * C, C), C)
        xt[...] = hid[:, r].T
        for n in range(d // C):
            dwd[r, tile(n)] = dot(xt[...], dyv[:, tile(n)]).astype(BF16)

    nf, nd = f // C, d // C
    w_sem, first_rows, gu, second_rows, rest, x_sem = 0, 1, 2, 4, 5, 6
    first = load(small, 0, first_rows)
    wds = [local(wd_h.at[tile(n)], wd.at[tile(n)], w_sem) for n in range(nf)]
    start(first[:1] + wds[:1] + first[1:] + wds[1:])
    for n in range(nd):
        start([local(w.at[tile(n)], wgu.at[tile(n), c * f : (c + 1) * f], gu + n // 2) for c, w in enumerate((wg_h, wu_h))])
    start(load(small, 1, second_rows))
    for e in range(2 * nb):
        start(load(big, e, rest))
    for e in range(SMALL, 2 * SMALL):
        start(load(small, e, rest))
    x_copy = local(x_h, xv, x_sem)
    start([x_copy])

    barrier = pltpu.get_barrier_semaphore()
    for to in (partner, peer, across):
        pl.semaphore_signal(barrier, inc=1, device_id={"tp": to}, device_id_type=MESH)

    with scope("w_first"):
        all_of(acts.at[pl.ds(base(small, 0), 2 * RS)], load_sem.at[first_rows]).wait()
    with scope("w_wd"):
        all_of(wd, load_sem.at[w_sem]).wait()
    hidden_part(small, 0)
    with scope("barrier"):
        pl.semaphore_wait(barrier, 3)
    halves = [slice(n * (d // 2), (n + 1) * (d // 2)) for n in range(2)]

    def halves_of_term(q, e):
        lhs = both(dgu, q, e)
        for n in range(2):
            if q is small and e == 0:
                with scope("w_wgu"):
                    all_of(wgu.at[halves[n]], load_sem.at[gu + n]).wait()
            for m in range(nd // 2):
                term_tile(q, e, n * (nd // 2) + m, lhs)
            cols = halves[n]
            if q is small and e == 0 and n == 0:
                psend_s[0, :, tile(0)] = own_s[0, :, tile(0)].astype(BF16)
                part_copy(small, 0, tile(0)).start()
                extra_copy().start()
                cols = rest_cols
            term_copy(q, e, cols, n).start()

    rest_cols = slice(C, d // 2)
    halves_of_term(small, 0)
    with scope("w_second"):
        all_of(acts.at[pl.ds(base(small, 1), 2 * RS)], load_sem.at[second_rows]).wait()
    hidden_part(small, 1)
    chip_sum(small, 0, True, rest_cols, 0)
    chip_sum(small, 0, True, halves[1], 1)
    halves_of_term(small, 1)
    chip_sum(small, 1, True, halves[0], 0)
    with scope("w_rest"):
        all_of(acts.at[0 : rows - SMALL * 2 * RS], load_sem.at[rest]).wait()
    hidden_part(big, 0)
    chip_sum(small, 1, True, halves[1], 1)
    halves_of_term(big, 0)

    @pl.loop(1, 2 * nb)
    def _(e):
        hidden_part(big, e)

        @pl.when(e == 1)
        def _():
            for n in range(2):
                chip_sum(big, 0, True, halves[n], n)

        term_part(big, e)

        @pl.when((e > 1) & (e <= nb))
        def _():
            chip_sum(big, e - 1, True)

        @pl.when(e > nb)
        def _():
            chip_sum(big, e - 1, False)

    for e in range(SMALL, 2 * SMALL):
        hidden_part(small, e)
        term_part(small, e)
        if e == SMALL:
            chip_sum(big, 2 * nb - 1, False)
        else:
            chip_sum(small, e - 1, False)

    with scope("w_x"):
        x_copy.wait()
    finish(big, 0)
    chip_sum(small, 2 * SMALL - 1, False)
    for j in range(SMALL):
        finish(small, j)
    for j in range(1, nb - 1):
        finish(big, j)

    @pl.loop(0, d // C)
    def _(m):
        grad_x(m)

    finish(big, nb - 1)

    @pl.loop(0, f // C)
    def _(m):
        grad_h(m)

        @pl.when(m == f // C - 2)
        def _():
            pass_on(big, 0)

    ahead = RB
    with scope("drain"):
        all_of(dx.at[0:half], sent.at[0]).wait()
    with scope("drain"):
        all_of(dx.at[0 : half // 2], sent.at[1]).wait()
    with scope("drain"):
        all_of(dx.at[0 : half // 2 + ahead], sent.at[3]).wait()
    with scope("drain"):
        all_of(dx.at[0 : half // 2 + ahead], landed).wait()

    @pl.when(core == EARLY)
    def _():
        with scope("drain"):
            all_of(dx.at[0:ahead], sent.at[2]).wait()

    @pl.when(core != EARLY)
    def _():
        for q in (small, big):
            for j in range(1 if q is big else 0, q.n):
                with scope("w_final"):
                    final_copy(q, j).wait_recv()
        with scope("drain"):
            all_of(dx.at[0 : half // 2], sent.at[2]).wait()


def rest_kernel(_, dx, recv, direct, ready, sent, landed):
    half = dx.shape[0] // 2
    me = lax.axis_index("tp")
    chip, core = me // 2, me % 2
    partner, peer, across = chip * 2 + (1 - core), (1 - chip) * 2 + core, (1 - chip) * 2 + (1 - core)
    big = [(SMALL * 2 * RS + j * 2 * RB, RB, 0, RB) for j in range(1, (half - SMALL * 2 * RS) // (2 * RB))]
    small = [(j * 2 * RS, RS, 0, RS) for j in range(SMALL - 1)]
    last = [((SMALL - 1) * 2 * RS, RS, n * RS // LAST, RS // LAST) for n in range(LAST)]
    pieces = big + small + last

    def rows(owner, piece):
        at, r, off, size = piece
        return pl.ds(pl.multiple_of(owner * half + at + core * r + off, size), size)

    def copy(r, send, recv, to):
        return pltpu.make_async_remote_copy(
            src_ref=dx.at[r], dst_ref=dx.at[r], send_sem=send, recv_sem=recv, device_id={"tp": to}, device_id_type=MESH
        )

    def final_copy(n):
        return copy(rows(chip, pieces[n]), sent.at[0], recv.at[n], peer)

    def core_copy(n):
        return copy(rows(1 - chip, pieces[n]), sent.at[1], landed, partner)

    end = len(pieces) - 1
    direct_copy = copy(rows(chip, pieces[end]), sent.at[0], direct, across)

    def all_of(n, sem):
        return pltpu.make_async_copy(dx.at[0:n], dx.at[0:n], sem)

    size = pieces[end][3]
    passes = half // 2 - RB
    barrier = pltpu.get_barrier_semaphore()

    @pl.when(core == EARLY)
    def _():
        for to in (peer, partner, across):
            pl.semaphore_signal(barrier, inc=1, device_id={"tp": to}, device_id_type=MESH)

    with scope("barrier"):
        pl.semaphore_wait(barrier, 1 + lax.rem(core + EARLY, 2))

    @pl.when(core == EARLY)
    def _():
        for n in range(len(pieces)):
            final_copy(n).start()
        with scope("w_ready"):
            pl.semaphore_wait(ready, 2)
        direct_copy.start()
        for n in range(len(pieces)):
            with scope("w_final"):
                final_copy(n).wait_recv()
            if n < end:
                core_copy(n).start()
        with scope("drain"):
            all_of(passes + size, sent.at[0]).wait()
        with scope("drain"):
            all_of(passes - size, sent.at[1]).wait()
        with scope("drain"):
            all_of(passes, landed).wait()

    @pl.when(core != EARLY)
    def _():
        for to in (partner, across):
            pl.semaphore_signal(ready, inc=1, device_id={"tp": to}, device_id_type=MESH)
        for n in range(len(pieces)):
            core_copy(n).start()
        with scope("drain"):
            all_of(passes, sent.at[1]).wait()
        with scope("drain"):
            all_of(passes - size, landed).wait()
        with scope("w_direct"):
            direct_copy.wait_recv()


def start_all(pairs, sem):
    copies = [pltpu.make_async_copy(a, b, sem) for a, b in pairs]
    for c in copies:
        c.start()
    return copies


def wait_all(copies):
    for c in copies:
        c.wait()


def rows_of(dx):
    half = dx.shape[0] // 2
    chip = lax.axis_index("tp") // 2
    first = SMALL * 2 * RS
    own = [(chip * half + n * (half // 2), half // 2) for n in range(2)]
    theirs = (1 - chip) * half
    steps = [(theirs + n * 2 * RS, RS) for n in range(SMALL)]
    steps += [(theirs + n, RB) for n in range(first + 2 * RB, half, 2 * RB)]

    def slices(parts):
        return [pl.ds(pl.multiple_of(at, RS), size) for at, size in parts]

    late, early = ([(at + k * size, size) for at, size in steps] for k in (1 - EARLY, EARLY))
    return slices(own + [(theirs + first, 2 * RB)]), slices(late), slices(early)


def write_most(dx_v, dwg_v, dwu_v, dwd_v, _, dx, dwg, dwu, dwd, sem):
    done, late, _ = rows_of(dx)
    pairs = [(dx_v.at[r], dx.at[r]) for r in done]
    for src, dst in ((dwg_v, dwg), (dwu_v, dwu), (dwd_v, dwd)):
        n = src.shape[0] // 2
        pairs += [(src.at[r], dst.at[r]) for r in (pl.ds(0, n), pl.ds(n, n))]
    copies = start_all(pairs, sem)

    @pl.when(lax.rem(lax.axis_index("tp"), 2) != EARLY)
    def _():
        wait_all(start_all([(dx_v.at[r], dx.at[r]) for r in late], sem))

    wait_all(copies)


def write_late(dx_v, _, dx, sem):
    _, late, early = rows_of(dx)
    copies = start_all([(dx_v.at[r], dx.at[r]) for r in early], sem)

    @pl.when(lax.rem(lax.axis_index("tp"), 2) == EARLY)
    def _():
        wait_all(start_all([(dx_v.at[r], dx.at[r]) for r in late], sem))

    wait_all(copies)


def solution(mesh):
    def step(x, dy, gate, up, w_gate, w_up, w_down):
        rows, d = x.shape
        f = gate.shape[1]
        nb = (rows // 2 - SMALL * 2 * RS) // (2 * RB)
        outs = [((rows, d), BF16), ((d, f), BF16), ((d, f), BF16), ((f, d), BF16)]
        dma = pltpu.SemaphoreType.DMA

        def buffers(n, r):
            shapes = ((2 * n, F32), (2 * n, BF16), (2 * n, BF16), (n, BF16), (n, BF16))
            return [pltpu.VMEM((m, r, d), t) for m, t in shapes]

        dx, *grads = pl.pallas_call(
            kernel,
            out_shape=[pltpu.VMEM(s, t) for s, t in outs],
            in_specs=[pl.BlockSpec(memory_space=pl.ANY)] * 7,
            out_specs=[pl.BlockSpec(memory_space=pltpu.VMEM)] * 4,
            scratch_shapes=[
                pltpu.VMEM((rows, d), BF16),
                pltpu.VMEM((rows, d + 2 * f), BF16),
                pltpu.VMEM((d, 2 * f), BF16),
                pltpu.VMEM((f, d), BF16),
                pltpu.VMEM((rows, 2 * f), BF16),
                pltpu.VMEM((rows, f), BF16),
                pltpu.VMEM((C, rows), BF16),
            ]
            + buffers(SMALL, RS)
            + buffers(nb, RB)
            + [
                pltpu.VMEM((RS, C), BF16),
                dma((7,)),
                dma((4,)),
                dma(()),
                dma((4 * (SMALL + nb),)),
                dma((SMALL + nb,)),
                dma((SMALL + nb,)),
                dma(()),
            ],
            compiler_params=pltpu.CompilerParams(
                collective_id=0, has_side_effects=True, vmem_limit_bytes=50 * 2**20
            ),
            name="block",
        )(x, dy, gate, up, w_gate, w_up, w_down)
        held, plain = pl.BlockSpec(memory_space=pltpu.VMEM), pl.BlockSpec(memory_space=pl.ANY)
        shapes = [jax.ShapeDtypeStruct(s, t) for s, t in outs]
        little = 2**20

        def pin(a):
            return pltpu.with_memory_space_constraint(a, pltpu.VMEM)

        dx, most, *grads = pl.pallas_call(
            write_most,
            out_shape=[pltpu.VMEM(*outs[0])] + shapes,
            in_specs=[plain] + [held] * 3,
            out_specs=[plain] * 5,
            scratch_shapes=[dma(())],
            input_output_aliases={0: 0},
            compiler_params=pltpu.CompilerParams(vmem_limit_bytes=little),
            name="write_most",
        )(pin(dx), *(pin(g) for g in grads))
        dx = pl.pallas_call(
            rest_kernel,
            out_shape=pltpu.VMEM(*outs[0]),
            in_specs=[plain],
            out_specs=plain,
            scratch_shapes=[
                dma((nb + SMALL - 2 + LAST,)), dma(()), pltpu.SemaphoreType.REGULAR, dma((2,)), dma(())
            ],
            input_output_aliases={0: 0},
            compiler_params=pltpu.CompilerParams(collective_id=1, has_side_effects=True, vmem_limit_bytes=little),
            name="rest",
        )(pin(dx))
        dx = pl.pallas_call(
            write_late,
            out_shape=shapes[0],
            in_specs=[held, plain],
            out_specs=plain,
            scratch_shapes=[dma(())],
            input_output_aliases={1: 0},
            compiler_params=pltpu.CompilerParams(vmem_limit_bytes=little),
            name="write_late",
        )(pin(dx), most)
        return dx, *grads

    tokens, columns, rows = P("dp", None), P(None, "tp"), P("tp", None)
    return jax.shard_map(
        step,
        mesh=mesh,
        in_specs=(tokens, tokens, P("dp", "tp"), P("dp", "tp"), columns, columns, rows),
        out_specs=(tokens, P("dp", "tp"), P("dp", "tp"), P(("dp", "tp"), None)),
        check_vma=False,
    )
```

```python
import types

import jax
import jax.numpy as jnp
from jax import lax
from jax.experimental import pallas as pl
from jax.experimental.pallas import tpu as pltpu
from jax.sharding import PartitionSpec as P

MESH = pl.DeviceIdType.MESH
F32, BF16 = jnp.float32, jnp.bfloat16
C = 256
SMALL, RS, RB = 2, 64, 128
EARLY, LAST = 1, 4


def dot_t(a, b):
    return lax.dot_general(a, b, (((1,), (1,)), ((), ())), preferred_element_type=F32)


def dot(a, b):
    return lax.dot_general(a, b, (((1,), (0,)), ((), ())), preferred_element_type=F32)


def tile(n, start=0):
    return slice(start + n * C, start + (n + 1) * C)


def kernel(
    x_h, dy_h, gate_h, up_h, wg_h, wu_h, wd_h,
    dx, dwg, dwu, dwd,
    xv, acts, wgu, wd, dgu, hid, xt,
    own_s, tsend_s, trecv_s, psend_s, precv_s, own_b, tsend_b, trecv_b, psend_b, precv_b, extra,
    load_sem, sent, landed, term_sem, part_sem, final_sem, extra_sem,
):
    rows, d = xv.shape
    f = wd.shape[0]
    half = rows // 2
    dyv, gv, uv = acts.at[:, 0:d], acts.at[:, d : d + f], acts.at[:, d + f : d + 2 * f]
    me = lax.axis_index("tp")
    chip, core = me // 2, me % 2
    partner, peer, across = chip * 2 + (1 - core), (1 - chip) * 2 + core, (1 - chip) * 2 + (1 - core)
    nb = (half - SMALL * 2 * RS) // (2 * RB)
    small = types.SimpleNamespace(
        r=RS, off=0, n=SMALL, at=0, own=own_s, tsend=tsend_s, trecv=trecv_s, psend=psend_s, precv=precv_s
    )
    big = types.SimpleNamespace(
        r=RB, off=SMALL * 2 * RS, n=nb, at=SMALL, own=own_b, tsend=tsend_b, trecv=trecv_b, psend=psend_b, precv=precv_b
    )

    def base(q, e):
        owner = lax.rem(chip + 1 + e // q.n, 2)
        return pl.multiple_of(owner * half + q.off + lax.rem(e, q.n) * (2 * q.r), 2 * RS)

    def block(q, e, k):
        return pl.ds(pl.multiple_of(base(q, e) + k * q.r, RS), q.r)

    def local(src, dst, sem):
        return pltpu.make_async_copy(src, dst, load_sem.at[sem])

    def load(q, e, sem):
        r = pl.ds(base(q, e), 2 * q.r)
        return [local(src.at[r], dst.at[r], sem) for src, dst in ((dy_h, dyv), (gate_h, gv), (up_h, uv))]

    def all_of(ref, sem):
        return pltpu.make_async_copy(ref, ref, sem)

    def remote(src, dst, send, recv, to):
        return pltpu.make_async_remote_copy(
            src_ref=src, dst_ref=dst, send_sem=send, recv_sem=recv, device_id={"tp": to}, device_id_type=MESH
        )

    def term_copy(q, e, cols=slice(None), n=0):
        recv = term_sem.at[2 * (2 * q.at + e) + n]
        return remote(q.tsend.at[e, :, cols], q.trecv.at[e, :, cols], sent.at[0], recv, partner)

    def part_copy(q, e, cols=slice(None)):
        return remote(q.psend.at[e, :, cols], q.precv.at[e, :, cols], sent.at[1], part_sem.at[q.at + e], peer)

    def extra_copy():
        return remote(tsend_s.at[0, :, tile(0)], extra, sent.at[0], extra_sem, across)

    def final_copy(q, j):
        r = block(q, q.n + j, core)
        return remote(dx.at[r], dx.at[r], sent.at[2], final_sem.at[q.at + j], peer)

    def core_copy(r):
        return remote(dx.at[r], dx.at[r], sent.at[3], landed, partner)

    def start(copies):
        for c in copies:
            c.start()

    def hidden_tile(q, e, n, dyb):
        dh = dot_t(dyb, wd[tile(n), :])
        for part, k in ((dh[: q.r], 1 - core), (dh[q.r :], core)):
            r = block(q, e, k)
            g, u = gv[r, tile(n)].astype(F32), uv[r, tile(n)].astype(F32)
            sig = jax.nn.sigmoid(g)
            act = g * sig
            hid[r, tile(n)] = (act * u).astype(BF16)
            dgu[r, tile(n)] = ((part * u) * (sig + act * (1.0 - sig))).astype(BF16)
            dgu[r, tile(n, f)] = (part * act).astype(BF16)

    def both(ref, q, e):
        return jnp.concatenate([ref[block(q, e, 1 - core), :], ref[block(q, e, core), :]], axis=0)

    def hidden_part(q, e):
        dyb = both(dyv, q, e)
        for n in range(f // C):
            hidden_tile(q, e, n, dyb)

    def term_tile(q, e, n, lhs):
        t = dot_t(lhs, wgu[tile(n), :])
        q.tsend[e, :, tile(n)] = t[: q.r].astype(BF16)
        q.own[e, :, tile(n)] = t[q.r :]

    def term_part(q, e):
        lhs = both(dgu, q, e)
        for n in range(d // C):
            term_tile(q, e, n, lhs)
        term_copy(q, e).start()

    def chip_sum(q, e, theirs, cols=slice(None), n=0):
        term_copy(q, e, cols, n).wait_recv()
        s = q.own[e, :, cols] + q.trecv[e, :, cols].astype(F32)
        if theirs:
            q.psend[e, :, cols] = s.astype(BF16)
            part_copy(q, e, cols).start()
        else:
            q.own[e, :, cols] = s

    def finish(q, j):
        part_copy(q, j).wait_recv()
        r = block(q, q.n + j, core)
        total = q.own[q.n + j] + q.precv[j].astype(F32)
        if q is small and j == 0:
            extra_copy().wait_recv()
            dx[r, C:] = total[:, C:].astype(BF16)
            dx[r, :C] = (total[:, :C] + extra[...].astype(F32)).astype(BF16)
        else:
            dx[r, :] = total.astype(BF16)
        if q is big and j == 0:
            final_copy(q, j).start()
        else:

            @pl.when(core != EARLY)
            def _():
                final_copy(q, j).start()

        core_copy(r).start()

    def pass_on(q, j):
        final_copy(q, j).wait_recv()
        core_copy(block(q, j, core)).start()

    def grad_x(m):
        r = pl.ds(pl.multiple_of(m * C, C), C)
        xt[...] = xv[:, r].T
        for n in range(f // C):
            dwg[r, tile(n)] = dot(xt[...], dgu[:, tile(n)]).astype(BF16)
            dwu[r, tile(n)] = dot(xt[...], dgu[:, tile(n, f)]).astype(BF16)

    def grad_h(m):
        r = pl.ds(pl.multiple_of(m * C, C), C)
        xt[...] = hid[:, r].T
        for n in range(d // C):
            dwd[r, tile(n)] = dot(xt[...], dyv[:, tile(n)]).astype(BF16)

    nf, nd = f // C, d // C
    w_sem, first_rows, gu, second_rows, rest, x_sem = 0, 1, 2, 4, 5, 6
    first = load(small, 0, first_rows)
    wds = [local(wd_h.at[tile(n)], wd.at[tile(n)], w_sem) for n in range(nf)]
    start(first[:1] + wds[:1] + first[1:] + wds[1:])
    for n in range(nd):
        start([local(w.at[tile(n)], wgu.at[tile(n), c * f : (c + 1) * f], gu + n // 2) for c, w in enumerate((wg_h, wu_h))])
    start(load(small, 1, second_rows))
    for e in range(2 * nb):
        start(load(big, e, rest))
    for e in range(SMALL, 2 * SMALL):
        start(load(small, e, rest))
    x_copy = local(x_h, xv, x_sem)
    start([x_copy])

    barrier = pltpu.get_barrier_semaphore()
    for to in (partner, peer, across):
        pl.semaphore_signal(barrier, inc=1, device_id={"tp": to}, device_id_type=MESH)

    all_of(acts.at[pl.ds(base(small, 0), 2 * RS)], load_sem.at[first_rows]).wait()
    all_of(wd, load_sem.at[w_sem]).wait()
    hidden_part(small, 0)
    pl.semaphore_wait(barrier, 3)
    halves = [slice(n * (d // 2), (n + 1) * (d // 2)) for n in range(2)]

    def halves_of_term(q, e):
        lhs = both(dgu, q, e)
        for n in range(2):
            if q is small and e == 0:
                all_of(wgu.at[halves[n]], load_sem.at[gu + n]).wait()
            for m in range(nd // 2):
                term_tile(q, e, n * (nd // 2) + m, lhs)
            cols = halves[n]
            if q is small and e == 0 and n == 0:
                psend_s[0, :, tile(0)] = own_s[0, :, tile(0)].astype(BF16)
                part_copy(small, 0, tile(0)).start()
                extra_copy().start()
                cols = rest_cols
            term_copy(q, e, cols, n).start()

    rest_cols = slice(C, d // 2)
    halves_of_term(small, 0)
    all_of(acts.at[pl.ds(base(small, 1), 2 * RS)], load_sem.at[second_rows]).wait()
    hidden_part(small, 1)
    chip_sum(small, 0, True, rest_cols, 0)
    chip_sum(small, 0, True, halves[1], 1)
    halves_of_term(small, 1)
    chip_sum(small, 1, True, halves[0], 0)
    all_of(acts.at[0 : rows - SMALL * 2 * RS], load_sem.at[rest]).wait()
    hidden_part(big, 0)
    chip_sum(small, 1, True, halves[1], 1)
    halves_of_term(big, 0)

    @pl.loop(1, 2 * nb)
    def _(e):
        hidden_part(big, e)

        @pl.when(e == 1)
        def _():
            for n in range(2):
                chip_sum(big, 0, True, halves[n], n)

        term_part(big, e)

        @pl.when((e > 1) & (e <= nb))
        def _():
            chip_sum(big, e - 1, True)

        @pl.when(e > nb)
        def _():
            chip_sum(big, e - 1, False)

    for e in range(SMALL, 2 * SMALL):
        hidden_part(small, e)
        term_part(small, e)
        if e == SMALL:
            chip_sum(big, 2 * nb - 1, False)
        else:
            chip_sum(small, e - 1, False)

    x_copy.wait()
    finish(big, 0)
    chip_sum(small, 2 * SMALL - 1, False)
    for j in range(SMALL):
        finish(small, j)
    for j in range(1, nb - 1):
        finish(big, j)

    @pl.loop(0, d // C)
    def _(m):
        grad_x(m)

    finish(big, nb - 1)

    @pl.loop(0, f // C)
    def _(m):
        grad_h(m)

        @pl.when(m == f // C - 2)
        def _():
            pass_on(big, 0)

    ahead = RB
    all_of(dx.at[0:half], sent.at[0]).wait()
    all_of(dx.at[0 : half // 2], sent.at[1]).wait()
    all_of(dx.at[0 : half // 2 + ahead], sent.at[3]).wait()
    all_of(dx.at[0 : half // 2 + ahead], landed).wait()

    @pl.when(core == EARLY)
    def _():
        all_of(dx.at[0:ahead], sent.at[2]).wait()

    @pl.when(core != EARLY)
    def _():
        for q in (small, big):
            for j in range(1 if q is big else 0, q.n):
                final_copy(q, j).wait_recv()
        all_of(dx.at[0 : half // 2], sent.at[2]).wait()


def rest_kernel(_, dx, recv, direct, ready, sent, landed):
    half = dx.shape[0] // 2
    me = lax.axis_index("tp")
    chip, core = me // 2, me % 2
    partner, peer, across = chip * 2 + (1 - core), (1 - chip) * 2 + core, (1 - chip) * 2 + (1 - core)
    big = [(SMALL * 2 * RS + j * 2 * RB, RB, 0, RB) for j in range(1, (half - SMALL * 2 * RS) // (2 * RB))]
    small = [(j * 2 * RS, RS, 0, RS) for j in range(SMALL - 1)]
    last = [((SMALL - 1) * 2 * RS, RS, n * RS // LAST, RS // LAST) for n in range(LAST)]
    pieces = big + small + last

    def rows(owner, piece):
        at, r, off, size = piece
        return pl.ds(pl.multiple_of(owner * half + at + core * r + off, size), size)

    def copy(r, send, recv, to):
        return pltpu.make_async_remote_copy(
            src_ref=dx.at[r], dst_ref=dx.at[r], send_sem=send, recv_sem=recv, device_id={"tp": to}, device_id_type=MESH
        )

    def final_copy(n):
        return copy(rows(chip, pieces[n]), sent.at[0], recv.at[n], peer)

    def core_copy(n):
        return copy(rows(1 - chip, pieces[n]), sent.at[1], landed, partner)

    end = len(pieces) - 1
    direct_copy = copy(rows(chip, pieces[end]), sent.at[0], direct, across)

    def all_of(n, sem):
        return pltpu.make_async_copy(dx.at[0:n], dx.at[0:n], sem)

    size = pieces[end][3]
    passes = half // 2 - RB
    barrier = pltpu.get_barrier_semaphore()

    @pl.when(core == EARLY)
    def _():
        for to in (peer, partner, across):
            pl.semaphore_signal(barrier, inc=1, device_id={"tp": to}, device_id_type=MESH)

    pl.semaphore_wait(barrier, 1 + lax.rem(core + EARLY, 2))

    @pl.when(core == EARLY)
    def _():
        for n in range(len(pieces)):
            final_copy(n).start()
        pl.semaphore_wait(ready, 2)
        direct_copy.start()
        for n in range(len(pieces)):
            final_copy(n).wait_recv()
            if n < end:
                core_copy(n).start()
        all_of(passes + size, sent.at[0]).wait()
        all_of(passes - size, sent.at[1]).wait()
        all_of(passes, landed).wait()

    @pl.when(core != EARLY)
    def _():
        for to in (partner, across):
            pl.semaphore_signal(ready, inc=1, device_id={"tp": to}, device_id_type=MESH)
        for n in range(len(pieces)):
            core_copy(n).start()
        all_of(passes, sent.at[1]).wait()
        all_of(passes - size, landed).wait()
        direct_copy.wait_recv()


def start_all(pairs, sem):
    copies = [pltpu.make_async_copy(a, b, sem) for a, b in pairs]
    for c in copies:
        c.start()
    return copies


def wait_all(copies):
    for c in copies:
        c.wait()


def rows_of(dx):
    half = dx.shape[0] // 2
    chip = lax.axis_index("tp") // 2
    first = SMALL * 2 * RS
    own = [(chip * half + n * (half // 2), half // 2) for n in range(2)]
    theirs = (1 - chip) * half
    steps = [(theirs + n * 2 * RS, RS) for n in range(SMALL)]
    steps += [(theirs + n, RB) for n in range(first + 2 * RB, half, 2 * RB)]

    def slices(parts):
        return [pl.ds(pl.multiple_of(at, RS), size) for at, size in parts]

    late, early = ([(at + k * size, size) for at, size in steps] for k in (1 - EARLY, EARLY))
    return slices(own + [(theirs + first, 2 * RB)]), slices(late), slices(early)


def write_most(dx_v, dwg_v, dwu_v, dwd_v, _, dx, dwg, dwu, dwd, sem):
    done, late, _ = rows_of(dx)
    pairs = [(dx_v.at[r], dx.at[r]) for r in done]
    for src, dst in ((dwg_v, dwg), (dwu_v, dwu), (dwd_v, dwd)):
        n = src.shape[0] // 2
        pairs += [(src.at[r], dst.at[r]) for r in (pl.ds(0, n), pl.ds(n, n))]
    copies = start_all(pairs, sem)

    @pl.when(lax.rem(lax.axis_index("tp"), 2) != EARLY)
    def _():
        wait_all(start_all([(dx_v.at[r], dx.at[r]) for r in late], sem))

    wait_all(copies)


def write_late(dx_v, _, dx, sem):
    _, late, early = rows_of(dx)
    copies = start_all([(dx_v.at[r], dx.at[r]) for r in early], sem)

    @pl.when(lax.rem(lax.axis_index("tp"), 2) == EARLY)
    def _():
        wait_all(start_all([(dx_v.at[r], dx.at[r]) for r in late], sem))

    wait_all(copies)


def solution(mesh):
    def step(x, dy, gate, up, w_gate, w_up, w_down):
        rows, d = x.shape
        f = gate.shape[1]
        nb = (rows // 2 - SMALL * 2 * RS) // (2 * RB)
        outs = [((rows, d), BF16), ((d, f), BF16), ((d, f), BF16), ((f, d), BF16)]
        dma = pltpu.SemaphoreType.DMA

        def buffers(n, r):
            shapes = ((2 * n, F32), (2 * n, BF16), (2 * n, BF16), (n, BF16), (n, BF16))
            return [pltpu.VMEM((m, r, d), t) for m, t in shapes]

        dx, *grads = pl.pallas_call(
            kernel,
            out_shape=[pltpu.VMEM(s, t) for s, t in outs],
            in_specs=[pl.BlockSpec(memory_space=pl.ANY)] * 7,
            out_specs=[pl.BlockSpec(memory_space=pltpu.VMEM)] * 4,
            scratch_shapes=[
                pltpu.VMEM((rows, d), BF16),
                pltpu.VMEM((rows, d + 2 * f), BF16),
                pltpu.VMEM((d, 2 * f), BF16),
                pltpu.VMEM((f, d), BF16),
                pltpu.VMEM((rows, 2 * f), BF16),
                pltpu.VMEM((rows, f), BF16),
                pltpu.VMEM((C, rows), BF16),
            ]
            + buffers(SMALL, RS)
            + buffers(nb, RB)
            + [
                pltpu.VMEM((RS, C), BF16),
                dma((7,)),
                dma((4,)),
                dma(()),
                dma((4 * (SMALL + nb),)),
                dma((SMALL + nb,)),
                dma((SMALL + nb,)),
                dma(()),
            ],
            compiler_params=pltpu.CompilerParams(
                collective_id=0, has_side_effects=True, vmem_limit_bytes=50 * 2**20
            ),
            name="block",
        )(x, dy, gate, up, w_gate, w_up, w_down)
        held, plain = pl.BlockSpec(memory_space=pltpu.VMEM), pl.BlockSpec(memory_space=pl.ANY)
        shapes = [jax.ShapeDtypeStruct(s, t) for s, t in outs]
        little = 2**20

        def pin(a):
            return pltpu.with_memory_space_constraint(a, pltpu.VMEM)

        dx, most, *grads = pl.pallas_call(
            write_most,
            out_shape=[pltpu.VMEM(*outs[0])] + shapes,
            in_specs=[plain] + [held] * 3,
            out_specs=[plain] * 5,
            scratch_shapes=[dma(())],
            input_output_aliases={0: 0},
            compiler_params=pltpu.CompilerParams(vmem_limit_bytes=little),
            name="write_most",
        )(pin(dx), *(pin(g) for g in grads))
        dx = pl.pallas_call(
            rest_kernel,
            out_shape=pltpu.VMEM(*outs[0]),
            in_specs=[plain],
            out_specs=plain,
            scratch_shapes=[
                dma((nb + SMALL - 2 + LAST,)), dma(()), pltpu.SemaphoreType.REGULAR, dma((2,)), dma(())
            ],
            input_output_aliases={0: 0},
            compiler_params=pltpu.CompilerParams(collective_id=1, has_side_effects=True, vmem_limit_bytes=little),
            name="rest",
        )(pin(dx))
        dx = pl.pallas_call(
            write_late,
            out_shape=shapes[0],
            in_specs=[held, plain],
            out_specs=plain,
            scratch_shapes=[dma(())],
            input_output_aliases={1: 0},
            compiler_params=pltpu.CompilerParams(vmem_limit_bytes=little),
            name="write_late",
        )(pin(dx), most)
        return dx, *grads

    tokens, columns, rows = P("dp", None), P(None, "tp"), P("tp", None)
    return jax.shard_map(
        step,
        mesh=mesh,
        in_specs=(tokens, tokens, P("dp", "tp"), P("dp", "tp"), columns, columns, rows),
        out_specs=(tokens, P("dp", "tp"), P("dp", "tp"), P(("dp", "tp"), None)),
        check_vma=False,
    )
```

```python
import types

import jax
import jax.numpy as jnp
from jax import lax
from jax.experimental import pallas as pl
from jax.experimental.pallas import tpu as pltpu
from jax.sharding import PartitionSpec as P

MESH = pl.DeviceIdType.MESH
F32, BF16 = jnp.float32, jnp.bfloat16
C = 256
SMALL, RS, RB = 2, 64, 128
EARLY, LAST = 1, 4


def dot_t(a, b):
    return lax.dot_general(a, b, (((1,), (1,)), ((), ())), preferred_element_type=F32)


def dot(a, b):
    return lax.dot_general(a, b, (((1,), (0,)), ((), ())), preferred_element_type=F32)


def tile(n, start=0):
    return slice(start + n * C, start + (n + 1) * C)


def kernel(
    x_h, dy_h, gate_h, up_h, wg_h, wu_h, wd_h,
    dx, dwg, dwu, dwd,
    xv, acts, wgu, wd, dgu, hid, xt,
    own_s, tsend_s, trecv_s, psend_s, precv_s, own_b, tsend_b, trecv_b, psend_b, precv_b, extra,
    load_sem, sent, landed, term_sem, part_sem, final_sem, extra_sem,
):
    rows, d = xv.shape
    f = wd.shape[0]
    half = rows // 2
    dyv, gv, uv = acts.at[:, 0:d], acts.at[:, d : d + f], acts.at[:, d + f : d + 2 * f]
    me = lax.axis_index("tp")
    chip, core = me // 2, me % 2
    partner, peer, across = chip * 2 + (1 - core), (1 - chip) * 2 + core, (1 - chip) * 2 + (1 - core)
    nb = (half - SMALL * 2 * RS) // (2 * RB)
    small = types.SimpleNamespace(
        r=RS, off=0, n=SMALL, at=0, own=own_s, tsend=tsend_s, trecv=trecv_s, psend=psend_s, precv=precv_s
    )
    big = types.SimpleNamespace(
        r=RB, off=SMALL * 2 * RS, n=nb, at=SMALL, own=own_b, tsend=tsend_b, trecv=trecv_b, psend=psend_b, precv=precv_b
    )

    def base(q, e):
        owner = lax.rem(chip + 1 + e // q.n, 2)
        return pl.multiple_of(owner * half + q.off + lax.rem(e, q.n) * (2 * q.r), 2 * RS)

    def block(q, e, k):
        return pl.ds(pl.multiple_of(base(q, e) + k * q.r, RS), q.r)

    def local(src, dst, sem):
        return pltpu.make_async_copy(src, dst, load_sem.at[sem])

    def load(q, e, sem):
        r = pl.ds(base(q, e), 2 * q.r)
        return [local(src.at[r], dst.at[r], sem) for src, dst in ((dy_h, dyv), (gate_h, gv), (up_h, uv))]

    def all_of(ref, sem):
        return pltpu.make_async_copy(ref, ref, sem)

    def remote(src, dst, send, recv, to):
        return pltpu.make_async_remote_copy(
            src_ref=src, dst_ref=dst, send_sem=send, recv_sem=recv, device_id={"tp": to}, device_id_type=MESH
        )

    def term_copy(q, e, cols=slice(None), n=0):
        recv = term_sem.at[2 * (2 * q.at + e) + n]
        return remote(q.tsend.at[e, :, cols], q.trecv.at[e, :, cols], sent.at[0], recv, partner)

    def part_copy(q, e, cols=slice(None)):
        return remote(q.psend.at[e, :, cols], q.precv.at[e, :, cols], sent.at[1], part_sem.at[q.at + e], peer)

    def extra_copy():
        return remote(tsend_s.at[0, :, tile(0)], extra, sent.at[0], extra_sem, across)

    def final_copy(q, j):
        r = block(q, q.n + j, core)
        return remote(dx.at[r], dx.at[r], sent.at[2], final_sem.at[q.at + j], peer)

    def core_copy(r):
        return remote(dx.at[r], dx.at[r], sent.at[3], landed, partner)

    def start(copies):
        for c in copies:
            c.start()

    def hidden_tile(q, e, n, dyb):
        dh = dot_t(dyb, wd[tile(n), :])
        for part, k in ((dh[: q.r], 1 - core), (dh[q.r :], core)):
            r = block(q, e, k)
            g, u = gv[r, tile(n)].astype(F32), uv[r, tile(n)].astype(F32)
            sig = jax.nn.sigmoid(g)
            act = g * sig
            hid[r, tile(n)] = (act * u).astype(BF16)
            dgu[r, tile(n)] = ((part * u) * (sig + act * (1.0 - sig))).astype(BF16)
            dgu[r, tile(n, f)] = (part * act).astype(BF16)

    def both(ref, q, e):
        return jnp.concatenate([ref[block(q, e, 1 - core), :], ref[block(q, e, core), :]], axis=0)

    def hidden_part(q, e):
        dyb = both(dyv, q, e)
        for n in range(f // C):
            hidden_tile(q, e, n, dyb)

    def term_tile(q, e, n, lhs):
        t = dot_t(lhs, wgu[tile(n), :])
        q.tsend[e, :, tile(n)] = t[: q.r].astype(BF16)
        q.own[e, :, tile(n)] = t[q.r :]

    def term_part(q, e):
        lhs = both(dgu, q, e)
        for n in range(d // C):
            term_tile(q, e, n, lhs)
        term_copy(q, e).start()

    def chip_sum(q, e, theirs, cols=slice(None), n=0):
        term_copy(q, e, cols, n).wait_recv()
        s = q.own[e, :, cols] + q.trecv[e, :, cols].astype(F32)
        if theirs:
            q.psend[e, :, cols] = s.astype(BF16)
            part_copy(q, e, cols).start()
        else:
            q.own[e, :, cols] = s

    def finish(q, j):
        part_copy(q, j).wait_recv()
        r = block(q, q.n + j, core)
        total = q.own[q.n + j] + q.precv[j].astype(F32)
        if q is small and j == 0:
            extra_copy().wait_recv()
            dx[r, C:] = total[:, C:].astype(BF16)
            dx[r, :C] = (total[:, :C] + extra[...].astype(F32)).astype(BF16)
        else:
            dx[r, :] = total.astype(BF16)
        if q is big and j == 0:
            final_copy(q, j).start()
        else:

            @pl.when(core != EARLY)
            def _():
                final_copy(q, j).start()

        core_copy(r).start()

    def pass_on(q, j):
        final_copy(q, j).wait_recv()
        core_copy(block(q, j, core)).start()

    def grad_x(m):
        r = pl.ds(pl.multiple_of(m * C, C), C)
        xt[...] = xv[:, r].T
        for n in range(f // C):
            dwg[r, tile(n)] = dot(xt[...], dgu[:, tile(n)]).astype(BF16)
            dwu[r, tile(n)] = dot(xt[...], dgu[:, tile(n, f)]).astype(BF16)

    def grad_h(m):
        r = pl.ds(pl.multiple_of(m * C, C), C)
        xt[...] = hid[:, r].T
        for n in range(d // C):
            dwd[r, tile(n)] = dot(xt[...], dyv[:, tile(n)]).astype(BF16)

    nf, nd = f // C, d // C
    w_sem, first_rows, gu, second_rows, rest, x_sem = 0, 1, 2, 4, 5, 6
    first = load(small, 0, first_rows)
    wds = [local(wd_h.at[tile(n)], wd.at[tile(n)], w_sem) for n in range(nf)]
    start(first[:1] + wds[:1] + first[1:] + wds[1:])
    for n in range(nd):
        start([local(w.at[tile(n)], wgu.at[tile(n), c * f : (c + 1) * f], gu + n // 2) for c, w in enumerate((wg_h, wu_h))])
    start(load(small, 1, second_rows))
    for e in range(2 * nb):
        start(load(big, e, rest))
    for e in range(SMALL, 2 * SMALL):
        start(load(small, e, rest))
    x_copy = local(x_h, xv, x_sem)
    start([x_copy])

    barrier = pltpu.get_barrier_semaphore()
    for to in (partner, peer, across):
        pl.semaphore_signal(barrier, inc=1, device_id={"tp": to}, device_id_type=MESH)

    all_of(acts.at[pl.ds(base(small, 0), 2 * RS)], load_sem.at[first_rows]).wait()
    all_of(wd, load_sem.at[w_sem]).wait()
    hidden_part(small, 0)
    pl.semaphore_wait(barrier, 3)
    halves = [slice(n * (d // 2), (n + 1) * (d // 2)) for n in range(2)]

    def halves_of_term(q, e):
        lhs = both(dgu, q, e)
        for n in range(2):
            if q is small and e == 0:
                all_of(wgu.at[halves[n]], load_sem.at[gu + n]).wait()
            for m in range(nd // 2):
                term_tile(q, e, n * (nd // 2) + m, lhs)
            cols = halves[n]
            if q is small and e == 0 and n == 0:
                psend_s[0, :, tile(0)] = own_s[0, :, tile(0)].astype(BF16)
                part_copy(small, 0, tile(0)).start()
                extra_copy().start()
                cols = rest_cols
            term_copy(q, e, cols, n).start()

    rest_cols = slice(C, d // 2)
    halves_of_term(small, 0)
    all_of(acts.at[pl.ds(base(small, 1), 2 * RS)], load_sem.at[second_rows]).wait()
    hidden_part(small, 1)
    chip_sum(small, 0, True, rest_cols, 0)
    chip_sum(small, 0, True, halves[1], 1)
    halves_of_term(small, 1)
    chip_sum(small, 1, True, halves[0], 0)
    all_of(acts.at[0 : rows - SMALL * 2 * RS], load_sem.at[rest]).wait()
    hidden_part(big, 0)
    chip_sum(small, 1, True, halves[1], 1)
    halves_of_term(big, 0)

    @pl.loop(1, 2 * nb)
    def _(e):
        hidden_part(big, e)

        @pl.when(e == 1)
        def _():
            for n in range(2):
                chip_sum(big, 0, True, halves[n], n)

        term_part(big, e)

        @pl.when((e > 1) & (e <= nb))
        def _():
            chip_sum(big, e - 1, True)

        @pl.when(e > nb)
        def _():
            chip_sum(big, e - 1, False)

    for e in range(SMALL, 2 * SMALL):
        hidden_part(small, e)
        term_part(small, e)
        if e == SMALL:
            chip_sum(big, 2 * nb - 1, False)
        else:
            chip_sum(small, e - 1, False)

    x_copy.wait()
    finish(big, 0)
    chip_sum(small, 2 * SMALL - 1, False)
    for j in range(SMALL):
        finish(small, j)
    for j in range(1, nb - 1):
        finish(big, j)

    @pl.loop(0, d // C)
    def _(m):
        grad_x(m)

    finish(big, nb - 1)

    @pl.loop(0, f // C)
    def _(m):
        grad_h(m)

        @pl.when(m == f // C - 2)
        def _():
            pass_on(big, 0)

    ahead = RB
    all_of(dx.at[0:half], sent.at[0]).wait()
    all_of(dx.at[0 : half // 2], sent.at[1]).wait()
    all_of(dx.at[0 : half // 2 + ahead], sent.at[3]).wait()
    all_of(dx.at[0 : half // 2 + ahead], landed).wait()

    @pl.when(core == EARLY)
    def _():
        all_of(dx.at[0:ahead], sent.at[2]).wait()

    @pl.when(core != EARLY)
    def _():
        for q in (small, big):
            for j in range(1 if q is big else 0, q.n):
                final_copy(q, j).wait_recv()
        all_of(dx.at[0 : half // 2], sent.at[2]).wait()


def rest_kernel(_, dx, recv, direct, ready, sent, landed):
    half = dx.shape[0] // 2
    me = lax.axis_index("tp")
    chip, core = me // 2, me % 2
    partner, peer, across = chip * 2 + (1 - core), (1 - chip) * 2 + core, (1 - chip) * 2 + (1 - core)
    big = [(SMALL * 2 * RS + j * 2 * RB, RB, 0, RB) for j in range(1, (half - SMALL * 2 * RS) // (2 * RB))]
    small = [(j * 2 * RS, RS, 0, RS) for j in range(SMALL - 1)]
    last = [((SMALL - 1) * 2 * RS, RS, n * RS // LAST, RS // LAST) for n in range(LAST)]
    pieces = big + small + last

    def rows(owner, piece):
        at, r, off, size = piece
        return pl.ds(pl.multiple_of(owner * half + at + core * r + off, size), size)

    def copy(r, send, recv, to):
        return pltpu.make_async_remote_copy(
            src_ref=dx.at[r], dst_ref=dx.at[r], send_sem=send, recv_sem=recv, device_id={"tp": to}, device_id_type=MESH
        )

    def final_copy(n):
        return copy(rows(chip, pieces[n]), sent.at[0], recv.at[n], peer)

    def core_copy(n):
        return copy(rows(1 - chip, pieces[n]), sent.at[1], landed, partner)

    end = len(pieces) - 1
    direct_copy = copy(rows(chip, pieces[end]), sent.at[0], direct, across)

    def all_of(n, sem):
        return pltpu.make_async_copy(dx.at[0:n], dx.at[0:n], sem)

    size = pieces[end][3]
    passes = half // 2 - RB
    barrier = pltpu.get_barrier_semaphore()

    @pl.when(core == EARLY)
    def _():
        for to in (peer, partner, across):
            pl.semaphore_signal(barrier, inc=1, device_id={"tp": to}, device_id_type=MESH)

    pl.semaphore_wait(barrier, 1 + lax.rem(core + EARLY, 2))

    @pl.when(core == EARLY)
    def _():
        for n in range(end):
            final_copy(n).start()
        pl.semaphore_wait(ready, 2)
        direct_copy.start()
        final_copy(end).start()
        for n in range(len(pieces)):
            final_copy(n).wait_recv()
            if n < end:
                core_copy(n).start()
        all_of(passes + size, sent.at[0]).wait()
        all_of(passes - size, sent.at[1]).wait()
        all_of(passes, landed).wait()

    @pl.when(core != EARLY)
    def _():
        for to in (partner, across):
            pl.semaphore_signal(ready, inc=1, device_id={"tp": to}, device_id_type=MESH)
        for n in range(len(pieces)):
            core_copy(n).start()
        all_of(passes, sent.at[1]).wait()
        all_of(passes - size, landed).wait()
        direct_copy.wait_recv()


def start_all(pairs, sem):
    copies = [pltpu.make_async_copy(a, b, sem) for a, b in pairs]
    for c in copies:
        c.start()
    return copies


def wait_all(copies):
    for c in copies:
        c.wait()


def rows_of(dx):
    half = dx.shape[0] // 2
    chip = lax.axis_index("tp") // 2
    first = SMALL * 2 * RS
    own = [(chip * half + n * (half // 2), half // 2) for n in range(2)]
    theirs = (1 - chip) * half
    steps = [(theirs + n * 2 * RS, RS) for n in range(SMALL)]
    steps += [(theirs + n, RB) for n in range(first + 2 * RB, half, 2 * RB)]

    def slices(parts):
        return [pl.ds(pl.multiple_of(at, RS), size) for at, size in parts]

    late, early = ([(at + k * size, size) for at, size in steps] for k in (1 - EARLY, EARLY))
    return slices(own + [(theirs + first, 2 * RB)]), slices(late), slices(early)


def write_most(dx_v, dwg_v, dwu_v, dwd_v, _, dx, dwg, dwu, dwd, sem):
    done, late, _ = rows_of(dx)
    pairs = [(dx_v.at[r], dx.at[r]) for r in done]
    for src, dst in ((dwg_v, dwg), (dwu_v, dwu), (dwd_v, dwd)):
        n = src.shape[0] // 2
        pairs += [(src.at[r], dst.at[r]) for r in (pl.ds(0, n), pl.ds(n, n))]
    copies = start_all(pairs, sem)

    @pl.when(lax.rem(lax.axis_index("tp"), 2) != EARLY)
    def _():
        wait_all(start_all([(dx_v.at[r], dx.at[r]) for r in late], sem))

    wait_all(copies)


def write_late(dx_v, _, dx, sem):
    _, late, early = rows_of(dx)
    copies = start_all([(dx_v.at[r], dx.at[r]) for r in early], sem)

    @pl.when(lax.rem(lax.axis_index("tp"), 2) == EARLY)
    def _():
        wait_all(start_all([(dx_v.at[r], dx.at[r]) for r in late], sem))

    wait_all(copies)


def solution(mesh):
    def step(x, dy, gate, up, w_gate, w_up, w_down):
        rows, d = x.shape
        f = gate.shape[1]
        nb = (rows // 2 - SMALL * 2 * RS) // (2 * RB)
        outs = [((rows, d), BF16), ((d, f), BF16), ((d, f), BF16), ((f, d), BF16)]
        dma = pltpu.SemaphoreType.DMA

        def buffers(n, r):
            shapes = ((2 * n, F32), (2 * n, BF16), (2 * n, BF16), (n, BF16), (n, BF16))
            return [pltpu.VMEM((m, r, d), t) for m, t in shapes]

        dx, *grads = pl.pallas_call(
            kernel,
            out_shape=[pltpu.VMEM(s, t) for s, t in outs],
            in_specs=[pl.BlockSpec(memory_space=pl.ANY)] * 7,
            out_specs=[pl.BlockSpec(memory_space=pltpu.VMEM)] * 4,
            scratch_shapes=[
                pltpu.VMEM((rows, d), BF16),
                pltpu.VMEM((rows, d + 2 * f), BF16),
                pltpu.VMEM((d, 2 * f), BF16),
                pltpu.VMEM((f, d), BF16),
                pltpu.VMEM((rows, 2 * f), BF16),
                pltpu.VMEM((rows, f), BF16),
                pltpu.VMEM((C, rows), BF16),
            ]
            + buffers(SMALL, RS)
            + buffers(nb, RB)
            + [
                pltpu.VMEM((RS, C), BF16),
                dma((7,)),
                dma((4,)),
                dma(()),
                dma((4 * (SMALL + nb),)),
                dma((SMALL + nb,)),
                dma((SMALL + nb,)),
                dma(()),
            ],
            compiler_params=pltpu.CompilerParams(
                collective_id=0, has_side_effects=True, vmem_limit_bytes=50 * 2**20
            ),
            name="block",
        )(x, dy, gate, up, w_gate, w_up, w_down)
        held, plain = pl.BlockSpec(memory_space=pltpu.VMEM), pl.BlockSpec(memory_space=pl.ANY)
        shapes = [jax.ShapeDtypeStruct(s, t) for s, t in outs]
        little = 2**20

        def pin(a):
            return pltpu.with_memory_space_constraint(a, pltpu.VMEM)

        dx, most, *grads = pl.pallas_call(
            write_most,
            out_shape=[pltpu.VMEM(*outs[0])] + shapes,
            in_specs=[plain] + [held] * 3,
            out_specs=[plain] * 5,
            scratch_shapes=[dma(())],
            input_output_aliases={0: 0},
            compiler_params=pltpu.CompilerParams(vmem_limit_bytes=little),
            name="write_most",
        )(pin(dx), *(pin(g) for g in grads))
        dx = pl.pallas_call(
            rest_kernel,
            out_shape=pltpu.VMEM(*outs[0]),
            in_specs=[plain],
            out_specs=plain,
            scratch_shapes=[
                dma((nb + SMALL - 2 + LAST,)), dma(()), pltpu.SemaphoreType.REGULAR, dma((2,)), dma(())
            ],
            input_output_aliases={0: 0},
            compiler_params=pltpu.CompilerParams(collective_id=1, has_side_effects=True, vmem_limit_bytes=little),
            name="rest",
        )(pin(dx))
        dx = pl.pallas_call(
            write_late,
            out_shape=shapes[0],
            in_specs=[held, plain],
            out_specs=plain,
            scratch_shapes=[dma(())],
            input_output_aliases={1: 0},
            compiler_params=pltpu.CompilerParams(vmem_limit_bytes=little),
            name="write_late",
        )(pin(dx), most)
        return dx, *grads

    tokens, columns, rows = P("dp", None), P(None, "tp"), P("tp", None)
    return jax.shard_map(
        step,
        mesh=mesh,
        in_specs=(tokens, tokens, P("dp", "tp"), P("dp", "tp"), columns, columns, rows),
        out_specs=(tokens, P("dp", "tp"), P("dp", "tp"), P(("dp", "tp"), None)),
        check_vma=False,
    )
```

```python
import types

import jax
import jax.numpy as jnp
from jax import lax
from jax.experimental import pallas as pl
from jax.experimental.pallas import tpu as pltpu
from jax.sharding import PartitionSpec as P

MESH = pl.DeviceIdType.MESH
F32, BF16 = jnp.float32, jnp.bfloat16
C = 256
SMALL, RS, RB = 2, 64, 128
EARLY, LAST = 1, (16, 24, 24)


def dot_t(a, b):
    return lax.dot_general(a, b, (((1,), (1,)), ((), ())), preferred_element_type=F32)


def dot(a, b):
    return lax.dot_general(a, b, (((1,), (0,)), ((), ())), preferred_element_type=F32)


def tile(n, start=0):
    return slice(start + n * C, start + (n + 1) * C)


def kernel(
    x_h, dy_h, gate_h, up_h, wg_h, wu_h, wd_h,
    dx, dwg, dwu, dwd,
    xv, acts, wgu, wd, dgu, hid, xt,
    own_s, tsend_s, trecv_s, psend_s, precv_s, own_b, tsend_b, trecv_b, psend_b, precv_b, extra,
    load_sem, sent, landed, term_sem, part_sem, final_sem, extra_sem,
):
    rows, d = xv.shape
    f = wd.shape[0]
    half = rows // 2
    dyv, gv, uv = acts.at[:, 0:d], acts.at[:, d : d + f], acts.at[:, d + f : d + 2 * f]
    me = lax.axis_index("tp")
    chip, core = me // 2, me % 2
    partner, peer, across = chip * 2 + (1 - core), (1 - chip) * 2 + core, (1 - chip) * 2 + (1 - core)
    nb = (half - SMALL * 2 * RS) // (2 * RB)
    small = types.SimpleNamespace(
        r=RS, off=0, n=SMALL, at=0, own=own_s, tsend=tsend_s, trecv=trecv_s, psend=psend_s, precv=precv_s
    )
    big = types.SimpleNamespace(
        r=RB, off=SMALL * 2 * RS, n=nb, at=SMALL, own=own_b, tsend=tsend_b, trecv=trecv_b, psend=psend_b, precv=precv_b
    )

    def base(q, e):
        owner = lax.rem(chip + 1 + e // q.n, 2)
        return pl.multiple_of(owner * half + q.off + lax.rem(e, q.n) * (2 * q.r), 2 * RS)

    def block(q, e, k):
        return pl.ds(pl.multiple_of(base(q, e) + k * q.r, RS), q.r)

    def local(src, dst, sem):
        return pltpu.make_async_copy(src, dst, load_sem.at[sem])

    def load(q, e, sem):
        r = pl.ds(base(q, e), 2 * q.r)
        return [local(src.at[r], dst.at[r], sem) for src, dst in ((dy_h, dyv), (gate_h, gv), (up_h, uv))]

    def all_of(ref, sem):
        return pltpu.make_async_copy(ref, ref, sem)

    def remote(src, dst, send, recv, to):
        return pltpu.make_async_remote_copy(
            src_ref=src, dst_ref=dst, send_sem=send, recv_sem=recv, device_id={"tp": to}, device_id_type=MESH
        )

    def term_copy(q, e, cols=slice(None), n=0):
        recv = term_sem.at[2 * (2 * q.at + e) + n]
        return remote(q.tsend.at[e, :, cols], q.trecv.at[e, :, cols], sent.at[0], recv, partner)

    def part_copy(q, e, cols=slice(None)):
        return remote(q.psend.at[e, :, cols], q.precv.at[e, :, cols], sent.at[1], part_sem.at[q.at + e], peer)

    def extra_copy():
        return remote(tsend_s.at[0, :, tile(0)], extra, sent.at[0], extra_sem, across)

    def final_copy(q, j):
        r = block(q, q.n + j, core)
        return remote(dx.at[r], dx.at[r], sent.at[2], final_sem.at[q.at + j], peer)

    def core_copy(r):
        return remote(dx.at[r], dx.at[r], sent.at[3], landed, partner)

    def start(copies):
        for c in copies:
            c.start()

    def hidden_tile(q, e, n, dyb):
        dh = dot_t(dyb, wd[tile(n), :])
        for part, k in ((dh[: q.r], 1 - core), (dh[q.r :], core)):
            r = block(q, e, k)
            g, u = gv[r, tile(n)].astype(F32), uv[r, tile(n)].astype(F32)
            sig = jax.nn.sigmoid(g)
            act = g * sig
            hid[r, tile(n)] = (act * u).astype(BF16)
            dgu[r, tile(n)] = ((part * u) * (sig + act * (1.0 - sig))).astype(BF16)
            dgu[r, tile(n, f)] = (part * act).astype(BF16)

    def both(ref, q, e):
        return jnp.concatenate([ref[block(q, e, 1 - core), :], ref[block(q, e, core), :]], axis=0)

    def hidden_part(q, e):
        dyb = both(dyv, q, e)
        for n in range(f // C):
            hidden_tile(q, e, n, dyb)

    def term_tile(q, e, n, lhs):
        t = dot_t(lhs, wgu[tile(n), :])
        q.tsend[e, :, tile(n)] = t[: q.r].astype(BF16)
        q.own[e, :, tile(n)] = t[q.r :]

    def term_part(q, e):
        lhs = both(dgu, q, e)
        for n in range(d // C):
            term_tile(q, e, n, lhs)
        term_copy(q, e).start()

    def chip_sum(q, e, theirs, cols=slice(None), n=0):
        term_copy(q, e, cols, n).wait_recv()
        s = q.own[e, :, cols] + q.trecv[e, :, cols].astype(F32)
        if theirs:
            q.psend[e, :, cols] = s.astype(BF16)
            part_copy(q, e, cols).start()
        else:
            q.own[e, :, cols] = s

    def finish(q, j):
        part_copy(q, j).wait_recv()
        r = block(q, q.n + j, core)
        total = q.own[q.n + j] + q.precv[j].astype(F32)
        if q is small and j == 0:
            extra_copy().wait_recv()
            dx[r, C:] = total[:, C:].astype(BF16)
            dx[r, :C] = (total[:, :C] + extra[...].astype(F32)).astype(BF16)
        else:
            dx[r, :] = total.astype(BF16)
        if q is big and j == 0:
            final_copy(q, j).start()
        else:

            @pl.when(core != EARLY)
            def _():
                final_copy(q, j).start()

        core_copy(r).start()

    def pass_on(q, j):
        final_copy(q, j).wait_recv()
        core_copy(block(q, j, core)).start()

    def grad_x(m):
        r = pl.ds(pl.multiple_of(m * C, C), C)
        xt[...] = xv[:, r].T
        for n in range(f // C):
            dwg[r, tile(n)] = dot(xt[...], dgu[:, tile(n)]).astype(BF16)
            dwu[r, tile(n)] = dot(xt[...], dgu[:, tile(n, f)]).astype(BF16)

    def grad_h(m):
        r = pl.ds(pl.multiple_of(m * C, C), C)
        xt[...] = hid[:, r].T
        for n in range(d // C):
            dwd[r, tile(n)] = dot(xt[...], dyv[:, tile(n)]).astype(BF16)

    nf, nd = f // C, d // C
    w_sem, first_rows, gu, second_rows, rest, x_sem = 0, 1, 2, 4, 5, 6
    first = load(small, 0, first_rows)
    wds = [local(wd_h.at[tile(n)], wd.at[tile(n)], w_sem) for n in range(nf)]
    start(first[:1] + wds[:1] + first[1:] + wds[1:])
    for n in range(nd):
        start([local(w.at[tile(n)], wgu.at[tile(n), c * f : (c + 1) * f], gu + n // 2) for c, w in enumerate((wg_h, wu_h))])
    start(load(small, 1, second_rows))
    for e in range(2 * nb):
        start(load(big, e, rest))
    for e in range(SMALL, 2 * SMALL):
        start(load(small, e, rest))
    x_copy = local(x_h, xv, x_sem)
    start([x_copy])

    barrier = pltpu.get_barrier_semaphore()
    for to in (partner, peer, across):
        pl.semaphore_signal(barrier, inc=1, device_id={"tp": to}, device_id_type=MESH)

    all_of(acts.at[pl.ds(base(small, 0), 2 * RS)], load_sem.at[first_rows]).wait()
    all_of(wd, load_sem.at[w_sem]).wait()
    hidden_part(small, 0)
    pl.semaphore_wait(barrier, 3)
    halves = [slice(n * (d // 2), (n + 1) * (d // 2)) for n in range(2)]

    def halves_of_term(q, e):
        lhs = both(dgu, q, e)
        for n in range(2):
            if q is small and e == 0:
                all_of(wgu.at[halves[n]], load_sem.at[gu + n]).wait()
            for m in range(nd // 2):
                term_tile(q, e, n * (nd // 2) + m, lhs)
            cols = halves[n]
            if q is small and e == 0 and n == 0:
                psend_s[0, :, tile(0)] = own_s[0, :, tile(0)].astype(BF16)
                part_copy(small, 0, tile(0)).start()
                extra_copy().start()
                cols = rest_cols
            term_copy(q, e, cols, n).start()

    rest_cols = slice(C, d // 2)
    halves_of_term(small, 0)
    all_of(acts.at[pl.ds(base(small, 1), 2 * RS)], load_sem.at[second_rows]).wait()
    hidden_part(small, 1)
    chip_sum(small, 0, True, rest_cols, 0)
    chip_sum(small, 0, True, halves[1], 1)
    halves_of_term(small, 1)
    chip_sum(small, 1, True, halves[0], 0)
    all_of(acts.at[0 : rows - SMALL * 2 * RS], load_sem.at[rest]).wait()
    hidden_part(big, 0)
    chip_sum(small, 1, True, halves[1], 1)
    halves_of_term(big, 0)

    @pl.loop(1, 2 * nb)
    def _(e):
        hidden_part(big, e)

        @pl.when(e == 1)
        def _():
            for n in range(2):
                chip_sum(big, 0, True, halves[n], n)

        term_part(big, e)

        @pl.when((e > 1) & (e <= nb))
        def _():
            chip_sum(big, e - 1, True)

        @pl.when(e > nb)
        def _():
            chip_sum(big, e - 1, False)

    for e in range(SMALL, 2 * SMALL):
        hidden_part(small, e)
        term_part(small, e)
        if e == SMALL:
            chip_sum(big, 2 * nb - 1, False)
        else:
            chip_sum(small, e - 1, False)

    x_copy.wait()
    finish(big, 0)
    chip_sum(small, 2 * SMALL - 1, False)
    for j in range(SMALL):
        finish(small, j)
    for j in range(1, nb - 1):
        finish(big, j)

    @pl.loop(0, d // C)
    def _(m):
        grad_x(m)

    finish(big, nb - 1)

    @pl.loop(0, f // C)
    def _(m):
        grad_h(m)

        @pl.when(m == f // C - 2)
        def _():
            pass_on(big, 0)

    ahead = RB
    all_of(dx.at[0:half], sent.at[0]).wait()
    all_of(dx.at[0 : half // 2], sent.at[1]).wait()
    all_of(dx.at[0 : half // 2 + ahead], sent.at[3]).wait()
    all_of(dx.at[0 : half // 2 + ahead], landed).wait()

    @pl.when(core == EARLY)
    def _():
        all_of(dx.at[0:ahead], sent.at[2]).wait()

    @pl.when(core != EARLY)
    def _():
        for q in (small, big):
            for j in range(1 if q is big else 0, q.n):
                final_copy(q, j).wait_recv()
        all_of(dx.at[0 : half // 2], sent.at[2]).wait()


def rest_kernel(_, dx, recv, ready, sent, landed):
    half = dx.shape[0] // 2
    me = lax.axis_index("tp")
    chip, core = me // 2, me % 2
    partner, peer, across = chip * 2 + (1 - core), (1 - chip) * 2 + core, (1 - chip) * 2 + (1 - core)
    big = [(SMALL * 2 * RS + j * 2 * RB, RB, 0, RB) for j in range(1, (half - SMALL * 2 * RS) // (2 * RB))]
    small = [(j * 2 * RS, RS, 0, RS) for j in range(SMALL - 1)]
    last = [((SMALL - 1) * 2 * RS, RS, sum(LAST[:n]), size) for n, size in enumerate(LAST)]
    pieces = big + small + last

    def rows(owner, piece):
        at, r, off, size = piece
        return pl.ds(pl.multiple_of(owner * half + at + core * r + off, 8), size)

    def copy(r, send, recv, to):
        return pltpu.make_async_remote_copy(
            src_ref=dx.at[r], dst_ref=dx.at[r], send_sem=send, recv_sem=recv, device_id={"tp": to}, device_id_type=MESH
        )

    def final_copy(n):
        return copy(rows(chip, pieces[n]), sent, recv.at[n], peer)

    def core_copy(n):
        return copy(rows(1 - chip, pieces[n]), sent, landed, partner)

    end = len(pieces) - 1
    direct_copy = copy(rows(chip, pieces[end]), sent, landed, across)

    def all_of(n, sem):
        return pltpu.make_async_copy(dx.at[0:n], dx.at[0:n], sem)

    passes = half // 2 - RB
    barrier = pltpu.get_barrier_semaphore()

    @pl.when(core == EARLY)
    def _():
        for to in (peer, partner, across):
            pl.semaphore_signal(barrier, inc=1, device_id={"tp": to}, device_id_type=MESH)

    pl.semaphore_wait(barrier, 1 + lax.rem(core + EARLY, 2))

    @pl.when(core == EARLY)
    def _():
        for n in range(end):
            final_copy(n).start()
        pl.semaphore_wait(ready, 2)
        direct_copy.start()
        final_copy(end).start()
        for n in range(len(pieces)):
            final_copy(n).wait_recv()
            if n < end:
                core_copy(n).start()
        all_of(2 * passes, sent).wait()

    @pl.when(core != EARLY)
    def _():
        for to in (partner, across):
            pl.semaphore_signal(ready, inc=1, device_id={"tp": to}, device_id_type=MESH)
        for n in range(len(pieces)):
            core_copy(n).start()
        all_of(passes, sent).wait()

    all_of(passes, landed).wait()


def start_all(pairs, sem):
    copies = [pltpu.make_async_copy(a, b, sem) for a, b in pairs]
    for c in copies:
        c.start()
    return copies


def wait_all(copies):
    for c in copies:
        c.wait()


def rows_of(dx):
    half = dx.shape[0] // 2
    chip = lax.axis_index("tp") // 2
    first = SMALL * 2 * RS
    own = [(chip * half + n * (half // 2), half // 2) for n in range(2)]
    theirs = (1 - chip) * half
    steps = [(theirs + n * 2 * RS, RS) for n in range(SMALL)]
    steps += [(theirs + n, RB) for n in range(first + 2 * RB, half, 2 * RB)]

    def slices(parts):
        return [pl.ds(pl.multiple_of(at, RS), size) for at, size in parts]

    late, early = ([(at + k * size, size) for at, size in steps] for k in (1 - EARLY, EARLY))
    return slices(own + [(theirs + first, 2 * RB)]), slices(late), slices(early)


def write_most(dx_v, dwg_v, dwu_v, dwd_v, _, dx, dwg, dwu, dwd, sem):
    done, late, _ = rows_of(dx)
    pairs = [(dx_v.at[r], dx.at[r]) for r in done]
    for src, dst in ((dwg_v, dwg), (dwu_v, dwu), (dwd_v, dwd)):
        n = src.shape[0] // 2
        pairs += [(src.at[r], dst.at[r]) for r in (pl.ds(0, n), pl.ds(n, n))]
    copies = start_all(pairs, sem)

    @pl.when(lax.rem(lax.axis_index("tp"), 2) != EARLY)
    def _():
        wait_all(start_all([(dx_v.at[r], dx.at[r]) for r in late], sem))

    wait_all(copies)


def write_late(dx_v, _, dx, sem):
    _, late, early = rows_of(dx)
    copies = start_all([(dx_v.at[r], dx.at[r]) for r in early], sem)

    @pl.when(lax.rem(lax.axis_index("tp"), 2) == EARLY)
    def _():
        wait_all(start_all([(dx_v.at[r], dx.at[r]) for r in late], sem))

    wait_all(copies)


def solution(mesh):
    def step(x, dy, gate, up, w_gate, w_up, w_down):
        rows, d = x.shape
        f = gate.shape[1]
        nb = (rows // 2 - SMALL * 2 * RS) // (2 * RB)
        outs = [((rows, d), BF16), ((d, f), BF16), ((d, f), BF16), ((f, d), BF16)]
        dma = pltpu.SemaphoreType.DMA

        def buffers(n, r):
            shapes = ((2 * n, F32), (2 * n, BF16), (2 * n, BF16), (n, BF16), (n, BF16))
            return [pltpu.VMEM((m, r, d), t) for m, t in shapes]

        dx, *grads = pl.pallas_call(
            kernel,
            out_shape=[pltpu.VMEM(s, t) for s, t in outs],
            in_specs=[pl.BlockSpec(memory_space=pl.ANY)] * 7,
            out_specs=[pl.BlockSpec(memory_space=pltpu.VMEM)] * 4,
            scratch_shapes=[
                pltpu.VMEM((rows, d), BF16),
                pltpu.VMEM((rows, d + 2 * f), BF16),
                pltpu.VMEM((d, 2 * f), BF16),
                pltpu.VMEM((f, d), BF16),
                pltpu.VMEM((rows, 2 * f), BF16),
                pltpu.VMEM((rows, f), BF16),
                pltpu.VMEM((C, rows), BF16),
            ]
            + buffers(SMALL, RS)
            + buffers(nb, RB)
            + [
                pltpu.VMEM((RS, C), BF16),
                dma((7,)),
                dma((4,)),
                dma(()),
                dma((4 * (SMALL + nb),)),
                dma((SMALL + nb,)),
                dma((SMALL + nb,)),
                dma(()),
            ],
            compiler_params=pltpu.CompilerParams(
                collective_id=0, has_side_effects=True, vmem_limit_bytes=50 * 2**20
            ),
            name="block",
        )(x, dy, gate, up, w_gate, w_up, w_down)
        held, plain = pl.BlockSpec(memory_space=pltpu.VMEM), pl.BlockSpec(memory_space=pl.ANY)
        shapes = [jax.ShapeDtypeStruct(s, t) for s, t in outs]
        little = 2**20

        def pin(a):
            return pltpu.with_memory_space_constraint(a, pltpu.VMEM)

        dx, most, *grads = pl.pallas_call(
            write_most,
            out_shape=[pltpu.VMEM(*outs[0])] + shapes,
            in_specs=[plain] + [held] * 3,
            out_specs=[plain] * 5,
            scratch_shapes=[dma(())],
            input_output_aliases={0: 0},
            compiler_params=pltpu.CompilerParams(vmem_limit_bytes=little),
            name="write_most",
        )(pin(dx), *(pin(g) for g in grads))
        dx = pl.pallas_call(
            rest_kernel,
            out_shape=pltpu.VMEM(*outs[0]),
            in_specs=[plain],
            out_specs=plain,
            scratch_shapes=[
                dma((nb + SMALL - 2 + len(LAST),)), pltpu.SemaphoreType.REGULAR, dma(()), dma(())
            ],
            input_output_aliases={0: 0},
            compiler_params=pltpu.CompilerParams(collective_id=1, has_side_effects=True, vmem_limit_bytes=little),
            name="rest",
        )(pin(dx))
        dx = pl.pallas_call(
            write_late,
            out_shape=shapes[0],
            in_specs=[held, plain],
            out_specs=plain,
            scratch_shapes=[dma(())],
            input_output_aliases={1: 0},
            compiler_params=pltpu.CompilerParams(vmem_limit_bytes=little),
            name="write_late",
        )(pin(dx), most)
        return dx, *grads

    tokens, columns, rows = P("dp", None), P(None, "tp"), P("tp", None)
    return jax.shard_map(
        step,
        mesh=mesh,
        in_specs=(tokens, tokens, P("dp", "tp"), P("dp", "tp"), columns, columns, rows),
        out_specs=(tokens, P("dp", "tp"), P("dp", "tp"), P(("dp", "tp"), None)),
        check_vma=False,
    )
```

```python
import types

import jax
import jax.numpy as jnp
from jax import lax
from jax.experimental import pallas as pl
from jax.experimental.pallas import tpu as pltpu
from jax.sharding import PartitionSpec as P

MESH = pl.DeviceIdType.MESH
F32, BF16 = jnp.float32, jnp.bfloat16
C = 256
SMALL, RS, RB = 2, 64, 128
EARLY, LAST = 1, (16, 24, 24)


def dot_t(a, b):
    return lax.dot_general(a, b, (((1,), (1,)), ((), ())), preferred_element_type=F32)


def dot(a, b):
    return lax.dot_general(a, b, (((1,), (0,)), ((), ())), preferred_element_type=F32)


def tile(n, start=0):
    return slice(start + n * C, start + (n + 1) * C)


def kernel(
    x_h, dy_h, gate_h, up_h, wg_h, wu_h, wd_h,
    dx, dwg, dwu, dwd,
    xv, acts, wgu, wd, dgu, hid, xt,
    own_s, tsend_s, trecv_s, psend_s, precv_s, own_b, tsend_b, trecv_b, psend_b, precv_b, extra,
    load_sem, sent, landed, term_sem, part_sem, final_sem, extra_sem,
):
    rows, d = xv.shape
    f = wd.shape[0]
    half = rows // 2
    dyv, gv, uv = acts.at[:, 0:d], acts.at[:, d : d + f], acts.at[:, d + f : d + 2 * f]
    me = lax.axis_index("tp")
    chip, core = me // 2, me % 2
    partner, peer, across = chip * 2 + (1 - core), (1 - chip) * 2 + core, (1 - chip) * 2 + (1 - core)
    nb = (half - SMALL * 2 * RS) // (2 * RB)
    small = types.SimpleNamespace(
        r=RS, off=0, n=SMALL, at=0, own=own_s, tsend=tsend_s, trecv=trecv_s, psend=psend_s, precv=precv_s
    )
    big = types.SimpleNamespace(
        r=RB, off=SMALL * 2 * RS, n=nb, at=SMALL, own=own_b, tsend=tsend_b, trecv=trecv_b, psend=psend_b, precv=precv_b
    )

    def base(q, e):
        owner = lax.rem(chip + 1 + e // q.n, 2)
        return pl.multiple_of(owner * half + q.off + lax.rem(e, q.n) * (2 * q.r), 2 * RS)

    def block(q, e, k):
        return pl.ds(pl.multiple_of(base(q, e) + k * q.r, RS), q.r)

    def local(src, dst, sem):
        return pltpu.make_async_copy(src, dst, load_sem.at[sem])

    def load(q, e, sem):
        r = pl.ds(base(q, e), 2 * q.r)
        return [local(src.at[r], dst.at[r], sem) for src, dst in ((dy_h, dyv), (gate_h, gv), (up_h, uv))]

    def all_of(ref, sem):
        return pltpu.make_async_copy(ref, ref, sem)

    def remote(src, dst, send, recv, to):
        return pltpu.make_async_remote_copy(
            src_ref=src, dst_ref=dst, send_sem=send, recv_sem=recv, device_id={"tp": to}, device_id_type=MESH
        )

    def term_copy(q, e, cols=slice(None), n=0):
        recv = term_sem.at[2 * (2 * q.at + e) + n]
        return remote(q.tsend.at[e, :, cols], q.trecv.at[e, :, cols], sent.at[0], recv, partner)

    def part_copy(q, e, cols=slice(None)):
        return remote(q.psend.at[e, :, cols], q.precv.at[e, :, cols], sent.at[1], part_sem.at[q.at + e], peer)

    def extra_copy():
        return remote(tsend_s.at[0, :, tile(0)], extra, sent.at[0], extra_sem, across)

    def final_copy(q, j):
        r = block(q, q.n + j, core)
        return remote(dx.at[r], dx.at[r], sent.at[2], final_sem.at[q.at + j], peer)

    def core_copy(r):
        return remote(dx.at[r], dx.at[r], sent.at[3], landed, partner)

    def start(copies):
        for c in copies:
            c.start()

    def hidden_tile(q, e, n, dyb):
        dh = dot_t(dyb, wd[tile(n), :])
        for part, k in ((dh[: q.r], 1 - core), (dh[q.r :], core)):
            r = block(q, e, k)
            g, u = gv[r, tile(n)].astype(F32), uv[r, tile(n)].astype(F32)
            sig = jax.nn.sigmoid(g)
            act = g * sig
            hid[r, tile(n)] = (act * u).astype(BF16)
            dgu[r, tile(n)] = ((part * u) * (sig + act * (1.0 - sig))).astype(BF16)
            dgu[r, tile(n, f)] = (part * act).astype(BF16)

    def both(ref, q, e):
        return jnp.concatenate([ref[block(q, e, 1 - core), :], ref[block(q, e, core), :]], axis=0)

    def hidden_part(q, e):
        dyb = both(dyv, q, e)
        for n in range(f // C):
            hidden_tile(q, e, n, dyb)

    def term_tile(q, e, n, lhs):
        t = dot_t(lhs, wgu[tile(n), :])
        q.tsend[e, :, tile(n)] = t[: q.r].astype(BF16)
        q.own[e, :, tile(n)] = t[q.r :]

    def term_part(q, e):
        lhs = both(dgu, q, e)
        for n in range(d // C):
            term_tile(q, e, n, lhs)
        term_copy(q, e).start()

    def chip_sum(q, e, theirs, cols=slice(None), n=0):
        term_copy(q, e, cols, n).wait_recv()
        s = q.own[e, :, cols] + q.trecv[e, :, cols].astype(F32)
        if theirs:
            q.psend[e, :, cols] = s.astype(BF16)
            part_copy(q, e, cols).start()
        else:
            q.own[e, :, cols] = s

    def finish(q, j):
        part_copy(q, j).wait_recv()
        r = block(q, q.n + j, core)
        total = q.own[q.n + j] + q.precv[j].astype(F32)
        if q is small and j == 0:
            extra_copy().wait_recv()
            dx[r, C:] = total[:, C:].astype(BF16)
            dx[r, :C] = (total[:, :C] + extra[...].astype(F32)).astype(BF16)
        else:
            dx[r, :] = total.astype(BF16)
        if j == 0:
            final_copy(q, j).start()
        else:

            @pl.when(core != EARLY)
            def _():
                final_copy(q, j).start()

        core_copy(r).start()

    def pass_on(q, j):
        final_copy(q, j).wait_recv()
        core_copy(block(q, j, core)).start()

    def grad_x(m):
        r = pl.ds(pl.multiple_of(m * C, C), C)
        xt[...] = xv[:, r].T
        for n in range(f // C):
            dwg[r, tile(n)] = dot(xt[...], dgu[:, tile(n)]).astype(BF16)
            dwu[r, tile(n)] = dot(xt[...], dgu[:, tile(n, f)]).astype(BF16)

    def grad_h(m):
        r = pl.ds(pl.multiple_of(m * C, C), C)
        xt[...] = hid[:, r].T
        for n in range(d // C):
            dwd[r, tile(n)] = dot(xt[...], dyv[:, tile(n)]).astype(BF16)

    nf, nd = f // C, d // C
    w_sem, first_rows, gu, second_rows, rest, x_sem = 0, 1, 2, 4, 5, 6
    first = load(small, 0, first_rows)
    wds = [local(wd_h.at[tile(n)], wd.at[tile(n)], w_sem) for n in range(nf)]
    start(first[:1] + wds[:1] + first[1:] + wds[1:])
    for n in range(nd):
        start([local(w.at[tile(n)], wgu.at[tile(n), c * f : (c + 1) * f], gu + n // 2) for c, w in enumerate((wg_h, wu_h))])
    start(load(small, 1, second_rows))
    for e in range(2 * nb):
        start(load(big, e, rest))
    for e in range(SMALL, 2 * SMALL):
        start(load(small, e, rest))
    x_copy = local(x_h, xv, x_sem)
    start([x_copy])

    barrier = pltpu.get_barrier_semaphore()
    for to in (partner, peer, across):
        pl.semaphore_signal(barrier, inc=1, device_id={"tp": to}, device_id_type=MESH)

    all_of(acts.at[pl.ds(base(small, 0), 2 * RS)], load_sem.at[first_rows]).wait()
    all_of(wd, load_sem.at[w_sem]).wait()
    hidden_part(small, 0)
    pl.semaphore_wait(barrier, 3)
    halves = [slice(n * (d // 2), (n + 1) * (d // 2)) for n in range(2)]

    def halves_of_term(q, e):
        lhs = both(dgu, q, e)
        for n in range(2):
            if q is small and e == 0:
                all_of(wgu.at[halves[n]], load_sem.at[gu + n]).wait()
            for m in range(nd // 2):
                term_tile(q, e, n * (nd // 2) + m, lhs)
            cols = halves[n]
            if q is small and e == 0 and n == 0:
                psend_s[0, :, tile(0)] = own_s[0, :, tile(0)].astype(BF16)
                part_copy(small, 0, tile(0)).start()
                extra_copy().start()
                cols = rest_cols
            term_copy(q, e, cols, n).start()

    rest_cols = slice(C, d // 2)
    halves_of_term(small, 0)
    all_of(acts.at[pl.ds(base(small, 1), 2 * RS)], load_sem.at[second_rows]).wait()
    hidden_part(small, 1)
    chip_sum(small, 0, True, rest_cols, 0)
    chip_sum(small, 0, True, halves[1], 1)
    halves_of_term(small, 1)
    chip_sum(small, 1, True, halves[0], 0)
    all_of(acts.at[0 : rows - SMALL * 2 * RS], load_sem.at[rest]).wait()
    hidden_part(big, 0)
    chip_sum(small, 1, True, halves[1], 1)
    halves_of_term(big, 0)

    @pl.loop(1, 2 * nb)
    def _(e):
        hidden_part(big, e)

        @pl.when(e == 1)
        def _():
            for n in range(2):
                chip_sum(big, 0, True, halves[n], n)

        term_part(big, e)

        @pl.when((e > 1) & (e <= nb))
        def _():
            chip_sum(big, e - 1, True)

        @pl.when(e > nb)
        def _():
            chip_sum(big, e - 1, False)

    for e in range(SMALL, 2 * SMALL):
        hidden_part(small, e)
        term_part(small, e)
        if e == SMALL:
            chip_sum(big, 2 * nb - 1, False)
        else:
            chip_sum(small, e - 1, False)

    x_copy.wait()
    finish(big, 0)
    chip_sum(small, 2 * SMALL - 1, False)
    for j in range(SMALL):
        finish(small, j)
    for j in range(1, nb - 1):
        finish(big, j)

    @pl.loop(0, d // C)
    def _(m):
        grad_x(m)

    finish(big, nb - 1)

    @pl.loop(0, f // C)
    def _(m):
        grad_h(m)

        @pl.when(m == f // C - 2)
        def _():
            pass_on(big, 0)

    all_of(dx.at[0:half], sent.at[0]).wait()
    all_of(dx.at[0 : half // 2], sent.at[1]).wait()

    @pl.when(core == EARLY)
    def _():
        pass_on(small, 0)
        all_of(dx.at[0 : RB + RS], sent.at[2]).wait()
        all_of(dx.at[0 : half // 2 + RB + RS], sent.at[3]).wait()
        all_of(dx.at[0 : half // 2 + RB], landed).wait()

    @pl.when(core != EARLY)
    def _():
        for q in (small, big):
            for j in range(1 if q is big else 0, q.n):
                final_copy(q, j).wait_recv()
        all_of(dx.at[0 : half // 2], sent.at[2]).wait()
        all_of(dx.at[0 : half // 2 + RB], sent.at[3]).wait()
        all_of(dx.at[0 : half // 2 + RB + RS], landed).wait()


def rest_kernel(_, dx, recv, ready, sent, landed):
    half = dx.shape[0] // 2
    me = lax.axis_index("tp")
    chip, core = me // 2, me % 2
    partner, peer, across = chip * 2 + (1 - core), (1 - chip) * 2 + core, (1 - chip) * 2 + (1 - core)
    big = [(SMALL * 2 * RS + j * 2 * RB, RB, 0, RB) for j in range(1, (half - SMALL * 2 * RS) // (2 * RB))]
    small = [(j * 2 * RS, RS, 0, RS) for j in range(1, SMALL - 1)]
    here = (0, RS, 0, RS)
    last = [((SMALL - 1) * 2 * RS, RS, sum(LAST[:n]), size) for n, size in enumerate(LAST)]
    pieces = big + small + last

    def rows(owner, piece):
        at, r, off, size = piece
        return pl.ds(pl.multiple_of(owner * half + at + core * r + off, 8), size)

    def copy(r, send, recv, to):
        return pltpu.make_async_remote_copy(
            src_ref=dx.at[r], dst_ref=dx.at[r], send_sem=send, recv_sem=recv, device_id={"tp": to}, device_id_type=MESH
        )

    def final_copy(n):
        return copy(rows(chip, pieces[n]), sent, recv.at[n], peer)

    def core_copy(n):
        return copy(rows(1 - chip, here if n is None else pieces[n]), sent, landed, partner)

    end = len(pieces) - 1
    direct_copy = copy(rows(chip, pieces[end]), sent, landed, across)

    def all_of(n, sem):
        return pltpu.make_async_copy(dx.at[0:n], dx.at[0:n], sem)

    passes = half // 2 - RB - RS
    barrier = pltpu.get_barrier_semaphore()

    @pl.when(core == EARLY)
    def _():
        for to in (peer, partner, across):
            pl.semaphore_signal(barrier, inc=1, device_id={"tp": to}, device_id_type=MESH)

    pl.semaphore_wait(barrier, 1 + lax.rem(core + EARLY, 2))

    @pl.when(core == EARLY)
    def _():
        for n in range(end):
            final_copy(n).start()
        pl.semaphore_wait(ready, 2)
        direct_copy.start()
        final_copy(end).start()
        for n in range(len(pieces)):
            final_copy(n).wait_recv()
            if n < end:
                core_copy(n).start()
        all_of(2 * passes, sent).wait()
        all_of(passes + RS, landed).wait()

    @pl.when(core != EARLY)
    def _():
        for to in (partner, across):
            pl.semaphore_signal(ready, inc=1, device_id={"tp": to}, device_id_type=MESH)
        core_copy(None).start()
        for n in range(len(pieces)):
            core_copy(n).start()
        all_of(passes + RS, sent).wait()
        all_of(passes, landed).wait()


def start_all(pairs, sem):
    copies = [pltpu.make_async_copy(a, b, sem) for a, b in pairs]
    for c in copies:
        c.start()
    return copies


def wait_all(copies):
    for c in copies:
        c.wait()


def rows_of(dx):
    half = dx.shape[0] // 2
    chip = lax.axis_index("tp") // 2
    first = SMALL * 2 * RS
    own = [(chip * half + n * (half // 2), half // 2) for n in range(2)]
    theirs = (1 - chip) * half
    steps = [(theirs + n * 2 * RS, RS) for n in range(SMALL)]
    steps += [(theirs + n, RB) for n in range(first + 2 * RB, half, 2 * RB)]

    def slices(parts):
        return [pl.ds(pl.multiple_of(at, RS), size) for at, size in parts]

    late, early = ([(at + k * size, size) for at, size in steps] for k in (1 - EARLY, EARLY))
    return slices(own + [(theirs + first, 2 * RB)]), slices(late), slices(early)


def write_most(dx_v, dwg_v, dwu_v, dwd_v, _, dx, dwg, dwu, dwd, sem):
    done, late, early = rows_of(dx)
    pairs = [(dx_v.at[r], dx.at[r]) for r in done + early[:1]]
    for src, dst in ((dwg_v, dwg), (dwu_v, dwu), (dwd_v, dwd)):
        n = src.shape[0] // 2
        pairs += [(src.at[r], dst.at[r]) for r in (pl.ds(0, n), pl.ds(n, n))]
    copies = start_all(pairs, sem)

    @pl.when(lax.rem(lax.axis_index("tp"), 2) != EARLY)
    def _():
        wait_all(start_all([(dx_v.at[r], dx.at[r]) for r in late], sem))

    wait_all(copies)


def write_late(dx_v, _, dx, sem):
    _, late, early = rows_of(dx)
    copies = start_all([(dx_v.at[r], dx.at[r]) for r in early[1:]], sem)

    @pl.when(lax.rem(lax.axis_index("tp"), 2) == EARLY)
    def _():
        wait_all(start_all([(dx_v.at[r], dx.at[r]) for r in late], sem))

    wait_all(copies)


def solution(mesh):
    def step(x, dy, gate, up, w_gate, w_up, w_down):
        rows, d = x.shape
        f = gate.shape[1]
        nb = (rows // 2 - SMALL * 2 * RS) // (2 * RB)
        outs = [((rows, d), BF16), ((d, f), BF16), ((d, f), BF16), ((f, d), BF16)]
        dma = pltpu.SemaphoreType.DMA

        def buffers(n, r):
            shapes = ((2 * n, F32), (2 * n, BF16), (2 * n, BF16), (n, BF16), (n, BF16))
            return [pltpu.VMEM((m, r, d), t) for m, t in shapes]

        dx, *grads = pl.pallas_call(
            kernel,
            out_shape=[pltpu.VMEM(s, t) for s, t in outs],
            in_specs=[pl.BlockSpec(memory_space=pl.ANY)] * 7,
            out_specs=[pl.BlockSpec(memory_space=pltpu.VMEM)] * 4,
            scratch_shapes=[
                pltpu.VMEM((rows, d), BF16),
                pltpu.VMEM((rows, d + 2 * f), BF16),
                pltpu.VMEM((d, 2 * f), BF16),
                pltpu.VMEM((f, d), BF16),
                pltpu.VMEM((rows, 2 * f), BF16),
                pltpu.VMEM((rows, f), BF16),
                pltpu.VMEM((C, rows), BF16),
            ]
            + buffers(SMALL, RS)
            + buffers(nb, RB)
            + [
                pltpu.VMEM((RS, C), BF16),
                dma((7,)),
                dma((4,)),
                dma(()),
                dma((4 * (SMALL + nb),)),
                dma((SMALL + nb,)),
                dma((SMALL + nb,)),
                dma(()),
            ],
            compiler_params=pltpu.CompilerParams(
                collective_id=0, has_side_effects=True, vmem_limit_bytes=50 * 2**20
            ),
            name="block",
        )(x, dy, gate, up, w_gate, w_up, w_down)
        held, plain = pl.BlockSpec(memory_space=pltpu.VMEM), pl.BlockSpec(memory_space=pl.ANY)
        shapes = [jax.ShapeDtypeStruct(s, t) for s, t in outs]
        little = 2**20

        def pin(a):
            return pltpu.with_memory_space_constraint(a, pltpu.VMEM)

        dx, most, *grads = pl.pallas_call(
            write_most,
            out_shape=[pltpu.VMEM(*outs[0])] + shapes,
            in_specs=[plain] + [held] * 3,
            out_specs=[plain] * 5,
            scratch_shapes=[dma(())],
            input_output_aliases={0: 0},
            compiler_params=pltpu.CompilerParams(vmem_limit_bytes=little),
            name="write_most",
        )(pin(dx), *(pin(g) for g in grads))
        dx = pl.pallas_call(
            rest_kernel,
            out_shape=pltpu.VMEM(*outs[0]),
            in_specs=[plain],
            out_specs=plain,
            scratch_shapes=[
                dma((nb + SMALL - 3 + len(LAST),)), pltpu.SemaphoreType.REGULAR, dma(()), dma(())
            ],
            input_output_aliases={0: 0},
            compiler_params=pltpu.CompilerParams(collective_id=1, has_side_effects=True, vmem_limit_bytes=little),
            name="rest",
        )(pin(dx))
        dx = pl.pallas_call(
            write_late,
            out_shape=shapes[0],
            in_specs=[held, plain],
            out_specs=plain,
            scratch_shapes=[dma(())],
            input_output_aliases={1: 0},
            compiler_params=pltpu.CompilerParams(vmem_limit_bytes=little),
            name="write_late",
        )(pin(dx), most)
        return dx, *grads

    tokens, columns, rows = P("dp", None), P(None, "tp"), P("tp", None)
    return jax.shard_map(
        step,
        mesh=mesh,
        in_specs=(tokens, tokens, P("dp", "tp"), P("dp", "tp"), columns, columns, rows),
        out_specs=(tokens, P("dp", "tp"), P("dp", "tp"), P(("dp", "tp"), None)),
        check_vma=False,
    )
```

```python
import types

import jax
import jax.numpy as jnp
from jax import lax
from jax.experimental import pallas as pl
from jax.experimental.pallas import tpu as pltpu
from jax.sharding import PartitionSpec as P

MESH = pl.DeviceIdType.MESH
F32, BF16 = jnp.float32, jnp.bfloat16
C = 256
SMALL, RS, RB = 2, 64, 128
EARLY, LAST = 1, (16, 24, 24)


def dot_t(a, b):
    return lax.dot_general(a, b, (((1,), (1,)), ((), ())), preferred_element_type=F32)


def dot(a, b):
    return lax.dot_general(a, b, (((1,), (0,)), ((), ())), preferred_element_type=F32)


def tile(n, start=0):
    return slice(start + n * C, start + (n + 1) * C)


def kernel(
    x_h, dy_h, gate_h, up_h, wg_h, wu_h, wd_h,
    dx, dwg, dwu, dwd,
    xv, acts, wgu, wd, dgu, hid, xt,
    own_s, tsend_s, trecv_s, psend_s, precv_s, own_b, tsend_b, trecv_b, psend_b, precv_b, extra,
    load_sem, sent, landed, term_sem, part_sem, final_sem, extra_sem,
):
    rows, d = xv.shape
    f = wd.shape[0]
    half = rows // 2
    dyv, gv, uv = acts.at[:, 0:d], acts.at[:, d : d + f], acts.at[:, d + f : d + 2 * f]
    me = lax.axis_index("tp")
    chip, core = me // 2, me % 2
    partner, peer, across = chip * 2 + (1 - core), (1 - chip) * 2 + core, (1 - chip) * 2 + (1 - core)
    nb = (half - SMALL * 2 * RS) // (2 * RB)
    small = types.SimpleNamespace(
        r=RS, off=0, n=SMALL, at=0, own=own_s, tsend=tsend_s, trecv=trecv_s, psend=psend_s, precv=precv_s
    )
    big = types.SimpleNamespace(
        r=RB, off=SMALL * 2 * RS, n=nb, at=SMALL, own=own_b, tsend=tsend_b, trecv=trecv_b, psend=psend_b, precv=precv_b
    )

    def base(q, e):
        owner = lax.rem(chip + 1 + e // q.n, 2)
        return pl.multiple_of(owner * half + q.off + lax.rem(e, q.n) * (2 * q.r), 2 * RS)

    def block(q, e, k):
        return pl.ds(pl.multiple_of(base(q, e) + k * q.r, RS), q.r)

    def local(src, dst, sem):
        return pltpu.make_async_copy(src, dst, load_sem.at[sem])

    def load(q, e, sem):
        r = pl.ds(base(q, e), 2 * q.r)
        return [local(src.at[r], dst.at[r], sem) for src, dst in ((dy_h, dyv), (gate_h, gv), (up_h, uv))]

    def all_of(ref, sem):
        return pltpu.make_async_copy(ref, ref, sem)

    def remote(src, dst, send, recv, to):
        return pltpu.make_async_remote_copy(
            src_ref=src, dst_ref=dst, send_sem=send, recv_sem=recv, device_id={"tp": to}, device_id_type=MESH
        )

    def term_copy(q, e, cols=slice(None), n=0):
        recv = term_sem.at[2 * (2 * q.at + e) + n]
        return remote(q.tsend.at[e, :, cols], q.trecv.at[e, :, cols], sent.at[0], recv, partner)

    def part_copy(q, e, cols=slice(None)):
        return remote(q.psend.at[e, :, cols], q.precv.at[e, :, cols], sent.at[1], part_sem.at[q.at + e], peer)

    def extra_copy():
        return remote(tsend_s.at[0, :, tile(0)], extra, sent.at[0], extra_sem, across)

    def final_copy(q, j):
        r = block(q, q.n + j, core)
        return remote(dx.at[r], dx.at[r], sent.at[2], final_sem.at[q.at + j], peer)

    def core_copy(r):
        return remote(dx.at[r], dx.at[r], sent.at[3], landed, partner)

    def start(copies):
        for c in copies:
            c.start()

    def hidden_tile(q, e, n, dyb):
        dh = dot_t(dyb, wd[tile(n), :])
        for part, k in ((dh[: q.r], 1 - core), (dh[q.r :], core)):
            r = block(q, e, k)
            g, u = gv[r, tile(n)].astype(F32), uv[r, tile(n)].astype(F32)
            sig = jax.nn.sigmoid(g)
            act = g * sig
            hid[r, tile(n)] = (act * u).astype(BF16)
            dgu[r, tile(n)] = ((part * u) * (sig + act * (1.0 - sig))).astype(BF16)
            dgu[r, tile(n, f)] = (part * act).astype(BF16)

    def both(ref, q, e):
        return jnp.concatenate([ref[block(q, e, 1 - core), :], ref[block(q, e, core), :]], axis=0)

    def hidden_part(q, e):
        dyb = both(dyv, q, e)
        for n in range(f // C):
            hidden_tile(q, e, n, dyb)

    def term_tile(q, e, n, lhs, alone=False):
        t = dot_t(lhs, wgu[tile(n), :])
        q.tsend[e, :, tile(n)] = t[: q.r].astype(BF16)
        if alone:
            q.psend[e, :, tile(n)] = t[q.r :].astype(BF16)
        else:
            q.own[e, :, tile(n)] = t[q.r :]

    def term_part(q, e):
        lhs = both(dgu, q, e)
        for n in range(d // C):
            term_tile(q, e, n, lhs)
        term_copy(q, e).start()

    def chip_sum(q, e, theirs, cols=slice(None), n=0):
        term_copy(q, e, cols, n).wait_recv()
        s = q.own[e, :, cols] + q.trecv[e, :, cols].astype(F32)
        if theirs:
            q.psend[e, :, cols] = s.astype(BF16)
            part_copy(q, e, cols).start()
        else:
            q.own[e, :, cols] = s

    def finish(q, j):
        part_copy(q, j).wait_recv()
        r = block(q, q.n + j, core)
        total = q.own[q.n + j] + q.precv[j].astype(F32)
        if q is small and j == 0:
            extra_copy().wait_recv()
            dx[r, C:] = total[:, C:].astype(BF16)
            dx[r, :C] = (total[:, :C] + extra[...].astype(F32)).astype(BF16)
        else:
            dx[r, :] = total.astype(BF16)
        if q is big and j == 0:
            final_copy(q, j).start()
        else:

            @pl.when(core != EARLY)
            def _():
                final_copy(q, j).start()

        core_copy(r).start()

    def pass_on(q, j):
        final_copy(q, j).wait_recv()
        core_copy(block(q, j, core)).start()

    def grad_x(m):
        r = pl.ds(pl.multiple_of(m * C, C), C)
        xt[...] = xv[:, r].T
        for n in range(f // C):
            dwg[r, tile(n)] = dot(xt[...], dgu[:, tile(n)]).astype(BF16)
            dwu[r, tile(n)] = dot(xt[...], dgu[:, tile(n, f)]).astype(BF16)

    def grad_h(m):
        r = pl.ds(pl.multiple_of(m * C, C), C)
        xt[...] = hid[:, r].T
        for n in range(d // C):
            dwd[r, tile(n)] = dot(xt[...], dyv[:, tile(n)]).astype(BF16)

    nf, nd = f // C, d // C
    w_sem, first_rows, gu, second_rows, rest, x_sem = 0, 1, 2, 4, 5, 6
    first = load(small, 0, first_rows)
    wds = [local(wd_h.at[tile(n)], wd.at[tile(n)], w_sem) for n in range(nf)]
    start(first[:1] + wds[:1] + first[1:] + wds[1:])
    for n in range(nd):
        start([local(w.at[tile(n)], wgu.at[tile(n), c * f : (c + 1) * f], gu + n // 2) for c, w in enumerate((wg_h, wu_h))])
    start(load(small, 1, second_rows))
    for e in range(2 * nb):
        start(load(big, e, rest))
    for e in range(SMALL, 2 * SMALL):
        start(load(small, e, rest))
    x_copy = local(x_h, xv, x_sem)
    start([x_copy])

    barrier = pltpu.get_barrier_semaphore()
    for to in (partner, peer, across):
        pl.semaphore_signal(barrier, inc=1, device_id={"tp": to}, device_id_type=MESH)

    all_of(acts.at[pl.ds(base(small, 0), 2 * RS)], load_sem.at[first_rows]).wait()
    all_of(wd, load_sem.at[w_sem]).wait()
    hidden_part(small, 0)
    pl.semaphore_wait(barrier, 3)
    halves = [slice(n * (d // 2), (n + 1) * (d // 2)) for n in range(2)]

    def halves_of_term(q, e):
        lhs = both(dgu, q, e)
        for n in range(2):
            if q is small and e == 0:
                all_of(wgu.at[halves[n]], load_sem.at[gu + n]).wait()
            for m in range(nd // 2):
                term_tile(q, e, n * (nd // 2) + m, lhs, alone=q is small and e == 0 and n == 0 and m == 0)
            cols = halves[n]
            if q is small and e == 0 and n == 0:
                part_copy(small, 0, tile(0)).start()
                extra_copy().start()
                cols = rest_cols
            term_copy(q, e, cols, n).start()

    rest_cols = slice(C, d // 2)
    halves_of_term(small, 0)
    all_of(acts.at[pl.ds(base(small, 1), 2 * RS)], load_sem.at[second_rows]).wait()
    hidden_part(small, 1)
    chip_sum(small, 0, True, rest_cols, 0)
    chip_sum(small, 0, True, halves[1], 1)
    halves_of_term(small, 1)
    chip_sum(small, 1, True, halves[0], 0)
    all_of(acts.at[0 : rows - SMALL * 2 * RS], load_sem.at[rest]).wait()
    hidden_part(big, 0)
    chip_sum(small, 1, True, halves[1], 1)
    halves_of_term(big, 0)

    @pl.loop(1, 2 * nb)
    def _(e):
        hidden_part(big, e)

        @pl.when(e == 1)
        def _():
            for n in range(2):
                chip_sum(big, 0, True, halves[n], n)

        term_part(big, e)

        @pl.when((e > 1) & (e <= nb))
        def _():
            chip_sum(big, e - 1, True)

        @pl.when(e > nb)
        def _():
            chip_sum(big, e - 1, False)

    for e in range(SMALL, 2 * SMALL):
        hidden_part(small, e)
        term_part(small, e)
        if e == SMALL:
            chip_sum(big, 2 * nb - 1, False)
        else:
            chip_sum(small, e - 1, False)

    x_copy.wait()
    finish(big, 0)
    chip_sum(small, 2 * SMALL - 1, False)
    for j in range(SMALL):
        finish(small, j)
    for j in range(1, nb - 1):
        finish(big, j)

    @pl.loop(0, d // C)
    def _(m):
        grad_x(m)

    finish(big, nb - 1)

    @pl.loop(0, f // C)
    def _(m):
        grad_h(m)

        @pl.when(m == f // C - 2)
        def _():
            pass_on(big, 0)

    ahead = RB
    all_of(dx.at[0:half], sent.at[0]).wait()
    all_of(dx.at[0 : half // 2], sent.at[1]).wait()
    all_of(dx.at[0 : half // 2 + ahead], sent.at[3]).wait()
    all_of(dx.at[0 : half // 2 + ahead], landed).wait()

    @pl.when(core == EARLY)
    def _():
        all_of(dx.at[0:ahead], sent.at[2]).wait()

    @pl.when(core != EARLY)
    def _():
        for q in (small, big):
            for j in range(1 if q is big else 0, q.n):
                final_copy(q, j).wait_recv()
        all_of(dx.at[0 : half // 2], sent.at[2]).wait()


def rest_kernel(_, dx, recv, ready, sent, landed):
    half = dx.shape[0] // 2
    me = lax.axis_index("tp")
    chip, core = me // 2, me % 2
    partner, peer, across = chip * 2 + (1 - core), (1 - chip) * 2 + core, (1 - chip) * 2 + (1 - core)
    big = [(SMALL * 2 * RS + j * 2 * RB, RB, 0, RB) for j in range(1, (half - SMALL * 2 * RS) // (2 * RB))]
    small = [(j * 2 * RS, RS, 0, RS) for j in range(SMALL - 1)]
    last = [((SMALL - 1) * 2 * RS, RS, sum(LAST[:n]), size) for n, size in enumerate(LAST)]
    pieces = big + small + last

    def rows(owner, piece):
        at, r, off, size = piece
        return pl.ds(pl.multiple_of(owner * half + at + core * r + off, 8), size)

    def copy(r, send, recv, to):
        return pltpu.make_async_remote_copy(
            src_ref=dx.at[r], dst_ref=dx.at[r], send_sem=send, recv_sem=recv, device_id={"tp": to}, device_id_type=MESH
        )

    def final_copy(n):
        return copy(rows(chip, pieces[n]), sent, recv.at[n], peer)

    def core_copy(n):
        return copy(rows(1 - chip, pieces[n]), sent, landed, partner)

    end = len(pieces) - 1
    direct_copy = copy(rows(chip, pieces[end]), sent, landed, across)

    def all_of(n, sem):
        return pltpu.make_async_copy(dx.at[0:n], dx.at[0:n], sem)

    passes = half // 2 - RB
    barrier = pltpu.get_barrier_semaphore()

    @pl.when(core == EARLY)
    def _():
        for to in (peer, partner, across):
            pl.semaphore_signal(barrier, inc=1, device_id={"tp": to}, device_id_type=MESH)

    pl.semaphore_wait(barrier, 1 + lax.rem(core + EARLY, 2))

    @pl.when(core == EARLY)
    def _():
        for n in range(end):
            final_copy(n).start()
        pl.semaphore_wait(ready, 2)
        direct_copy.start()
        final_copy(end).start()
        for n in range(len(pieces)):
            final_copy(n).wait_recv()
            if n < end:
                core_copy(n).start()
        all_of(2 * passes, sent).wait()

    @pl.when(core != EARLY)
    def _():
        for to in (partner, across):
            pl.semaphore_signal(ready, inc=1, device_id={"tp": to}, device_id_type=MESH)
        for n in range(len(pieces)):
            core_copy(n).start()
        all_of(passes, sent).wait()

    all_of(passes, landed).wait()


def start_all(pairs, sem):
    copies = [pltpu.make_async_copy(a, b, sem) for a, b in pairs]
    for c in copies:
        c.start()
    return copies


def wait_all(copies):
    for c in copies:
        c.wait()


def rows_of(dx):
    half = dx.shape[0] // 2
    chip = lax.axis_index("tp") // 2
    first = SMALL * 2 * RS
    own = [(chip * half + n * (half // 2), half // 2) for n in range(2)]
    theirs = (1 - chip) * half
    steps = [(theirs + n * 2 * RS, RS) for n in range(SMALL)]
    steps += [(theirs + n, RB) for n in range(first + 2 * RB, half, 2 * RB)]

    def slices(parts):
        return [pl.ds(pl.multiple_of(at, RS), size) for at, size in parts]

    late, early = ([(at + k * size, size) for at, size in steps] for k in (1 - EARLY, EARLY))
    return slices(own + [(theirs + first, 2 * RB)]), slices(late), slices(early)


def write_most(dx_v, dwg_v, dwu_v, dwd_v, _, dx, dwg, dwu, dwd, sem):
    done, late, _ = rows_of(dx)
    pairs = [(dx_v.at[r], dx.at[r]) for r in done]
    for src, dst in ((dwg_v, dwg), (dwu_v, dwu), (dwd_v, dwd)):
        n = src.shape[0] // 2
        pairs += [(src.at[r], dst.at[r]) for r in (pl.ds(0, n), pl.ds(n, n))]
    copies = start_all(pairs, sem)

    @pl.when(lax.rem(lax.axis_index("tp"), 2) != EARLY)
    def _():
        wait_all(start_all([(dx_v.at[r], dx.at[r]) for r in late], sem))

    wait_all(copies)


def write_late(dx_v, _, dx, sem):
    _, late, early = rows_of(dx)
    copies = start_all([(dx_v.at[r], dx.at[r]) for r in early], sem)

    @pl.when(lax.rem(lax.axis_index("tp"), 2) == EARLY)
    def _():
        wait_all(start_all([(dx_v.at[r], dx.at[r]) for r in late], sem))

    wait_all(copies)


def solution(mesh):
    def step(x, dy, gate, up, w_gate, w_up, w_down):
        rows, d = x.shape
        f = gate.shape[1]
        nb = (rows // 2 - SMALL * 2 * RS) // (2 * RB)
        outs = [((rows, d), BF16), ((d, f), BF16), ((d, f), BF16), ((f, d), BF16)]
        dma = pltpu.SemaphoreType.DMA

        def buffers(n, r):
            shapes = ((2 * n, F32), (2 * n, BF16), (2 * n, BF16), (n, BF16), (n, BF16))
            return [pltpu.VMEM((m, r, d), t) for m, t in shapes]

        dx, *grads = pl.pallas_call(
            kernel,
            out_shape=[pltpu.VMEM(s, t) for s, t in outs],
            in_specs=[pl.BlockSpec(memory_space=pl.ANY)] * 7,
            out_specs=[pl.BlockSpec(memory_space=pltpu.VMEM)] * 4,
            scratch_shapes=[
                pltpu.VMEM((rows, d), BF16),
                pltpu.VMEM((rows, d + 2 * f), BF16),
                pltpu.VMEM((d, 2 * f), BF16),
                pltpu.VMEM((f, d), BF16),
                pltpu.VMEM((rows, 2 * f), BF16),
                pltpu.VMEM((rows, f), BF16),
                pltpu.VMEM((C, rows), BF16),
            ]
            + buffers(SMALL, RS)
            + buffers(nb, RB)
            + [
                pltpu.VMEM((RS, C), BF16),
                dma((7,)),
                dma((4,)),
                dma(()),
                dma((4 * (SMALL + nb),)),
                dma((SMALL + nb,)),
                dma((SMALL + nb,)),
                dma(()),
            ],
            compiler_params=pltpu.CompilerParams(
                collective_id=0, has_side_effects=True, vmem_limit_bytes=50 * 2**20
            ),
            name="block",
        )(x, dy, gate, up, w_gate, w_up, w_down)
        held, plain = pl.BlockSpec(memory_space=pltpu.VMEM), pl.BlockSpec(memory_space=pl.ANY)
        shapes = [jax.ShapeDtypeStruct(s, t) for s, t in outs]
        little = 2**20

        def pin(a):
            return pltpu.with_memory_space_constraint(a, pltpu.VMEM)

        dx, most, *grads = pl.pallas_call(
            write_most,
            out_shape=[pltpu.VMEM(*outs[0])] + shapes,
            in_specs=[plain] + [held] * 3,
            out_specs=[plain] * 5,
            scratch_shapes=[dma(())],
            input_output_aliases={0: 0},
            compiler_params=pltpu.CompilerParams(vmem_limit_bytes=little),
            name="write_most",
        )(pin(dx), *(pin(g) for g in grads))
        dx = pl.pallas_call(
            rest_kernel,
            out_shape=pltpu.VMEM(*outs[0]),
            in_specs=[plain],
            out_specs=plain,
            scratch_shapes=[
                dma((nb + SMALL - 2 + len(LAST),)), pltpu.SemaphoreType.REGULAR, dma(()), dma(())
            ],
            input_output_aliases={0: 0},
            compiler_params=pltpu.CompilerParams(collective_id=1, has_side_effects=True, vmem_limit_bytes=little),
            name="rest",
        )(pin(dx))
        dx = pl.pallas_call(
            write_late,
            out_shape=shapes[0],
            in_specs=[held, plain],
            out_specs=plain,
            scratch_shapes=[dma(())],
            input_output_aliases={1: 0},
            compiler_params=pltpu.CompilerParams(vmem_limit_bytes=little),
            name="write_late",
        )(pin(dx), most)
        return dx, *grads

    tokens, columns, rows = P("dp", None), P(None, "tp"), P("tp", None)
    return jax.shard_map(
        step,
        mesh=mesh,
        in_specs=(tokens, tokens, P("dp", "tp"), P("dp", "tp"), columns, columns, rows),
        out_specs=(tokens, P("dp", "tp"), P("dp", "tp"), P(("dp", "tp"), None)),
        check_vma=False,
    )
```

```python
import types

import jax
import jax.numpy as jnp
from jax import lax
from jax.experimental import pallas as pl
from jax.experimental.pallas import tpu as pltpu
from jax.sharding import PartitionSpec as P

MESH = pl.DeviceIdType.MESH
F32, BF16 = jnp.float32, jnp.bfloat16
C = 256
SMALL, RS, RB = 2, 64, 128
EARLY, LAST = 1, (16, 24, 24)


def dot_t(a, b):
    return lax.dot_general(a, b, (((1,), (1,)), ((), ())), preferred_element_type=F32)


def dot(a, b):
    return lax.dot_general(a, b, (((1,), (0,)), ((), ())), preferred_element_type=F32)


def tile(n, start=0):
    return slice(start + n * C, start + (n + 1) * C)


def kernel(
    x_h, dy_h, gate_h, up_h, wg_h, wu_h, wd_h,
    dx, dwg, dwu, dwd,
    xv, acts, wgu, wd, dgu, hid, xt,
    own_s, tsend_s, trecv_s, psend_s, precv_s, own_b, tsend_b, trecv_b, psend_b, precv_b, extra,
    load_sem, sent, landed, term_sem, part_sem, final_sem, extra_sem,
):
    rows, d = xv.shape
    f = wd.shape[0]
    half = rows // 2
    dyv, gv, uv = acts.at[:, 0:d], acts.at[:, d : d + f], acts.at[:, d + f : d + 2 * f]
    me = lax.axis_index("tp")
    chip, core = me // 2, me % 2
    partner, peer, across = chip * 2 + (1 - core), (1 - chip) * 2 + core, (1 - chip) * 2 + (1 - core)
    nb = (half - SMALL * 2 * RS) // (2 * RB)
    small = types.SimpleNamespace(
        r=RS, off=0, n=SMALL, at=0, own=own_s, tsend=tsend_s, trecv=trecv_s, psend=psend_s, precv=precv_s
    )
    big = types.SimpleNamespace(
        r=RB, off=SMALL * 2 * RS, n=nb, at=SMALL, own=own_b, tsend=tsend_b, trecv=trecv_b, psend=psend_b, precv=precv_b
    )

    def base(q, e):
        owner = lax.rem(chip + 1 + e // q.n, 2)
        return pl.multiple_of(owner * half + q.off + lax.rem(e, q.n) * (2 * q.r), 2 * RS)

    def block(q, e, k):
        return pl.ds(pl.multiple_of(base(q, e) + k * q.r, RS), q.r)

    def local(src, dst, sem):
        return pltpu.make_async_copy(src, dst, load_sem.at[sem])

    def load(q, e, sem):
        r = pl.ds(base(q, e), 2 * q.r)
        return [local(src.at[r], dst.at[r], sem) for src, dst in ((dy_h, dyv), (gate_h, gv), (up_h, uv))]

    def all_of(ref, sem):
        return pltpu.make_async_copy(ref, ref, sem)

    def remote(src, dst, send, recv, to):
        return pltpu.make_async_remote_copy(
            src_ref=src, dst_ref=dst, send_sem=send, recv_sem=recv, device_id={"tp": to}, device_id_type=MESH
        )

    def term_copy(q, e, cols=slice(None), n=0):
        recv = term_sem.at[2 * (2 * q.at + e) + n]
        return remote(q.tsend.at[e, :, cols], q.trecv.at[e, :, cols], sent.at[0], recv, partner)

    def part_copy(q, e, cols=slice(None)):
        return remote(q.psend.at[e, :, cols], q.precv.at[e, :, cols], sent.at[1], part_sem.at[q.at + e], peer)

    def extra_copy():
        return remote(tsend_s.at[0, :, tile(0)], extra, sent.at[0], extra_sem, across)

    def final_copy(q, j):
        r = block(q, q.n + j, core)
        return remote(dx.at[r], dx.at[r], sent.at[2], final_sem.at[q.at + j], peer)

    def core_copy(r):
        return remote(dx.at[r], dx.at[r], sent.at[3], landed, partner)

    def start(copies):
        for c in copies:
            c.start()

    def hidden_tile(q, e, n, dyb):
        dh = dot_t(dyb, wd[tile(n), :])
        for part, k in ((dh[: q.r], 1 - core), (dh[q.r :], core)):
            r = block(q, e, k)
            g, u = gv[r, tile(n)].astype(F32), uv[r, tile(n)].astype(F32)
            sig = jax.nn.sigmoid(g)
            act = g * sig
            hid[r, tile(n)] = (act * u).astype(BF16)
            dgu[r, tile(n)] = ((part * u) * (sig + act * (1.0 - sig))).astype(BF16)
            dgu[r, tile(n, f)] = (part * act).astype(BF16)

    def both(ref, q, e):
        return jnp.concatenate([ref[block(q, e, 1 - core), :], ref[block(q, e, core), :]], axis=0)

    def hidden_part(q, e):
        dyb = both(dyv, q, e)
        for n in range(f // C):
            hidden_tile(q, e, n, dyb)

    def term_tile(q, e, n, lhs, alone=False):
        t = dot_t(lhs, wgu[tile(n), :])
        q.tsend[e, :, tile(n)] = t[: q.r].astype(BF16)
        if alone:
            q.psend[e, :, tile(n)] = t[q.r :].astype(BF16)
        else:
            q.own[e, :, tile(n)] = t[q.r :]

    def term_part(q, e):
        lhs = both(dgu, q, e)
        for n in range(d // C):
            term_tile(q, e, n, lhs)
        term_copy(q, e).start()

    def chip_sum(q, e, theirs, cols=slice(None), n=0):
        term_copy(q, e, cols, n).wait_recv()
        s = q.own[e, :, cols] + q.trecv[e, :, cols].astype(F32)
        if theirs:
            q.psend[e, :, cols] = s.astype(BF16)
            part_copy(q, e, cols).start()
        else:
            q.own[e, :, cols] = s

    def finish(q, j):
        part_copy(q, j).wait_recv()
        r = block(q, q.n + j, core)
        total = q.own[q.n + j] + q.precv[j].astype(F32)
        if q is small and j == 0:
            extra_copy().wait_recv()
            dx[r, C:] = total[:, C:].astype(BF16)
            dx[r, :C] = (total[:, :C] + extra[...].astype(F32)).astype(BF16)
        else:
            dx[r, :] = total.astype(BF16)
        if q is big and j == 0:
            final_copy(q, j).start()
        else:

            @pl.when(core != EARLY)
            def _():
                final_copy(q, j).start()

        core_copy(r).start()

    def pass_on(q, j):
        final_copy(q, j).wait_recv()
        core_copy(block(q, j, core)).start()

    def grad_x(m):
        r = pl.ds(pl.multiple_of(m * C, C), C)
        xt[...] = xv[:, r].T
        for n in range(f // C):
            dwg[r, tile(n)] = dot(xt[...], dgu[:, tile(n)]).astype(BF16)
            dwu[r, tile(n)] = dot(xt[...], dgu[:, tile(n, f)]).astype(BF16)

    def grad_h(m):
        r = pl.ds(pl.multiple_of(m * C, C), C)
        xt[...] = hid[:, r].T
        for n in range(d // C):
            dwd[r, tile(n)] = dot(xt[...], dyv[:, tile(n)]).astype(BF16)

    nf, nd = f // C, d // C
    w_sem, first_rows, gu, second_rows, rest, x_sem = 0, 2, 3, 5, 6, 7
    first = load(small, 0, first_rows)
    wds = [local(wd_h.at[tile(n)], wd.at[tile(n)], w_sem + min(n, 1)) for n in range(nf)]
    start(first[:1] + wds[:1] + first[1:] + wds[1:])
    for n in range(nd):
        start([local(w.at[tile(n)], wgu.at[tile(n), c * f : (c + 1) * f], gu + n // 2) for c, w in enumerate((wg_h, wu_h))])
    start(load(small, 1, second_rows))
    for e in range(2 * nb):
        start(load(big, e, rest))
    for e in range(SMALL, 2 * SMALL):
        start(load(small, e, rest))
    x_copy = local(x_h, xv, x_sem)
    start([x_copy])

    barrier = pltpu.get_barrier_semaphore()
    for to in (partner, peer, across):
        pl.semaphore_signal(barrier, inc=1, device_id={"tp": to}, device_id_type=MESH)

    all_of(acts.at[pl.ds(base(small, 0), 2 * RS)], load_sem.at[first_rows]).wait()
    wds[0].wait()
    dyb = both(dyv, small, 0)
    hidden_tile(small, 0, 0, dyb)
    all_of(wd.at[C:f], load_sem.at[w_sem + 1]).wait()
    for n in range(1, nf):
        hidden_tile(small, 0, n, dyb)
    pl.semaphore_wait(barrier, 3)
    halves = [slice(n * (d // 2), (n + 1) * (d // 2)) for n in range(2)]

    def halves_of_term(q, e):
        lhs = both(dgu, q, e)
        for n in range(2):
            if q is small and e == 0:
                all_of(wgu.at[halves[n]], load_sem.at[gu + n]).wait()
            for m in range(nd // 2):
                term_tile(q, e, n * (nd // 2) + m, lhs, alone=q is small and e == 0 and n == 0 and m == 0)
            cols = halves[n]
            if q is small and e == 0 and n == 0:
                part_copy(small, 0, tile(0)).start()
                extra_copy().start()
                cols = rest_cols
            term_copy(q, e, cols, n).start()

    rest_cols = slice(C, d // 2)
    halves_of_term(small, 0)
    all_of(acts.at[pl.ds(base(small, 1), 2 * RS)], load_sem.at[second_rows]).wait()
    hidden_part(small, 1)
    chip_sum(small, 0, True, rest_cols, 0)
    chip_sum(small, 0, True, halves[1], 1)
    halves_of_term(small, 1)
    chip_sum(small, 1, True, halves[0], 0)
    all_of(acts.at[0 : rows - SMALL * 2 * RS], load_sem.at[rest]).wait()
    hidden_part(big, 0)
    chip_sum(small, 1, True, halves[1], 1)
    halves_of_term(big, 0)

    @pl.loop(1, 2 * nb)
    def _(e):
        hidden_part(big, e)

        @pl.when(e == 1)
        def _():
            for n in range(2):
                chip_sum(big, 0, True, halves[n], n)

        term_part(big, e)

        @pl.when((e > 1) & (e <= nb))
        def _():
            chip_sum(big, e - 1, True)

        @pl.when(e > nb)
        def _():
            chip_sum(big, e - 1, False)

    for e in range(SMALL, 2 * SMALL):
        hidden_part(small, e)
        term_part(small, e)
        if e == SMALL:
            chip_sum(big, 2 * nb - 1, False)
        else:
            chip_sum(small, e - 1, False)

    x_copy.wait()
    finish(big, 0)
    chip_sum(small, 2 * SMALL - 1, False)
    for j in range(SMALL):
        finish(small, j)
    for j in range(1, nb - 1):
        finish(big, j)

    @pl.loop(0, d // C)
    def _(m):
        grad_x(m)

    finish(big, nb - 1)

    @pl.loop(0, f // C)
    def _(m):
        grad_h(m)

        @pl.when(m == f // C - 2)
        def _():
            pass_on(big, 0)

    ahead = RB
    all_of(dx.at[0:half], sent.at[0]).wait()
    all_of(dx.at[0 : half // 2], sent.at[1]).wait()
    all_of(dx.at[0 : half // 2 + ahead], sent.at[3]).wait()
    all_of(dx.at[0 : half // 2 + ahead], landed).wait()

    @pl.when(core == EARLY)
    def _():
        all_of(dx.at[0:ahead], sent.at[2]).wait()

    @pl.when(core != EARLY)
    def _():
        for q in (small, big):
            for j in range(1 if q is big else 0, q.n):
                final_copy(q, j).wait_recv()
        all_of(dx.at[0 : half // 2], sent.at[2]).wait()


def rest_kernel(_, dx, recv, ready, sent, landed):
    half = dx.shape[0] // 2
    me = lax.axis_index("tp")
    chip, core = me // 2, me % 2
    partner, peer, across = chip * 2 + (1 - core), (1 - chip) * 2 + core, (1 - chip) * 2 + (1 - core)
    big = [(SMALL * 2 * RS + j * 2 * RB, RB, 0, RB) for j in range(1, (half - SMALL * 2 * RS) // (2 * RB))]
    small = [(j * 2 * RS, RS, 0, RS) for j in range(SMALL - 1)]
    last = [((SMALL - 1) * 2 * RS, RS, sum(LAST[:n]), size) for n, size in enumerate(LAST)]
    pieces = big + small + last

    def rows(owner, piece):
        at, r, off, size = piece
        return pl.ds(pl.multiple_of(owner * half + at + core * r + off, 8), size)

    def copy(r, send, recv, to):
        return pltpu.make_async_remote_copy(
            src_ref=dx.at[r], dst_ref=dx.at[r], send_sem=send, recv_sem=recv, device_id={"tp": to}, device_id_type=MESH
        )

    def final_copy(n):
        return copy(rows(chip, pieces[n]), sent, recv.at[max(n - len(big) + 1, 0)], peer)

    def core_copy(n):
        return copy(rows(1 - chip, pieces[n]), sent, landed, partner)

    end = len(pieces) - 1
    direct_copy = copy(rows(chip, pieces[end]), sent, landed, across)

    def all_of(n, sem):
        return pltpu.make_async_copy(dx.at[0:n], dx.at[0:n], sem)

    passes = half // 2 - RB
    barrier = pltpu.get_barrier_semaphore()

    @pl.when(core == EARLY)
    def _():
        for to in (peer, partner, across):
            pl.semaphore_signal(barrier, inc=1, device_id={"tp": to}, device_id_type=MESH)

    pl.semaphore_wait(barrier, 1 + lax.rem(core + EARLY, 2))

    @pl.when(core == EARLY)
    def _():
        for n in range(end):
            final_copy(n).start()
        pl.semaphore_wait(ready, 2)
        direct_copy.start()
        final_copy(end).start()
        for n in range(len(pieces)):
            if n == 0:
                all_of(len(big) * RB, recv.at[0]).wait()
            elif n >= len(big):
                final_copy(n).wait_recv()
            if n < end:
                core_copy(n).start()
        all_of(2 * passes, sent).wait()

    @pl.when(core != EARLY)
    def _():
        for to in (partner, across):
            pl.semaphore_signal(ready, inc=1, device_id={"tp": to}, device_id_type=MESH)
        for n in range(len(pieces)):
            core_copy(n).start()
        all_of(passes, sent).wait()

    all_of(passes, landed).wait()


def start_all(pairs, sem):
    copies = [pltpu.make_async_copy(a, b, sem) for a, b in pairs]
    for c in copies:
        c.start()
    return copies


def wait_all(copies):
    for c in copies:
        c.wait()


def rows_of(dx):
    half = dx.shape[0] // 2
    chip = lax.axis_index("tp") // 2
    first = SMALL * 2 * RS
    own = [(chip * half + n * (half // 2), half // 2) for n in range(2)]
    theirs = (1 - chip) * half
    steps = [(theirs + n * 2 * RS, RS) for n in range(SMALL)]
    steps += [(theirs + n, RB) for n in range(first + 2 * RB, half, 2 * RB)]

    def slices(parts):
        return [pl.ds(pl.multiple_of(at, RS), size) for at, size in parts]

    late, early = ([(at + k * size, size) for at, size in steps] for k in (1 - EARLY, EARLY))
    return slices(own + [(theirs + first, 2 * RB)]), slices(late), slices(early)


def write_most(dx_v, dwg_v, dwu_v, dwd_v, _, dx, dwg, dwu, dwd, sem):
    done, late, _ = rows_of(dx)
    pairs = [(dx_v.at[r], dx.at[r]) for r in done]
    for src, dst in ((dwg_v, dwg), (dwu_v, dwu), (dwd_v, dwd)):
        n = src.shape[0] // 2
        pairs += [(src.at[r], dst.at[r]) for r in (pl.ds(0, n), pl.ds(n, n))]
    copies = start_all(pairs, sem)

    @pl.when(lax.rem(lax.axis_index("tp"), 2) != EARLY)
    def _():
        wait_all(start_all([(dx_v.at[r], dx.at[r]) for r in late], sem))

    wait_all(copies)


def write_late(dx_v, _, dx, sem):
    _, late, early = rows_of(dx)
    copies = start_all([(dx_v.at[r], dx.at[r]) for r in early], sem)

    @pl.when(lax.rem(lax.axis_index("tp"), 2) == EARLY)
    def _():
        wait_all(start_all([(dx_v.at[r], dx.at[r]) for r in late], sem))

    wait_all(copies)


def solution(mesh):
    def step(x, dy, gate, up, w_gate, w_up, w_down):
        rows, d = x.shape
        f = gate.shape[1]
        nb = (rows // 2 - SMALL * 2 * RS) // (2 * RB)
        outs = [((rows, d), BF16), ((d, f), BF16), ((d, f), BF16), ((f, d), BF16)]
        dma = pltpu.SemaphoreType.DMA

        def buffers(n, r):
            shapes = ((2 * n, F32), (2 * n, BF16), (2 * n, BF16), (n, BF16), (n, BF16))
            return [pltpu.VMEM((m, r, d), t) for m, t in shapes]

        dx, *grads = pl.pallas_call(
            kernel,
            out_shape=[pltpu.VMEM(s, t) for s, t in outs],
            in_specs=[pl.BlockSpec(memory_space=pl.ANY)] * 7,
            out_specs=[pl.BlockSpec(memory_space=pltpu.VMEM)] * 4,
            scratch_shapes=[
                pltpu.VMEM((rows, d), BF16),
                pltpu.VMEM((rows, d + 2 * f), BF16),
                pltpu.VMEM((d, 2 * f), BF16),
                pltpu.VMEM((f, d), BF16),
                pltpu.VMEM((rows, 2 * f), BF16),
                pltpu.VMEM((rows, f), BF16),
                pltpu.VMEM((C, rows), BF16),
            ]
            + buffers(SMALL, RS)
            + buffers(nb, RB)
            + [
                pltpu.VMEM((RS, C), BF16),
                dma((8,)),
                dma((4,)),
                dma(()),
                dma((4 * (SMALL + nb),)),
                dma((SMALL + nb,)),
                dma((SMALL + nb,)),
                dma(()),
            ],
            compiler_params=pltpu.CompilerParams(
                collective_id=0, has_side_effects=True, vmem_limit_bytes=50 * 2**20
            ),
            name="block",
        )(x, dy, gate, up, w_gate, w_up, w_down)
        held, plain = pl.BlockSpec(memory_space=pltpu.VMEM), pl.BlockSpec(memory_space=pl.ANY)
        shapes = [jax.ShapeDtypeStruct(s, t) for s, t in outs]
        little = 2**20

        def pin(a):
            return pltpu.with_memory_space_constraint(a, pltpu.VMEM)

        dx, most, *grads = pl.pallas_call(
            write_most,
            out_shape=[pltpu.VMEM(*outs[0])] + shapes,
            in_specs=[plain] + [held] * 3,
            out_specs=[plain] * 5,
            scratch_shapes=[dma(())],
            input_output_aliases={0: 0},
            compiler_params=pltpu.CompilerParams(vmem_limit_bytes=little),
            name="write_most",
        )(pin(dx), *(pin(g) for g in grads))
        dx = pl.pallas_call(
            rest_kernel,
            out_shape=pltpu.VMEM(*outs[0]),
            in_specs=[plain],
            out_specs=plain,
            scratch_shapes=[
                dma((SMALL + len(LAST),)), pltpu.SemaphoreType.REGULAR, dma(()), dma(())
            ],
            input_output_aliases={0: 0},
            compiler_params=pltpu.CompilerParams(collective_id=1, has_side_effects=True, vmem_limit_bytes=little),
            name="rest",
        )(pin(dx))
        dx = pl.pallas_call(
            write_late,
            out_shape=shapes[0],
            in_specs=[held, plain],
            out_specs=plain,
            scratch_shapes=[dma(())],
            input_output_aliases={1: 0},
            compiler_params=pltpu.CompilerParams(vmem_limit_bytes=little),
            name="write_late",
        )(pin(dx), most)
        return dx, *grads

    tokens, columns, rows = P("dp", None), P(None, "tp"), P("tp", None)
    return jax.shard_map(
        step,
        mesh=mesh,
        in_specs=(tokens, tokens, P("dp", "tp"), P("dp", "tp"), columns, columns, rows),
        out_specs=(tokens, P("dp", "tp"), P("dp", "tp"), P(("dp", "tp"), None)),
        check_vma=False,
    )
```

```python
import types

import jax
import jax.numpy as jnp
from jax import lax
from jax.experimental import pallas as pl
from jax.experimental.pallas import tpu as pltpu
from jax.sharding import PartitionSpec as P

MESH = pl.DeviceIdType.MESH
F32, BF16 = jnp.float32, jnp.bfloat16
C = 256
SMALL, RS, RB = 2, 64, 128
EARLY, LAST = 1, (16, 24, 24)


def dot_t(a, b):
    return lax.dot_general(a, b, (((1,), (1,)), ((), ())), preferred_element_type=F32)


def dot(a, b):
    return lax.dot_general(a, b, (((1,), (0,)), ((), ())), preferred_element_type=F32)


def tile(n, start=0):
    return slice(start + n * C, start + (n + 1) * C)


def kernel(
    x_h, dy_h, gate_h, up_h, wg_h, wu_h, wd_h,
    dx, dwg, dwu, dwd,
    xv, acts, wgu, wd, dgu, hid, xt,
    own_s, tsend_s, trecv_s, psend_s, precv_s, own_b, tsend_b, trecv_b, psend_b, precv_b, extra,
    load_sem, sent, landed, term_sem, part_sem, final_sem, extra_sem,
):
    rows, d = xv.shape
    f = wd.shape[0]
    half = rows // 2
    dyv, gv, uv = acts.at[:, 0:d], acts.at[:, d : d + f], acts.at[:, d + f : d + 2 * f]
    me = lax.axis_index("tp")
    chip, core = me // 2, me % 2
    partner, peer, across = chip * 2 + (1 - core), (1 - chip) * 2 + core, (1 - chip) * 2 + (1 - core)
    nb = (half - SMALL * 2 * RS) // (2 * RB)
    small = types.SimpleNamespace(
        r=RS, off=0, n=SMALL, at=0, own=own_s, tsend=tsend_s, trecv=trecv_s, psend=psend_s, precv=precv_s
    )
    big = types.SimpleNamespace(
        r=RB, off=SMALL * 2 * RS, n=nb, at=SMALL, own=own_b, tsend=tsend_b, trecv=trecv_b, psend=psend_b, precv=precv_b
    )

    def base(q, e):
        owner = lax.rem(chip + 1 + e // q.n, 2)
        return pl.multiple_of(owner * half + q.off + lax.rem(e, q.n) * (2 * q.r), 2 * RS)

    def block(q, e, k):
        return pl.ds(pl.multiple_of(base(q, e) + k * q.r, RS), q.r)

    def local(src, dst, sem):
        return pltpu.make_async_copy(src, dst, load_sem.at[sem])

    def load(q, e, sem):
        r = pl.ds(base(q, e), 2 * q.r)
        return [local(src.at[r], dst.at[r], sem) for src, dst in ((dy_h, dyv), (gate_h, gv), (up_h, uv))]

    def all_of(ref, sem):
        return pltpu.make_async_copy(ref, ref, sem)

    def remote(src, dst, send, recv, to):
        return pltpu.make_async_remote_copy(
            src_ref=src, dst_ref=dst, send_sem=send, recv_sem=recv, device_id={"tp": to}, device_id_type=MESH
        )

    def term_copy(q, e, cols=slice(None), n=0):
        recv = term_sem.at[2 * (2 * q.at + e) + n]
        return remote(q.tsend.at[e, :, cols], q.trecv.at[e, :, cols], sent.at[0], recv, partner)

    def part_copy(q, e, cols=slice(None)):
        return remote(q.psend.at[e, :, cols], q.precv.at[e, :, cols], sent.at[1], part_sem.at[q.at + e], peer)

    def extra_copy():
        return remote(tsend_s.at[0, :, tile(0)], extra, sent.at[0], extra_sem, across)

    def final_copy(q, j):
        r = block(q, q.n + j, core)
        return remote(dx.at[r], dx.at[r], sent.at[2], final_sem.at[q.at + j], peer)

    def core_copy(r):
        return remote(dx.at[r], dx.at[r], sent.at[3], landed, partner)

    def start(copies):
        for c in copies:
            c.start()

    def hidden_tile(q, e, n, dyb):
        dh = dot_t(dyb, wd[tile(n), :])
        for part, k in ((dh[: q.r], 1 - core), (dh[q.r :], core)):
            r = block(q, e, k)
            g, u = gv[r, tile(n)].astype(F32), uv[r, tile(n)].astype(F32)
            sig = jax.nn.sigmoid(g)
            act = g * sig
            hid[r, tile(n)] = (act * u).astype(BF16)
            dgu[r, tile(n)] = ((part * u) * (sig + act * (1.0 - sig))).astype(BF16)
            dgu[r, tile(n, f)] = (part * act).astype(BF16)

    def both(ref, q, e):
        return jnp.concatenate([ref[block(q, e, 1 - core), :], ref[block(q, e, core), :]], axis=0)

    def hidden_part(q, e):
        dyb = both(dyv, q, e)
        for n in range(f // C):
            hidden_tile(q, e, n, dyb)

    def term_tile(q, e, n, lhs, alone=False):
        t = dot_t(lhs, wgu[tile(n), :])
        q.tsend[e, :, tile(n)] = t[: q.r].astype(BF16)
        if alone:
            q.psend[e, :, tile(n)] = t[q.r :].astype(BF16)
        else:
            q.own[e, :, tile(n)] = t[q.r :]

    def term_part(q, e):
        lhs = both(dgu, q, e)
        for n in range(d // C):
            term_tile(q, e, n, lhs)
        term_copy(q, e).start()

    def chip_sum(q, e, theirs, cols=slice(None), n=0):
        term_copy(q, e, cols, n).wait_recv()
        s = q.own[e, :, cols] + q.trecv[e, :, cols].astype(F32)
        if theirs:
            q.psend[e, :, cols] = s.astype(BF16)
            part_copy(q, e, cols).start()
        else:
            q.own[e, :, cols] = s

    def finish(q, j):
        part_copy(q, j).wait_recv()
        r = block(q, q.n + j, core)
        total = q.own[q.n + j] + q.precv[j].astype(F32)
        if q is small and j == 0:
            extra_copy().wait_recv()
            dx[r, C:] = total[:, C:].astype(BF16)
            dx[r, :C] = (total[:, :C] + extra[...].astype(F32)).astype(BF16)
        else:
            dx[r, :] = total.astype(BF16)
        if q is big and j == 0:
            final_copy(q, j).start()
        else:

            @pl.when(core != EARLY)
            def _():
                final_copy(q, j).start()

        core_copy(r).start()

    def pass_on(q, j):
        final_copy(q, j).wait_recv()
        core_copy(block(q, j, core)).start()

    def grad_x(m):
        r = pl.ds(pl.multiple_of(m * C, C), C)
        xt[...] = xv[:, r].T
        for n in range(f // C):
            dwg[r, tile(n)] = dot(xt[...], dgu[:, tile(n)]).astype(BF16)
            dwu[r, tile(n)] = dot(xt[...], dgu[:, tile(n, f)]).astype(BF16)

    def grad_h(m):
        r = pl.ds(pl.multiple_of(m * C, C), C)
        xt[...] = hid[:, r].T
        for n in range(d // C):
            dwd[r, tile(n)] = dot(xt[...], dyv[:, tile(n)]).astype(BF16)

    nf, nd = f // C, d // C
    w_sem, first_rows, gu, second_rows, rest, x_sem = 0, 2, 3, 5, 6, 7
    now = pl.ds(base(small, 0), 2 * RS)
    first = [local(dy_h.at[now], dyv.at[now], first_rows)]
    later = []
    for src, dst in ((gate_h, gv), (up_h, uv)):
        first.append(local(src.at[now, 0:C], dst.at[now, 0:C], first_rows))
        later.append(local(src.at[now, C:f], dst.at[now, C:f], w_sem + 1))
    wds = [local(wd_h.at[tile(n)], wd.at[tile(n)], w_sem + min(n, 1)) for n in range(nf)]
    start(first[:1] + wds[:1] + first[1:] + wds[1:] + later)
    for n in range(nd):
        start([local(w.at[tile(n)], wgu.at[tile(n), c * f : (c + 1) * f], gu + n // 2) for c, w in enumerate((wg_h, wu_h))])
    start(load(small, 1, second_rows))
    for e in range(2 * nb):
        start(load(big, e, rest))
    for e in range(SMALL, 2 * SMALL):
        start(load(small, e, rest))
    x_copy = local(x_h, xv, x_sem)
    start([x_copy])

    barrier = pltpu.get_barrier_semaphore()
    for to in (partner, peer, across):
        pl.semaphore_signal(barrier, inc=1, device_id={"tp": to}, device_id_type=MESH)

    all_of(acts.at[now, 0 : d + 2 * C], load_sem.at[first_rows]).wait()
    wds[0].wait()
    dyb = both(dyv, small, 0)
    hidden_tile(small, 0, 0, dyb)
    more = 2 * RS * 2 * (f - C) // d
    all_of(xv.at[0 : f - C + more], load_sem.at[w_sem + 1]).wait()
    for n in range(1, nf):
        hidden_tile(small, 0, n, dyb)
    pl.semaphore_wait(barrier, 3)
    halves = [slice(n * (d // 2), (n + 1) * (d // 2)) for n in range(2)]

    def halves_of_term(q, e):
        lhs = both(dgu, q, e)
        for n in range(2):
            if q is small and e == 0:
                all_of(wgu.at[halves[n]], load_sem.at[gu + n]).wait()
            for m in range(nd // 2):
                term_tile(q, e, n * (nd // 2) + m, lhs, alone=q is small and e == 0 and n == 0 and m == 0)
            cols = halves[n]
            if q is small and e == 0 and n == 0:
                part_copy(small, 0, tile(0)).start()
                extra_copy().start()
                cols = rest_cols
            term_copy(q, e, cols, n).start()

    rest_cols = slice(C, d // 2)
    halves_of_term(small, 0)
    all_of(acts.at[pl.ds(base(small, 1), 2 * RS)], load_sem.at[second_rows]).wait()
    hidden_part(small, 1)
    chip_sum(small, 0, True, rest_cols, 0)
    chip_sum(small, 0, True, halves[1], 1)
    halves_of_term(small, 1)
    chip_sum(small, 1, True, halves[0], 0)
    all_of(acts.at[0 : rows - SMALL * 2 * RS], load_sem.at[rest]).wait()
    hidden_part(big, 0)
    chip_sum(small, 1, True, halves[1], 1)
    halves_of_term(big, 0)

    @pl.loop(1, 2 * nb)
    def _(e):
        hidden_part(big, e)

        @pl.when(e == 1)
        def _():
            for n in range(2):
                chip_sum(big, 0, True, halves[n], n)

        term_part(big, e)

        @pl.when((e > 1) & (e <= nb))
        def _():
            chip_sum(big, e - 1, True)

        @pl.when(e > nb)
        def _():
            chip_sum(big, e - 1, False)

    for e in range(SMALL, 2 * SMALL):
        hidden_part(small, e)
        term_part(small, e)
        if e == SMALL:
            chip_sum(big, 2 * nb - 1, False)
        else:
            chip_sum(small, e - 1, False)

    x_copy.wait()
    finish(big, 0)
    chip_sum(small, 2 * SMALL - 1, False)
    for j in range(SMALL):
        finish(small, j)
    for j in range(1, nb - 1):
        finish(big, j)

    @pl.loop(0, d // C)
    def _(m):
        grad_x(m)

    finish(big, nb - 1)

    @pl.loop(0, f // C)
    def _(m):
        grad_h(m)

        @pl.when(m == f // C - 2)
        def _():
            pass_on(big, 0)

    ahead = RB
    all_of(dx.at[0:half], sent.at[0]).wait()
    all_of(dx.at[0 : half // 2], sent.at[1]).wait()
    all_of(dx.at[0 : half // 2 + ahead], sent.at[3]).wait()
    all_of(dx.at[0 : half // 2 + ahead], landed).wait()

    @pl.when(core == EARLY)
    def _():
        all_of(dx.at[0:ahead], sent.at[2]).wait()

    @pl.when(core != EARLY)
    def _():
        for q in (small, big):
            for j in range(1 if q is big else 0, q.n):
                final_copy(q, j).wait_recv()
        all_of(dx.at[0 : half // 2], sent.at[2]).wait()


def rest_kernel(_, dx, recv, ready, sent, landed):
    half = dx.shape[0] // 2
    me = lax.axis_index("tp")
    chip, core = me // 2, me % 2
    partner, peer, across = chip * 2 + (1 - core), (1 - chip) * 2 + core, (1 - chip) * 2 + (1 - core)
    big = [(SMALL * 2 * RS + j * 2 * RB, RB, 0, RB) for j in range(1, (half - SMALL * 2 * RS) // (2 * RB))]
    small = [(j * 2 * RS, RS, 0, RS) for j in range(SMALL - 1)]
    last = [((SMALL - 1) * 2 * RS, RS, sum(LAST[:n]), size) for n, size in enumerate(LAST)]
    pieces = big + small + last

    def rows(owner, piece):
        at, r, off, size = piece
        return pl.ds(pl.multiple_of(owner * half + at + core * r + off, 8), size)

    def copy(r, send, recv, to):
        return pltpu.make_async_remote_copy(
            src_ref=dx.at[r], dst_ref=dx.at[r], send_sem=send, recv_sem=recv, device_id={"tp": to}, device_id_type=MESH
        )

    def final_copy(n):
        return copy(rows(chip, pieces[n]), sent, recv.at[max(n - len(big) + 1, 0)], peer)

    def core_copy(n):
        return copy(rows(1 - chip, pieces[n]), sent, landed, partner)

    end = len(pieces) - 1
    direct_copy = copy(rows(chip, pieces[end]), sent, landed, across)

    def all_of(n, sem):
        return pltpu.make_async_copy(dx.at[0:n], dx.at[0:n], sem)

    passes = half // 2 - RB
    barrier = pltpu.get_barrier_semaphore()

    @pl.when(core == EARLY)
    def _():
        for to in (peer, partner, across):
            pl.semaphore_signal(barrier, inc=1, device_id={"tp": to}, device_id_type=MESH)

    pl.semaphore_wait(barrier, 1 + lax.rem(core + EARLY, 2))

    @pl.when(core == EARLY)
    def _():
        for n in range(end):
            final_copy(n).start()
        pl.semaphore_wait(ready, 2)
        direct_copy.start()
        final_copy(end).start()
        for n in range(len(pieces)):
            if n == 0:
                all_of(len(big) * RB, recv.at[0]).wait()
            elif n >= len(big):
                final_copy(n).wait_recv()
            if n < end:
                core_copy(n).start()
        all_of(2 * passes, sent).wait()

    @pl.when(core != EARLY)
    def _():
        for to in (partner, across):
            pl.semaphore_signal(ready, inc=1, device_id={"tp": to}, device_id_type=MESH)
        for n in range(len(pieces)):
            core_copy(n).start()
        all_of(passes, sent).wait()

    all_of(passes, landed).wait()


def start_all(pairs, sem):
    copies = [pltpu.make_async_copy(a, b, sem) for a, b in pairs]
    for c in copies:
        c.start()
    return copies


def wait_all(copies):
    for c in copies:
        c.wait()


def rows_of(dx):
    half = dx.shape[0] // 2
    chip = lax.axis_index("tp") // 2
    first = SMALL * 2 * RS
    own = [(chip * half + n * (half // 2), half // 2) for n in range(2)]
    theirs = (1 - chip) * half
    steps = [(theirs + n * 2 * RS, RS) for n in range(SMALL)]
    steps += [(theirs + n, RB) for n in range(first + 2 * RB, half, 2 * RB)]

    def slices(parts):
        return [pl.ds(pl.multiple_of(at, RS), size) for at, size in parts]

    late, early = ([(at + k * size, size) for at, size in steps] for k in (1 - EARLY, EARLY))
    return slices(own + [(theirs + first, 2 * RB)]), slices(late), slices(early)


def write_most(dx_v, dwg_v, dwu_v, dwd_v, _, dx, dwg, dwu, dwd, sem):
    done, late, _ = rows_of(dx)
    pairs = [(dx_v.at[r], dx.at[r]) for r in done]
    for src, dst in ((dwg_v, dwg), (dwu_v, dwu), (dwd_v, dwd)):
        n = src.shape[0] // 2
        pairs += [(src.at[r], dst.at[r]) for r in (pl.ds(0, n), pl.ds(n, n))]
    copies = start_all(pairs, sem)

    @pl.when(lax.rem(lax.axis_index("tp"), 2) != EARLY)
    def _():
        wait_all(start_all([(dx_v.at[r], dx.at[r]) for r in late], sem))

    wait_all(copies)


def write_late(dx_v, _, dx, sem):
    _, late, early = rows_of(dx)
    copies = start_all([(dx_v.at[r], dx.at[r]) for r in early], sem)

    @pl.when(lax.rem(lax.axis_index("tp"), 2) == EARLY)
    def _():
        wait_all(start_all([(dx_v.at[r], dx.at[r]) for r in late], sem))

    wait_all(copies)


def solution(mesh):
    def step(x, dy, gate, up, w_gate, w_up, w_down):
        rows, d = x.shape
        f = gate.shape[1]
        nb = (rows // 2 - SMALL * 2 * RS) // (2 * RB)
        outs = [((rows, d), BF16), ((d, f), BF16), ((d, f), BF16), ((f, d), BF16)]
        dma = pltpu.SemaphoreType.DMA

        def buffers(n, r):
            shapes = ((2 * n, F32), (2 * n, BF16), (2 * n, BF16), (n, BF16), (n, BF16))
            return [pltpu.VMEM((m, r, d), t) for m, t in shapes]

        dx, *grads = pl.pallas_call(
            kernel,
            out_shape=[pltpu.VMEM(s, t) for s, t in outs],
            in_specs=[pl.BlockSpec(memory_space=pl.ANY)] * 7,
            out_specs=[pl.BlockSpec(memory_space=pltpu.VMEM)] * 4,
            scratch_shapes=[
                pltpu.VMEM((rows, d), BF16),
                pltpu.VMEM((rows, d + 2 * f), BF16),
                pltpu.VMEM((d, 2 * f), BF16),
                pltpu.VMEM((f, d), BF16),
                pltpu.VMEM((rows, 2 * f), BF16),
                pltpu.VMEM((rows, f), BF16),
                pltpu.VMEM((C, rows), BF16),
            ]
            + buffers(SMALL, RS)
            + buffers(nb, RB)
            + [
                pltpu.VMEM((RS, C), BF16),
                dma((8,)),
                dma((4,)),
                dma(()),
                dma((4 * (SMALL + nb),)),
                dma((SMALL + nb,)),
                dma((SMALL + nb,)),
                dma(()),
            ],
            compiler_params=pltpu.CompilerParams(
                collective_id=0, has_side_effects=True, vmem_limit_bytes=50 * 2**20
            ),
            name="block",
        )(x, dy, gate, up, w_gate, w_up, w_down)
        held, plain = pl.BlockSpec(memory_space=pltpu.VMEM), pl.BlockSpec(memory_space=pl.ANY)
        shapes = [jax.ShapeDtypeStruct(s, t) for s, t in outs]
        little = 2**20

        def pin(a):
            return pltpu.with_memory_space_constraint(a, pltpu.VMEM)

        dx, most, *grads = pl.pallas_call(
            write_most,
            out_shape=[pltpu.VMEM(*outs[0])] + shapes,
            in_specs=[plain] + [held] * 3,
            out_specs=[plain] * 5,
            scratch_shapes=[dma(())],
            input_output_aliases={0: 0},
            compiler_params=pltpu.CompilerParams(vmem_limit_bytes=little),
            name="write_most",
        )(pin(dx), *(pin(g) for g in grads))
        dx = pl.pallas_call(
            rest_kernel,
            out_shape=pltpu.VMEM(*outs[0]),
            in_specs=[plain],
            out_specs=plain,
            scratch_shapes=[
                dma((SMALL + len(LAST),)), pltpu.SemaphoreType.REGULAR, dma(()), dma(())
            ],
            input_output_aliases={0: 0},
            compiler_params=pltpu.CompilerParams(collective_id=1, has_side_effects=True, vmem_limit_bytes=little),
            name="rest",
        )(pin(dx))
        dx = pl.pallas_call(
            write_late,
            out_shape=shapes[0],
            in_specs=[held, plain],
            out_specs=plain,
            scratch_shapes=[dma(())],
            input_output_aliases={1: 0},
            compiler_params=pltpu.CompilerParams(vmem_limit_bytes=little),
            name="write_late",
        )(pin(dx), most)
        return dx, *grads

    tokens, columns, rows = P("dp", None), P(None, "tp"), P("tp", None)
    return jax.shard_map(
        step,
        mesh=mesh,
        in_specs=(tokens, tokens, P("dp", "tp"), P("dp", "tp"), columns, columns, rows),
        out_specs=(tokens, P("dp", "tp"), P("dp", "tp"), P(("dp", "tp"), None)),
        check_vma=False,
    )
```

```python
import types

import jax
import jax.numpy as jnp
from jax import lax
from jax.experimental import pallas as pl
from jax.experimental.pallas import tpu as pltpu
from jax.sharding import PartitionSpec as P

MESH = pl.DeviceIdType.MESH
F32, BF16 = jnp.float32, jnp.bfloat16
C = 256
SMALL, RS, RB = 2, 64, 128
EARLY, LAST = 1, (16, 24, 24)


def dot_t(a, b):
    return lax.dot_general(a, b, (((1,), (1,)), ((), ())), preferred_element_type=F32)


def dot(a, b):
    return lax.dot_general(a, b, (((1,), (0,)), ((), ())), preferred_element_type=F32)


def tile(n, start=0):
    return slice(start + n * C, start + (n + 1) * C)


def kernel(
    x_h, dy_h, gate_h, up_h, wg_h, wu_h, wd_h,
    dx, dwg, dwu, dwd,
    xv, acts, wgu, wd, dgu, hid, xt,
    own_s, tsend_s, trecv_s, psend_s, precv_s, own_b, tsend_b, trecv_b, psend_b, precv_b, extra,
    load_sem, sent, landed, term_sem, part_sem, final_sem, extra_sem,
):
    rows, d = xv.shape
    f = wd.shape[0]
    half = rows // 2
    dyv, gv, uv = acts.at[:, 0:d], acts.at[:, d : d + f], acts.at[:, d + f : d + 2 * f]
    me = lax.axis_index("tp")
    chip, core = me // 2, me % 2
    partner, peer, across = chip * 2 + (1 - core), (1 - chip) * 2 + core, (1 - chip) * 2 + (1 - core)
    nb = (half - SMALL * 2 * RS) // (2 * RB)
    small = types.SimpleNamespace(
        r=RS, off=0, n=SMALL, at=0, own=own_s, tsend=tsend_s, trecv=trecv_s, psend=psend_s, precv=precv_s
    )
    big = types.SimpleNamespace(
        r=RB, off=SMALL * 2 * RS, n=nb, at=SMALL, own=own_b, tsend=tsend_b, trecv=trecv_b, psend=psend_b, precv=precv_b
    )

    def base(q, e):
        owner = lax.rem(chip + 1 + e // q.n, 2)
        return pl.multiple_of(owner * half + q.off + lax.rem(e, q.n) * (2 * q.r), 2 * RS)

    def block(q, e, k):
        return pl.ds(pl.multiple_of(base(q, e) + k * q.r, RS), q.r)

    def local(src, dst, sem):
        return pltpu.make_async_copy(src, dst, load_sem.at[sem])

    def load(q, e, sem):
        r = pl.ds(base(q, e), 2 * q.r)
        return [local(src.at[r], dst.at[r], sem) for src, dst in ((dy_h, dyv), (gate_h, gv), (up_h, uv))]

    def all_of(ref, sem):
        return pltpu.make_async_copy(ref, ref, sem)

    def remote(src, dst, send, recv, to):
        return pltpu.make_async_remote_copy(
            src_ref=src, dst_ref=dst, send_sem=send, recv_sem=recv, device_id={"tp": to}, device_id_type=MESH
        )

    def term_copy(q, e, cols=slice(None), n=0):
        recv = term_sem.at[2 * (2 * q.at + e) + n]
        return remote(q.tsend.at[e, :, cols], q.trecv.at[e, :, cols], sent.at[0], recv, partner)

    def part_copy(q, e, cols=slice(None)):
        return remote(q.psend.at[e, :, cols], q.precv.at[e, :, cols], sent.at[1], part_sem.at[q.at + e], peer)

    def extra_copy():
        return remote(tsend_s.at[0, :, tile(0)], extra, sent.at[0], extra_sem, across)

    def final_copy(q, j):
        r = block(q, q.n + j, core)
        return remote(dx.at[r], dx.at[r], sent.at[2], final_sem.at[q.at + j], peer)

    def core_copy(r):
        return remote(dx.at[r], dx.at[r], sent.at[3], landed, partner)

    def start(copies):
        for c in copies:
            c.start()

    def hidden_tile(q, e, n, dyb):
        dh = dot_t(dyb, wd[tile(n), :])
        for part, k in ((dh[: q.r], 1 - core), (dh[q.r :], core)):
            r = block(q, e, k)
            g, u = gv[r, tile(n)].astype(F32), uv[r, tile(n)].astype(F32)
            sig = jax.nn.sigmoid(g)
            act = g * sig
            hid[r, tile(n)] = (act * u).astype(BF16)
            dgu[r, tile(n)] = ((part * u) * (sig + act * (1.0 - sig))).astype(BF16)
            dgu[r, tile(n, f)] = (part * act).astype(BF16)

    def both(ref, q, e):
        return jnp.concatenate([ref[block(q, e, 1 - core), :], ref[block(q, e, core), :]], axis=0)

    def hidden_part(q, e):
        dyb = both(dyv, q, e)
        for n in range(f // C):
            hidden_tile(q, e, n, dyb)

    def term_tile(q, e, n, lhs, alone=False):
        t = dot_t(lhs, wgu[tile(n), :])
        q.tsend[e, :, tile(n)] = t[: q.r].astype(BF16)
        if alone:
            q.psend[e, :, tile(n)] = t[q.r :].astype(BF16)
        else:
            q.own[e, :, tile(n)] = t[q.r :]

    def term_part(q, e):
        lhs = both(dgu, q, e)
        for n in range(d // C):
            term_tile(q, e, n, lhs)
        term_copy(q, e).start()

    def chip_sum(q, e, theirs, cols=slice(None), n=0):
        term_copy(q, e, cols, n).wait_recv()
        s = q.own[e, :, cols] + q.trecv[e, :, cols].astype(F32)
        if theirs:
            q.psend[e, :, cols] = s.astype(BF16)
            part_copy(q, e, cols).start()
        else:
            q.own[e, :, cols] = s

    def finish(q, j):
        part_copy(q, j).wait_recv()
        r = block(q, q.n + j, core)
        total = q.own[q.n + j] + q.precv[j].astype(F32)
        if q is small and j == 0:
            extra_copy().wait_recv()
            dx[r, C:] = total[:, C:].astype(BF16)
            dx[r, :C] = (total[:, :C] + extra[...].astype(F32)).astype(BF16)
        else:
            dx[r, :] = total.astype(BF16)
        if q is big and j == 0:
            final_copy(q, j).start()
        else:

            @pl.when(core != EARLY)
            def _():
                final_copy(q, j).start()

        core_copy(r).start()

    def pass_on(q, j):
        final_copy(q, j).wait_recv()
        core_copy(block(q, j, core)).start()

    def grad_x(m):
        r = pl.ds(pl.multiple_of(m * C, C), C)
        xt[...] = xv[:, r].T
        for n in range(f // C):
            dwg[r, tile(n)] = dot(xt[...], dgu[:, tile(n)]).astype(BF16)
            dwu[r, tile(n)] = dot(xt[...], dgu[:, tile(n, f)]).astype(BF16)

    def grad_h(m):
        r = pl.ds(pl.multiple_of(m * C, C), C)
        xt[...] = hid[:, r].T
        for n in range(d // C):
            dwd[r, tile(n)] = dot(xt[...], dyv[:, tile(n)]).astype(BF16)

    nf, nd = f // C, d // C
    w_sem, first_rows, gu, second_rows, rest, x_sem = 0, 2, 3, 5, 6, 7
    now = pl.ds(base(small, 0), 2 * RS)
    first = [local(dy_h.at[now], dyv.at[now], first_rows)]
    later = []
    for src, dst in ((gate_h, gv), (up_h, uv)):
        first.append(local(src.at[now, 0:C], dst.at[now, 0:C], first_rows))
        later.append(local(src.at[now, C:f], dst.at[now, C:f], w_sem + 1))
    wds = [local(wd_h.at[tile(n)], wd.at[tile(n)], w_sem + min(n, 1)) for n in range(nf)]
    start(first[:1] + wds[:1] + first[1:] + wds[1:] + later)
    for n in range(nd):
        start([local(w.at[tile(n)], wgu.at[tile(n), c * f : (c + 1) * f], gu + n // 2) for c, w in enumerate((wg_h, wu_h))])
    start(load(small, 1, second_rows))
    for e in range(2 * nb):
        start(load(big, e, rest))
    for e in range(SMALL, 2 * SMALL):
        start(load(small, e, rest))
    x_copy = local(x_h, xv, x_sem)
    start([x_copy])

    barrier = pltpu.get_barrier_semaphore()
    for to in (partner, peer, across):
        pl.semaphore_signal(barrier, inc=1, device_id={"tp": to}, device_id_type=MESH)

    all_of(acts.at[now, 0 : d + 2 * C], load_sem.at[first_rows]).wait()
    wds[0].wait()
    dyb = both(dyv, small, 0)
    hidden_tile(small, 0, 0, dyb)
    more = 2 * RS * 2 * (f - C) // d
    all_of(xv.at[0 : f - C + more], load_sem.at[w_sem + 1]).wait()
    for n in range(1, nf):
        hidden_tile(small, 0, n, dyb)
    halves = [slice(n * (d // 2), (n + 1) * (d // 2)) for n in range(2)]

    def halves_of_term(q, e):
        lhs = both(dgu, q, e)
        for n in range(2):
            if q is small and e == 0:
                all_of(wgu.at[halves[n]], load_sem.at[gu + n]).wait()
            for m in range(nd // 2):
                term_tile(q, e, n * (nd // 2) + m, lhs, alone=q is small and e == 0 and n == 0 and m == 0)
            cols = halves[n]
            if q is small and e == 0 and n == 0:
                pl.semaphore_wait(barrier, 3)
                part_copy(small, 0, tile(0)).start()
                extra_copy().start()
                cols = rest_cols
            term_copy(q, e, cols, n).start()

    rest_cols = slice(C, d // 2)
    halves_of_term(small, 0)
    all_of(acts.at[pl.ds(base(small, 1), 2 * RS)], load_sem.at[second_rows]).wait()
    hidden_part(small, 1)
    chip_sum(small, 0, True, rest_cols, 0)
    chip_sum(small, 0, True, halves[1], 1)
    halves_of_term(small, 1)
    chip_sum(small, 1, True, halves[0], 0)
    all_of(acts.at[0 : rows - SMALL * 2 * RS], load_sem.at[rest]).wait()
    hidden_part(big, 0)
    chip_sum(small, 1, True, halves[1], 1)
    halves_of_term(big, 0)

    @pl.loop(1, 2 * nb)
    def _(e):
        hidden_part(big, e)

        @pl.when(e == 1)
        def _():
            for n in range(2):
                chip_sum(big, 0, True, halves[n], n)

        term_part(big, e)

        @pl.when((e > 1) & (e <= nb))
        def _():
            chip_sum(big, e - 1, True)

        @pl.when(e > nb)
        def _():
            chip_sum(big, e - 1, False)

    for e in range(SMALL, 2 * SMALL):
        hidden_part(small, e)
        term_part(small, e)
        if e == SMALL:
            chip_sum(big, 2 * nb - 1, False)
        else:
            chip_sum(small, e - 1, False)

    x_copy.wait()
    finish(big, 0)
    chip_sum(small, 2 * SMALL - 1, False)
    for j in range(SMALL):
        finish(small, j)
    for j in range(1, nb - 1):
        finish(big, j)

    @pl.loop(0, d // C)
    def _(m):
        grad_x(m)

    finish(big, nb - 1)

    @pl.loop(0, f // C)
    def _(m):
        grad_h(m)

        @pl.when(m == f // C - 2)
        def _():
            pass_on(big, 0)

    ahead = RB
    all_of(dx.at[0:half], sent.at[0]).wait()
    all_of(dx.at[0 : half // 2], sent.at[1]).wait()
    all_of(dx.at[0 : half // 2 + ahead], sent.at[3]).wait()
    all_of(dx.at[0 : half // 2 + ahead], landed).wait()

    @pl.when(core == EARLY)
    def _():
        all_of(dx.at[0:ahead], sent.at[2]).wait()

    @pl.when(core != EARLY)
    def _():
        for q in (small, big):
            for j in range(1 if q is big else 0, q.n):
                final_copy(q, j).wait_recv()
        all_of(dx.at[0 : half // 2], sent.at[2]).wait()


def rest_kernel(_, dx, recv, ready, sent, landed):
    half = dx.shape[0] // 2
    me = lax.axis_index("tp")
    chip, core = me // 2, me % 2
    partner, peer, across = chip * 2 + (1 - core), (1 - chip) * 2 + core, (1 - chip) * 2 + (1 - core)
    big = [(SMALL * 2 * RS + j * 2 * RB, RB, 0, RB) for j in range(1, (half - SMALL * 2 * RS) // (2 * RB))]
    small = [(j * 2 * RS, RS, 0, RS) for j in range(SMALL - 1)]
    last = [((SMALL - 1) * 2 * RS, RS, sum(LAST[:n]), size) for n, size in enumerate(LAST)]
    pieces = big + small + last

    def rows(owner, piece):
        at, r, off, size = piece
        return pl.ds(pl.multiple_of(owner * half + at + core * r + off, 8), size)

    def copy(r, send, recv, to):
        return pltpu.make_async_remote_copy(
            src_ref=dx.at[r], dst_ref=dx.at[r], send_sem=send, recv_sem=recv, device_id={"tp": to}, device_id_type=MESH
        )

    def final_copy(n):
        return copy(rows(chip, pieces[n]), sent, recv.at[max(n - len(big) + 1, 0)], peer)

    def core_copy(n):
        return copy(rows(1 - chip, pieces[n]), sent, landed, partner)

    end = len(pieces) - 1
    direct_copy = copy(rows(chip, pieces[end]), sent, landed, across)

    def all_of(n, sem):
        return pltpu.make_async_copy(dx.at[0:n], dx.at[0:n], sem)

    passes = half // 2 - RB
    barrier = pltpu.get_barrier_semaphore()

    @pl.when(core == EARLY)
    def _():
        for to in (peer, partner, across):
            pl.semaphore_signal(barrier, inc=1, device_id={"tp": to}, device_id_type=MESH)

    pl.semaphore_wait(barrier, 1 + lax.rem(core + EARLY, 2))

    @pl.when(core == EARLY)
    def _():
        for n in range(end):
            final_copy(n).start()
        pl.semaphore_wait(ready, 2)
        direct_copy.start()
        final_copy(end).start()
        for n in range(len(pieces)):
            if n == 0:
                all_of(len(big) * RB, recv.at[0]).wait()
            elif n >= len(big):
                final_copy(n).wait_recv()
            if n < end:
                core_copy(n).start()
        all_of(2 * passes, sent).wait()

    @pl.when(core != EARLY)
    def _():
        for to in (partner, across):
            pl.semaphore_signal(ready, inc=1, device_id={"tp": to}, device_id_type=MESH)
        for n in range(len(pieces)):
            core_copy(n).start()
        all_of(passes, sent).wait()

    all_of(passes, landed).wait()


def start_all(pairs, sem):
    copies = [pltpu.make_async_copy(a, b, sem) for a, b in pairs]
    for c in copies:
        c.start()
    return copies


def wait_all(copies):
    for c in copies:
        c.wait()


def rows_of(dx):
    half = dx.shape[0] // 2
    chip = lax.axis_index("tp") // 2
    first = SMALL * 2 * RS
    own = [(chip * half + n * (half // 2), half // 2) for n in range(2)]
    theirs = (1 - chip) * half
    steps = [(theirs + n * 2 * RS, RS) for n in range(SMALL)]
    steps += [(theirs + n, RB) for n in range(first + 2 * RB, half, 2 * RB)]

    def slices(parts):
        return [pl.ds(pl.multiple_of(at, RS), size) for at, size in parts]

    late, early = ([(at + k * size, size) for at, size in steps] for k in (1 - EARLY, EARLY))
    return slices(own + [(theirs + first, 2 * RB)]), slices(late), slices(early)


def write_most(dx_v, dwg_v, dwu_v, dwd_v, _, dx, dwg, dwu, dwd, sem):
    done, late, _ = rows_of(dx)
    pairs = [(dx_v.at[r], dx.at[r]) for r in done]
    for src, dst in ((dwg_v, dwg), (dwu_v, dwu), (dwd_v, dwd)):
        n = src.shape[0] // 2
        pairs += [(src.at[r], dst.at[r]) for r in (pl.ds(0, n), pl.ds(n, n))]
    copies = start_all(pairs, sem)

    @pl.when(lax.rem(lax.axis_index("tp"), 2) != EARLY)
    def _():
        wait_all(start_all([(dx_v.at[r], dx.at[r]) for r in late], sem))

    wait_all(copies)


def write_late(dx_v, _, dx, sem):
    _, late, early = rows_of(dx)
    copies = start_all([(dx_v.at[r], dx.at[r]) for r in early], sem)

    @pl.when(lax.rem(lax.axis_index("tp"), 2) == EARLY)
    def _():
        wait_all(start_all([(dx_v.at[r], dx.at[r]) for r in late], sem))

    wait_all(copies)


def solution(mesh):
    def step(x, dy, gate, up, w_gate, w_up, w_down):
        rows, d = x.shape
        f = gate.shape[1]
        nb = (rows // 2 - SMALL * 2 * RS) // (2 * RB)
        outs = [((rows, d), BF16), ((d, f), BF16), ((d, f), BF16), ((f, d), BF16)]
        dma = pltpu.SemaphoreType.DMA

        def buffers(n, r):
            shapes = ((2 * n, F32), (2 * n, BF16), (2 * n, BF16), (n, BF16), (n, BF16))
            return [pltpu.VMEM((m, r, d), t) for m, t in shapes]

        dx, *grads = pl.pallas_call(
            kernel,
            out_shape=[pltpu.VMEM(s, t) for s, t in outs],
            in_specs=[pl.BlockSpec(memory_space=pl.ANY)] * 7,
            out_specs=[pl.BlockSpec(memory_space=pltpu.VMEM)] * 4,
            scratch_shapes=[
                pltpu.VMEM((rows, d), BF16),
                pltpu.VMEM((rows, d + 2 * f), BF16),
                pltpu.VMEM((d, 2 * f), BF16),
                pltpu.VMEM((f, d), BF16),
                pltpu.VMEM((rows, 2 * f), BF16),
                pltpu.VMEM((rows, f), BF16),
                pltpu.VMEM((C, rows), BF16),
            ]
            + buffers(SMALL, RS)
            + buffers(nb, RB)
            + [
                pltpu.VMEM((RS, C), BF16),
                dma((8,)),
                dma((4,)),
                dma(()),
                dma((4 * (SMALL + nb),)),
                dma((SMALL + nb,)),
                dma((SMALL + nb,)),
                dma(()),
            ],
            compiler_params=pltpu.CompilerParams(
                collective_id=0, has_side_effects=True, vmem_limit_bytes=50 * 2**20
            ),
            name="block",
        )(x, dy, gate, up, w_gate, w_up, w_down)
        held, plain = pl.BlockSpec(memory_space=pltpu.VMEM), pl.BlockSpec(memory_space=pl.ANY)
        shapes = [jax.ShapeDtypeStruct(s, t) for s, t in outs]
        little = 2**20

        def pin(a):
            return pltpu.with_memory_space_constraint(a, pltpu.VMEM)

        dx, most, *grads = pl.pallas_call(
            write_most,
            out_shape=[pltpu.VMEM(*outs[0])] + shapes,
            in_specs=[plain] + [held] * 3,
            out_specs=[plain] * 5,
            scratch_shapes=[dma(())],
            input_output_aliases={0: 0},
            compiler_params=pltpu.CompilerParams(vmem_limit_bytes=little),
            name="write_most",
        )(pin(dx), *(pin(g) for g in grads))
        dx = pl.pallas_call(
            rest_kernel,
            out_shape=pltpu.VMEM(*outs[0]),
            in_specs=[plain],
            out_specs=plain,
            scratch_shapes=[
                dma((SMALL + len(LAST),)), pltpu.SemaphoreType.REGULAR, dma(()), dma(())
            ],
            input_output_aliases={0: 0},
            compiler_params=pltpu.CompilerParams(collective_id=1, has_side_effects=True, vmem_limit_bytes=little),
            name="rest",
        )(pin(dx))
        dx = pl.pallas_call(
            write_late,
            out_shape=shapes[0],
            in_specs=[held, plain],
            out_specs=plain,
            scratch_shapes=[dma(())],
            input_output_aliases={1: 0},
            compiler_params=pltpu.CompilerParams(vmem_limit_bytes=little),
            name="write_late",
        )(pin(dx), most)
        return dx, *grads

    tokens, columns, rows = P("dp", None), P(None, "tp"), P("tp", None)
    return jax.shard_map(
        step,
        mesh=mesh,
        in_specs=(tokens, tokens, P("dp", "tp"), P("dp", "tp"), columns, columns, rows),
        out_specs=(tokens, P("dp", "tp"), P("dp", "tp"), P(("dp", "tp"), None)),
        check_vma=False,
    )
```
